256 devices in a mesh: groups: 2 (over y), dp: 2 (over core), tensor: 64 (over x, z).
Axes of the slice: x: 4, y: 2, z: 16, core: 2. Of those that a mesh axis runs over, the one named last changes fastest.
The devices are a block of a 4x16x16 slice.
Arguments:
- hidden_in: bfloat16 [4, 1024, 5120], P(('groups', 'dp'), 'tensor'), parts along dimension 0, may hold values from -40 to 40
- first_values: bfloat16 [4, 1024, 8192], P(('groups', 'dp'), 'tensor'), parts along dimension 0, may hold values from -6 to 6
- qkv_weight: bfloat16 [5120, 3, 8192], P(None, None, 'tensor'), may hold values from -1 to 1
- out_weight: bfloat16 [8192, 5120], P('tensor'), may hold values from -0.1875 to 0.1875
- mix_table: float32 [8, 2], replicated, may hold values from 0.2 to 1
- mix_index: int32 [64], P('tensor'), may hold values from 0 to 7
- lengths: int32 [4], P(('groups', 'dp')), parts along dimension 0, may hold values from 256 to 1024
Outputs:
- attn_out: bfloat16 [4, 1024, 5120], P(('groups', 'dp'), 'tensor'), parts along dimension 0
The draws below stay inside these ranges and needn't reach their ends.
There are 2 independent parts, one for each index of `groups`. The reference program is written for one: setup_inputs(seed, part) draws one part's arguments, and reference() takes and returns one part's arrays. A program takes and returns all parts, laid end to end along the dimension named above; an argument that names none is the same for every part. Nothing has to cross between parts.
All inputs are finite; a program needn't handle non-finite values.
Results may differ from the reference program's by a relative error of at most 0.0077.
Values may be sent and summed in bfloat16 or wider, within the bound.
A program may use at most 128 MiB of HBM per device.

```python
import math
import jax
import jax.numpy as jnp
from jax import lax

D = 5120
HS = 128
MIXES = 8
SEQ = 1024
HEADS = 64
SEQS = 2


def draw_hidden_in(key, part):
    samples = jnp.clip(jax.random.normal(jax.random.fold_in(key, 11), (SEQS, SEQ, D), jnp.float32), -6.0, 6.0)
    return samples.astype(jnp.bfloat16)


def draw_qkv_weight(key, part):
    inner_width = HEADS * HS
    spread = 1.0 / math.sqrt(D)
    weights = jax.random.normal(jax.random.fold_in(key, 21), (D, 3, inner_width), jnp.float32) * spread
    return jnp.clip(weights, -1.0, 1.0).astype(jnp.bfloat16)


def with_ends(drawn, own_key, least, top_value):
    longest = drawn.shape.index(max(drawn.shape))
    spots = []
    for shift in (0, 1):
        where = [jax.random.randint(jax.random.fold_in(own_key, axis), (), 0, length) for axis, length in enumerate(drawn.shape)]
        where[longest] = (where[longest] + shift) % drawn.shape[longest]
        spots.append(tuple(where))
    return drawn.at[spots[0]].set(least).at[spots[1]].set(top_value)


def level_of(key, dims, cuts, smallest, high):
    gain, own = 1.0, jax.random.fold_in(key, 6)
    for position, shards_of in cuts:
        steps = jnp.exp(jax.random.uniform(jax.random.fold_in(own, position), (shards_of,), jnp.float32, smallest / len(cuts), high / len(cuts)))
        gain = gain * jnp.repeat(steps, dims[position] // shards_of).reshape([-1 if axis == position else 1 for axis in range(len(dims))])
    return gain


def scatter_about(stream_key, dims, width, limit, shards=(), kind=jnp.bfloat16):
    values = width * jax.random.normal(stream_key, dims, jnp.float32)
    if shards:
        values = values * level_of(stream_key, dims, shards, -0.22, 0.18)
    return jnp.clip(values, -limit, limit).astype(kind)


def setup_inputs(seed: int = 0, part: int = 0) -> dict:
    splits = jax.random.split(jax.random.key(seed), 8)
    own_keys = jax.random.split(jax.random.fold_in(splits[7], part), 8)
    hidden_in = draw_hidden_in(jax.random.fold_in(jax.random.fold_in(splits[7], part), 71), part)
    first_values = scatter_about(own_keys[1], (SEQS, SEQ, HEADS * HS), 1.0, 6.0, ((0, 2), (1, 64)))
    qkv_weight = draw_qkv_weight(jax.random.fold_in(splits[7], 71), part)
    out_weight = scatter_about(splits[3], (HEADS * HS, D), (8 * HS) ** -0.5, 0.1875, ((0, 64),))
    mix_table = jnp.clip(jax.random.uniform(splits[4], (MIXES, 2), jnp.float32, 0.2, 1.0), 0.2, 1.0)
    mix_index = with_ends(jax.random.randint(splits[5], (HEADS,), 0, MIXES), jax.random.fold_in(splits[5], 1), 0, MIXES - 1).astype(jnp.int32)
    lengths = jax.random.randint(own_keys[6], (SEQS,), SEQ // 4, SEQ + 1).astype(jnp.int32)
    return {"hidden_in": hidden_in, "first_values": first_values, "qkv_weight": qkv_weight, "out_weight": out_weight, "mix_table": mix_table, "mix_index": mix_index, "lengths": lengths}


NEG_FILL = -1e+30

def reference(hidden_in, first_values, qkv_weight, out_weight, mix_table, mix_index, lengths):
    merged_weight = qkv_weight.reshape(D, 3 * HEADS * HS)
    lambdas = mix_table[mix_index]
    score_scale = 1.0 / math.sqrt(HS)
    positions = jnp.arange(SEQ, dtype=jnp.int32)

    def one_sequence(packed):
        tok_rows, firsts, valid_length = packed
        projected = jnp.dot(tok_rows, merged_weight, preferred_element_type=jnp.float32).astype(jnp.bfloat16)
        split_parts = projected.reshape(SEQ, 3, HEADS, HS)
        first_float = firsts.reshape(SEQ, HEADS, HS).astype(jnp.float32)
        value_float = split_parts[:, 2].astype(jnp.float32)
        mixed_values = (lambdas[None, :, 0:1] * value_float + lambdas[None, :, 1:2] * first_float).astype(jnp.bfloat16)
        allowed = (positions[None, :] <= positions[:, None]) & (positions[None, :] < valid_length)

        def one_head(items):
            query_rows, key_rows, value_rows = items
            scores = jnp.dot(query_rows, key_rows.T, preferred_element_type=jnp.float32) * score_scale
            scores = jnp.where(allowed, scores, NEG_FILL)
            row_max = lax.optimization_barrier(jnp.max(scores, axis=1, keepdims=True))
            raised = jnp.exp(scores - row_max)
            weights = (raised / lax.optimization_barrier(jnp.sum(raised, axis=1, keepdims=True))).astype(jnp.bfloat16)
            return jnp.dot(weights, value_rows, preferred_element_type=jnp.float32).astype(jnp.bfloat16)
        per_head = lax.map(one_head, (jnp.transpose(split_parts[:, 0], (1, 0, 2)), jnp.transpose(split_parts[:, 1], (1, 0, 2)), jnp.transpose(mixed_values, (1, 0, 2))))
        attended = jnp.transpose(per_head, (1, 0, 2)).reshape(SEQ, HEADS * HS)
        return jnp.dot(attended, out_weight, preferred_element_type=jnp.float32).astype(jnp.bfloat16)
    return lax.map(one_sequence, (hidden_in, first_values, lengths))
```

```python
import functools
import math

import jax
import jax.numpy as jnp
from jax import lax
from jax.experimental import pallas as pl
from jax.experimental.pallas import tpu as pltpu
from jax.sharding import Mesh
from jax.sharding import PartitionSpec as P

TENSOR = ("tensor_0", "tensor_1")
NEG_FILL = -1e30
BF = jnp.bfloat16
F32 = jnp.float32
NX = 4
SUB = 256
LAG = 2


def kernel(
    nz,
    hid,
    firsts,
    w_qkv,
    w_out,
    mix_table,
    mix_index,
    lengths,
    out,
    h_buf,
    w2,
    w_relay,
    wo2,
    wo_relay,
    fv_stage,
    fv_own,
    fv_plus,
    fv_minus,
    stash,
    a_send,
    a_recv,
    b_send,
    b_recv,
    q_buf,
    k_buf,
    v_buf,
    att,
    rs_send,
    rs_recv,
    fin,
    out_v,
    local_sem,
    send_sem,
    hid_sem,
    ag_sem,
    w_sem,
    wo_sem,
    fx_sem,
    fz_sem,
    a_sem,
    b_sem,
    att_sem,
    rs_sem,
    fin_sem,
):
    rows, model = hid.shape
    hs = w_qkv.shape[2]
    quarter = model // NX
    half = quarter // 2
    subs = quarter // SUB
    turns = nz // 2
    block = NX * rows

    x = lax.axis_index("tensor_0")
    z = lax.axis_index("tensor_1")
    core = lax.axis_index("dp")
    xs = [x] + [lax.rem(x + d, NX) for d in range(1, NX)]
    z_up = lax.rem(z + 1, nz)
    z_down = lax.rem(z + nz - 1, nz)
    x_way = lax.rem(x + 1 + 2 * core, NX)

    def remote(src, dst, send, recv, **where):
        return pltpu.make_async_remote_copy(
            src_ref=src,
            dst_ref=dst,
            send_sem=send,
            recv_sem=recv,
            device_id=where,
            device_id_type=pl.DeviceIdType.MESH,
        )

    def arrived(ref, sem):
        pltpu.make_async_copy(ref, ref, sem).wait()

    barrier = pltpu.get_barrier_semaphore()
    partners = [
        {"dp": 1 - core},
        {"tensor_0": xs[1]},
        {"tensor_0": xs[2]},
        {"tensor_0": xs[3]},
        {"tensor_1": z_up},
        {"tensor_1": z_down},
    ]
    for partner in partners:
        pl.semaphore_signal(
            barrier, inc=1, device_id=partner, device_id_type=pl.DeviceIdType.MESH
        )
    pl.semaphore_wait(barrier, len(partners))

    for d in (1, 2, 3):
        for s in range(subs):
            column = pl.multiple_of(xs[d] * quarter + s * SUB, 128)
            remote(
                hid.at[:, pl.ds(column, SUB)],
                h_buf.at[0, s, x],
                send_sem.at[0],
                hid_sem.at[d, s],
                tensor_0=xs[d],
            ).start()
    own_hidden = []
    for s in range(subs):
        column = pl.multiple_of(x * quarter + s * SUB, 128)
        own_hidden.append(
            pltpu.make_async_copy(
                hid.at[:, pl.ds(column, SUB)], h_buf.at[0, s, x], hid_sem.at[0, s]
            )
        )
        own_hidden[-1].start()

    my_half = pl.multiple_of(core * half, 128)

    def w_rows(to):
        return pl.ds(pl.multiple_of(to * quarter + core * half, 128), half)

    for p in range(3):
        remote(
            w_qkv.at[p, w_rows(xs[2])],
            w_relay.at[p],
            send_sem.at[1],
            w_sem.at[0, p],
            tensor_0=x_way,
        ).start()
    for d, r, sem in ((1, 3, 1), (3, 1, 2)):
        for p in range(3):
            remote(
                w_qkv.at[p, w_rows(xs[d])],
                w2.at[pl.ds(my_half, half), pl.ds((r * 3 + p) * hs, hs)],
                send_sem.at[1],
                w_sem.at[sem, p],
                tensor_0=xs[d],
            ).start()
    own_weights = []
    for p in range(3):
        own_weights.append(
            pltpu.make_async_copy(
                w_qkv.at[p, pl.ds(pl.multiple_of(x * quarter, 128), quarter)],
                w2.at[:, pl.ds(p * hs, hs)],
                local_sem.at[p],
            )
        )
    own_weights.append(
        pltpu.make_async_copy(
            w_out.at[:, pl.ds(pl.multiple_of(x * quarter, 128), quarter)],
            wo2.at[pl.ds(0, hs)],
            local_sem.at[3],
        )
    )
    for copy in own_weights:
        copy.start()

    def stage_firsts(head, carry):
        away = lax.rem(head - z + nz, nz)
        for d in range(NX):
            column = pl.multiple_of((xs[d] * nz + head) * hs, 128)
            piece = firsts[:, pl.ds(column, hs)]
            if d == 0:
                fv_own[away, x] = piece
            else:
                fv_stage[d - 1, away] = piece
        return carry

    lax.fori_loop(0, nz, stage_firsts, 0)
    for d in (1, 2, 3):
        remote(
            fv_stage.at[d - 1],
            fv_own.at[:, x],
            send_sem.at[2],
            fx_sem.at[d],
            tensor_0=xs[d],
        ).start()

    def length_of(way, s):
        return turns if (s % 2 == 0) == (way == 0) else turns - 1

    def gather_send(step):
        for s in range(subs):
            if step <= length_of(0, s):
                remote(
                    h_buf.at[(nz - step + 1) % nz, s],
                    h_buf.at[nz - step, s],
                    send_sem.at[3],
                    ag_sem.at[0, step - 1, s],
                    tensor_1=z_up,
                ).start()
            if step <= length_of(1, s):
                remote(
                    h_buf.at[step - 1, s],
                    h_buf.at[step, s],
                    send_sem.at[3],
                    ag_sem.at[1, step - 1, s],
                    tensor_1=z_down,
                ).start()

    def gather_step(step):
        for s in range(subs):
            if step <= length_of(0, s):
                arrived(h_buf.at[nz - step, s], ag_sem.at[0, step - 1, s])
            if step <= length_of(1, s):
                arrived(h_buf.at[step, s], ag_sem.at[1, step - 1, s])
            if step + 1 <= length_of(0, s):
                remote(
                    h_buf.at[nz - step, s],
                    h_buf.at[nz - step - 1, s],
                    send_sem.at[3],
                    ag_sem.at[0, step, s],
                    tensor_1=z_up,
                ).start()
            if step + 1 <= length_of(1, s):
                remote(
                    h_buf.at[step, s],
                    h_buf.at[step + 1, s],
                    send_sem.at[3],
                    ag_sem.at[1, step, s],
                    tensor_1=z_down,
                ).start()

    def half_columns(r):
        return w2.at[pl.ds(my_half, half), pl.ds(r * 3 * hs, 3 * hs)]

    def to_sibling(r):
        remote(
            half_columns(r), half_columns(r), send_sem.at[4], w_sem.at[4, r - 1], dp=1 - core
        ).start()

    def w_piece(r, p):
        return w2.at[pl.ds(my_half, half), pl.ds((r * 3 + p) * hs, hs)]

    def weights_relay():
        for p in range(3):
            arrived(w_relay.at[p], w_sem.at[0, p])
            remote(
                w_relay.at[p], w_piece(2, p), send_sem.at[5], w_sem.at[3, p], tensor_0=x_way
            ).start()

    def weights_direct():
        for r, sem in ((3, 1), (1, 2)):
            for p in range(3):
                arrived(w_piece(r, p), w_sem.at[sem, p])
            to_sibling(r)

    def weights_last():
        for p in range(3):
            arrived(w_piece(2, p), w_sem.at[3, p])
        to_sibling(2)
        for r in (1, 2, 3):
            other = pl.multiple_of((1 - core) * half, 128)
            arrived(
                w2.at[pl.ds(other, half), pl.ds(r * 3 * hs, 3 * hs)], w_sem.at[4, r - 1]
            )
        for copy in own_weights:
            copy.wait()

    for d in (1, 2, 3):
        for s in range(subs):
            arrived(h_buf.at[0, s, xs[d]], hid_sem.at[d, s])
    for copy in own_hidden:
        copy.wait()
    gather_send(1)
    early = max(turns - 3, 0)
    for step in range(1, early + 1):
        gather_step(step)
        if step == 2:
            weights_relay()
        if step == 4:
            weights_direct()
    if early < 2:
        weights_relay()
    if early < 4:
        weights_direct()
    weights_last()

    minus_turns = turns - 1

    def plus_at(step):
        return sum(turns + 1 - u for u in range(1, step))

    def minus_at(step):
        return sum(minus_turns + 1 - u for u in range(1, step))

    def firsts_step(step):
        if step == 0:
            for d in (1, 2, 3):
                arrived(fv_stage.at[d - 1], fx_sem.at[d])
            plus_src = fv_own.at[pl.ds(1, turns)]
            minus_src = fv_own.at[pl.ds(nz - minus_turns, minus_turns)]
        else:
            n_plus = turns + 1 - step
            arrived(fv_plus.at[pl.ds(plus_at(step), n_plus)], fz_sem.at[0, step - 1])
            plus_src = fv_plus.at[pl.ds(plus_at(step) + 1, n_plus - 1)] if n_plus > 1 else None
            n_minus = minus_turns + 1 - step
            minus_src = None
            if n_minus >= 1:
                arrived(fv_minus.at[pl.ds(minus_at(step), n_minus)], fz_sem.at[1, step - 1])
                if n_minus > 1:
                    minus_src = fv_minus.at[pl.ds(minus_at(step), n_minus - 1)]
        if plus_src is not None:
            remote(
                plus_src,
                fv_plus.at[pl.ds(plus_at(step + 1), turns - step)],
                send_sem.at[6],
                fz_sem.at[0, step],
                tensor_1=z_up,
            ).start()
        if minus_src is not None:
            remote(
                minus_src,
                fv_minus.at[pl.ds(minus_at(step + 1), minus_turns - step)],
                send_sem.at[7],
                fz_sem.at[1, step],
                tensor_1=z_down,
            ).start()

    width = 3 * hs
    low, high = pl.ds(0, block // 2), pl.ds(block // 2, block // 2)

    def place_of(i):
        return jnp.where(i % 2 == 1, (i + 1) // 2, lax.rem(nz - i // 2, nz))

    def project(i):
        place = place_of(i)
        lhs = jnp.concatenate(
            [h_buf[place, s].reshape(block, SUB) for s in range(subs)], axis=1
        )
        for r in (2, 1, 3, 0):
            term = jnp.dot(
                lhs, w2[:, r * width : (r + 1) * width], preferred_element_type=F32
            )
            if r == 2:
                a_send[i] = term.astype(BF)
                remote(
                    a_send.at[i, low],
                    a_recv.at[i, low],
                    send_sem.at[8],
                    a_sem.at[0, i],
                    tensor_0=xs[1],
                ).start()
                remote(
                    a_send.at[i, high],
                    a_recv.at[i, high],
                    send_sem.at[8],
                    a_sem.at[1, i],
                    tensor_0=xs[3],
                ).start()
            else:
                stash[i, r % 3 if r < 3 else 2] = term

    def pass_on(i):
        arrived(a_recv.at[i, low], a_sem.at[0, i])
        b_send[i, 0, low] = (stash[i, 1, low] + a_recv[i, low].astype(F32)).astype(BF)
        b_send[i, 0, high] = stash[i, 1, high].astype(BF)
        remote(
            b_send.at[i, 0], b_recv.at[i, 0], send_sem.at[9], b_sem.at[0, i], tensor_0=xs[1]
        ).start()
        arrived(a_recv.at[i, high], a_sem.at[1, i])
        b_send[i, 1, low] = stash[i, 2, low].astype(BF)
        b_send[i, 1, high] = (stash[i, 2, high] + a_recv[i, high].astype(F32)).astype(BF)
        remote(
            b_send.at[i, 1], b_recv.at[i, 1], send_sem.at[9], b_sem.at[1, i], tensor_0=xs[3]
        ).start()

    def finish(i):
        arrived(b_recv.at[i, 0], b_sem.at[0, i])
        arrived(b_recv.at[i, 1], b_sem.at[1, i])
        total = stash[i, 0] + b_recv[i, 0].astype(F32) + b_recv[i, 1].astype(F32)
        total = total.astype(BF).reshape(NX, rows, width)
        origin = lax.rem(z + place_of(i), nz)
        q_buf[:, origin] = total[:, :, :hs]
        k_buf[:, origin] = total[:, :, hs : 2 * hs]
        v_buf[:, origin] = total[:, :, 2 * hs :]

    def wo_columns(to):
        return pl.ds(pl.multiple_of(to * quarter + core * half, 128), half)

    def wo_piece(r):
        return wo2.at[pl.ds(r * hs, hs), pl.ds(my_half, half)]

    def out_weights_send():
        remote(
            w_out.at[:, wo_columns(xs[2])], wo_relay, send_sem.at[10], wo_sem.at[0], tensor_0=x_way
        ).start()
        for d, r, sem in ((1, 3, 1), (3, 1, 2)):
            remote(
                w_out.at[:, wo_columns(xs[d])],
                wo_piece(r),
                send_sem.at[10],
                wo_sem.at[sem],
                tensor_0=xs[d],
            ).start()

    def out_to_sibling(r):
        remote(
            wo_piece(r), wo_piece(r), send_sem.at[11], wo_sem.at[3 + r], dp=1 - core
        ).start()

    def out_weights_relay():
        arrived(wo_relay, wo_sem.at[0])
        remote(wo_relay, wo_piece(2), send_sem.at[12], wo_sem.at[3], tensor_0=x_way).start()

    def out_weights_direct():
        for r, sem in ((3, 1), (1, 2)):
            arrived(wo_piece(r), wo_sem.at[sem])
            out_to_sibling(r)

    def out_weights_last():
        arrived(wo_piece(2), wo_sem.at[3])
        out_to_sibling(2)

    def out_weights_wait():
        other = pl.multiple_of((1 - core) * half, 128)
        for r in (1, 2, 3):
            arrived(wo2.at[pl.ds(r * hs, hs), pl.ds(other, half)], wo_sem.at[3 + r])

    trips = nz + 2 * LAG
    late = {}
    for step in range(early + 1, turns + 1):
        late.setdefault(2 * (step - early) - 1, []).append(functools.partial(gather_step, step))
    for step in range(turns + 1):
        if 2 * step + 2 < trips:
            late.setdefault(2 * step + 2, []).append(functools.partial(firsts_step, step))

    def trip(i, carry):
        for at, steps in late.items():

            @pl.when(i == at)
            def _(steps=steps):
                for step in steps:
                    step()

        @pl.when(i < nz)
        def _():
            project(i)

        @pl.when((i >= LAG) & (i < nz + LAG))
        def _():
            pass_on(i - LAG)

        @pl.when(i == nz + LAG)
        def _():
            out_weights_send()

        @pl.when(i >= 2 * LAG)
        def _():
            finish(i - 2 * LAG)

        return carry

    lax.fori_loop(0, trips, trip, 0)
    for step in range(turns + 1):
        if 2 * step + 2 >= trips:
            firsts_step(step)

    row = mix_index[0]
    weight_now = mix_table[row, 0]
    weight_first = mix_table[row, 1]

    def mix(origin, first):
        now = v_buf[:, origin].astype(F32)
        v_buf[:, origin] = (weight_now * now + weight_first * first.astype(F32)).astype(BF)

    mix(z, fv_own[0])
    for step in range(1, turns + 1):
        mix(lax.rem(z + nz - step, nz), fv_plus[plus_at(step)])
    for step in range(1, minus_turns + 1):
        mix(lax.rem(z + step, nz), fv_minus[minus_at(step) + minus_turns - step])

    scale = 1.0 / math.sqrt(hs)
    valid = lengths[0]
    stripe = nz * rows
    q_blocks = min(nz, 128 // rows)
    q_rows = q_blocks * rows

    def attend(b):
        n = (b + 1) * stripe
        keys = k_buf[0 : b + 1].reshape(n, hs)
        values = v_buf[0 : b + 1].reshape(n, hs)

        def one(t, carry):
            at = pl.ds(t * q_blocks, q_blocks)
            query = q_buf[b, at].reshape(q_rows, hs)
            scores = (
                lax.dot_general(query, keys, (((1,), (1,)), ((), ())), preferred_element_type=F32)
                * scale
            )
            col = lax.broadcasted_iota(jnp.int32, (q_rows, n), 1)
            line = b * stripe + t * q_rows + lax.broadcasted_iota(jnp.int32, (q_rows, n), 0)
            scores = jnp.where((col <= line) & (col < valid), scores, NEG_FILL)
            raised = jnp.exp(scores - jnp.max(scores, axis=1, keepdims=True))
            weights = (raised * (1.0 / jnp.sum(raised, axis=1, keepdims=True))).astype(BF)
            result = jnp.dot(weights, values, preferred_element_type=F32).astype(BF)
            att[0, at, b] = result.reshape(q_blocks, rows, hs)
            return carry

        lax.fori_loop(0, nz // q_blocks, one, 0)

    near, far = pl.ds(0, nz // 2), pl.ds(nz // 2, nz // 2)

    def att_send(b):
        remote(
            att.at[0, :, b], att.at[3, :, b], send_sem.at[13], att_sem.at[0, b], tensor_0=xs[1]
        ).start()
        remote(
            att.at[0, :, b], att.at[1, :, b], send_sem.at[14], att_sem.at[1, b], tensor_0=xs[3]
        ).start()

    def att_pass(b):
        arrived(att.at[3, :, b], att_sem.at[0, b])
        remote(
            att.at[3, near, b], att.at[2, near, b], send_sem.at[15], att_sem.at[2, b], tensor_0=xs[1]
        ).start()
        arrived(att.at[1, :, b], att_sem.at[1, b])
        remote(
            att.at[1, far, b], att.at[2, far, b], send_sem.at[16], att_sem.at[3, b], tensor_0=xs[3]
        ).start()

    attend(0)
    att_send(0)
    out_weights_relay()
    attend(1)
    att_send(1)
    att_pass(0)
    attend(2)
    att_send(2)
    att_pass(1)
    out_weights_direct()
    attend(3)
    att_send(3)
    att_pass(2)
    out_weights_last()
    rs_recv[:, 0] = jnp.zeros(rs_recv.shape[:1] + rs_recv.shape[2:], BF)
    att_pass(3)
    out_weights_wait()
    for b in range(NX):
        arrived(att.at[2, near, b], att_sem.at[2, b])
        arrived(att.at[2, far, b], att_sem.at[3, b])

    def heads_of(away):
        origin = lax.rem(z + away + nz, nz)
        return jnp.concatenate([att[r, origin].reshape(block, hs) for r in range(NX)], axis=1)

    def columns(s):
        return wo2[:, s * SUB : (s + 1) * SUB]

    def reduce_step(step, carry):
        for s in range(subs):
            for way in (0, 1):
                length = length_of(way, s)
                sign = 1 - 2 * way

                @pl.when(step <= length)
                def _(s=s, way=way, length=length, sign=sign):
                    lhs = heads_of(sign * (length - step + 1))
                    term = jnp.dot(lhs, columns(s), preferred_element_type=F32)

                    @pl.when(step > 1)
                    def _():
                        arrived(rs_recv.at[way, step - 1, s], rs_sem.at[way, step - 1, s])

                    term = term + rs_recv[way, step - 1, s].astype(F32)
                    rs_send[step - 1, way, s] = term.astype(BF)
                    remote(
                        rs_send.at[step - 1, way, s],
                        rs_recv.at[way, step, s],
                        send_sem.at[17],
                        rs_sem.at[way, step, s],
                        tensor_1=z_up if way == 0 else z_down,
                    ).start()

        return carry

    lax.fori_loop(1, turns + 1, reduce_step, 0)
    own = heads_of(0)
    for s in range(subs):
        term = jnp.dot(own, columns(s), preferred_element_type=F32)
        for way in (0, 1):
            length = length_of(way, s)
            arrived(rs_recv.at[way, length, s], rs_sem.at[way, length, s])
            term = term + rs_recv[way, length, s].astype(F32)
        fin[s] = term.astype(BF).reshape(NX, rows, SUB)
        column = pl.multiple_of(x * quarter + s * SUB, 128)
        for d in (1, 2, 3):
            remote(
                fin.at[s, xs[d]],
                out_v.at[:, pl.ds(column, SUB)],
                send_sem.at[18],
                fin_sem.at[d, s],
                tensor_0=xs[d],
            ).start()
        out_v[:, pl.ds(column, SUB)] = fin[s, x]

    n_sub = turns * 2 - 1
    arrived(h_buf.at[pl.ds(0, 3), :, 0], send_sem.at[0])
    arrived(w2.at[:, pl.ds(0, 9 * hs)].at[pl.ds(0, half)], send_sem.at[1])
    arrived(fv_stage, send_sem.at[2])
    arrived(h_buf.at[pl.ds(0, n_sub)], send_sem.at[3])
    arrived(w2.at[pl.ds(0, half), pl.ds(0, 9 * hs)], send_sem.at[4])
    arrived(w_relay, send_sem.at[5])
    arrived(fv_plus, send_sem.at[6])
    arrived(fv_minus, send_sem.at[7])
    arrived(a_send, send_sem.at[8])
    arrived(b_send, send_sem.at[9])
    arrived(wo2.at[pl.ds(0, 3 * hs), pl.ds(0, half)], send_sem.at[10])
    arrived(wo2.at[pl.ds(0, 3 * hs), pl.ds(0, half)], send_sem.at[11])
    arrived(wo_relay, send_sem.at[12])
    arrived(att.at[0], send_sem.at[13])
    arrived(att.at[0], send_sem.at[14])
    arrived(att.at[0, near], send_sem.at[15])
    arrived(att.at[0, far], send_sem.at[16])
    for s in range(subs):
        for d in (1, 2, 3):
            column = pl.multiple_of(xs[d] * quarter + s * SUB, 128)
            column = pl.multiple_of(xs[NX - d] * quarter + s * SUB, 128)
            arrived(out_v.at[:, pl.ds(column, SUB)], fin_sem.at[d, s])
    arrived(h_buf.at[pl.ds(0, n_sub)], send_sem.at[17])
    arrived(fin.at[:, pl.ds(0, 3)], send_sem.at[18])
    out[...] = out_v[...]


def body(hidden_in, first_values, qkv_weight, out_weight, mix_table, mix_index, lengths, *, nz):
    rows, model = hidden_in.shape[1:]
    hs = qkv_weight.shape[2]
    quarter = model // NX
    half = quarter // 2
    subs = quarter // SUB
    turns = nz // 2
    block = NX * rows
    vmem = pl.BlockSpec(memory_space=pltpu.VMEM)
    smem = pl.BlockSpec(memory_space=pltpu.SMEM)
    anywhere = pl.BlockSpec(memory_space=pl.ANY)
    dma = pltpu.SemaphoreType.DMA
    scratch = [
        pltpu.VMEM((nz, subs, NX, rows, SUB), BF),
        pltpu.VMEM((quarter, NX * 3 * hs), BF),
        pltpu.VMEM((3, half, hs), BF),
        pltpu.VMEM((NX * hs, quarter), BF),
        pltpu.VMEM((hs, half), BF),
        pltpu.VMEM((NX - 1, nz, rows, hs), BF),
        pltpu.VMEM((nz, NX, rows, hs), BF),
        pltpu.VMEM((turns * (turns + 1) // 2, NX, rows, hs), BF),
        pltpu.VMEM((turns * (turns - 1) // 2, NX, rows, hs), BF),
        pltpu.VMEM((nz, 3, block, 3 * hs), F32),
        pltpu.VMEM((nz, block, 3 * hs), BF),
        pltpu.VMEM((nz, block, 3 * hs), BF),
        pltpu.VMEM((nz, 2, block, 3 * hs), BF),
        pltpu.VMEM((nz, 2, block, 3 * hs), BF),
        pltpu.VMEM((NX, nz, rows, hs), BF),
        pltpu.VMEM((NX, nz, rows, hs), BF),
        pltpu.VMEM((NX, nz, rows, hs), BF),
        pltpu.VMEM((NX, nz, NX, rows, hs), BF),
        pltpu.VMEM((turns, 2, subs, block, SUB), BF),
        pltpu.VMEM((2, turns + 1, subs, block, SUB), BF),
        pltpu.VMEM((subs, NX, rows, SUB), BF),
        pltpu.VMEM((rows, model), BF),
        dma((4,)),
        dma((19,)),
        dma((NX, subs)),
        dma((2, turns, subs)),
        dma((5, 3)),
        dma((7,)),
        dma((NX,)),
        dma((2, turns)),
        dma((2, nz)),
        dma((2, nz)),
        dma((4, NX)),
        dma((2, turns + 1, subs)),
        dma((NX, subs)),
    ]
    result = pl.pallas_call(
        functools.partial(kernel, nz),
        out_shape=jax.ShapeDtypeStruct((rows, model), BF),
        in_specs=[vmem, vmem, anywhere, anywhere, smem, smem, smem],
        out_specs=vmem,
        scratch_shapes=scratch,
        compiler_params=pltpu.CompilerParams(
            collective_id=0, has_side_effects=True, vmem_limit_bytes=60 * 1024 * 1024
        ),
    )(
        hidden_in[0],
        first_values[0],
        jnp.transpose(qkv_weight, (1, 0, 2)),
        out_weight,
        mix_table,
        mix_index,
        lengths,
    )
    return result[None]


def solution(mesh):
    nz = mesh.shape["tensor"] // NX
    torus = Mesh(
        mesh.devices.reshape(mesh.shape["groups"], mesh.shape["dp"], NX, nz),
        ("groups", "dp", "tensor_0", "tensor_1"),
    )
    placed = (
        P(("groups", "dp"), TENSOR, None),
        P(("groups", "dp"), TENSOR, None),
        P(None, None, TENSOR),
        P(TENSOR, None),
        P(),
        P(TENSOR),
        P(("groups", "dp")),
    )
    return jax.shard_map(
        functools.partial(body, nz=nz),
        mesh=torus,
        in_specs=placed,
        out_specs=P(("groups", "dp"), TENSOR, None),
        check_vma=False,
    )
```

```python
import functools
import math

import jax
import jax.numpy as jnp
from jax import lax
from jax.experimental import pallas as pl
from jax.experimental.pallas import tpu as pltpu
from jax.sharding import Mesh
from jax.sharding import PartitionSpec as P

TENSOR = ("tensor_0", "tensor_1")
NEG_FILL = -1e30
BF = jnp.bfloat16
F32 = jnp.float32
NX = 4
SUB = 256
LAG = 3


def kernel(
    nz,
    hid,
    firsts,
    w_qkv,
    w_out,
    mix_table,
    mix_index,
    lengths,
    out,
    x_wide,
    z_part,
    w2,
    wo2,
    wo_relay,
    fv_stage,
    fv_own,
    fv_plus,
    fv_minus,
    stash,
    b_send,
    b_recv,
    q_buf,
    k_buf,
    v_buf,
    att,
    rs_send,
    rs_recv,
    fin,
    out_v,
    local_sem,
    send_sem,
    own_sem,
    hid_sem,
    ag_sem,
    oz_sem,
    w_sem,
    wo_sem,
    fx_sem,
    fz_sem,
    b_sem,
    att_sem,
    rs_sem,
    fin_sem,
):
    rows, model = hid.shape
    hs = w_qkv.shape[2]
    quarter = model // NX
    half = quarter // 2
    halves = model // 2
    subs = quarter // SUB
    turns = nz // 2
    block = NX * rows

    x = lax.axis_index("tensor_0")
    z = lax.axis_index("tensor_1")
    core = lax.axis_index("dp")
    xs = [x] + [lax.rem(x + d, NX) for d in range(1, NX)]
    z_up = lax.rem(z + 1, nz)
    z_down = lax.rem(z + nz - 1, nz)
    x_way = lax.rem(x + 1 + 2 * core, NX)
    odd = lax.rem(x, 2)
    pair = x + 1 - 2 * odd
    other = lax.rem(x + NX - 1 + 2 * odd, NX)

    def remote(src, dst, send, recv, **where):
        return pltpu.make_async_remote_copy(
            src_ref=src,
            dst_ref=dst,
            send_sem=send,
            recv_sem=recv,
            device_id=where,
            device_id_type=pl.DeviceIdType.MESH,
        )

    def arrived(ref, sem):
        pltpu.make_async_copy(ref, ref, sem).wait()

    barrier = pltpu.get_barrier_semaphore()
    partners = [
        {"dp": 1 - core},
        {"tensor_0": xs[1]},
        {"tensor_0": xs[2]},
        {"tensor_0": xs[3]},
        {"tensor_1": z_up},
        {"tensor_1": z_down},
    ]
    for partner in partners:
        pl.semaphore_signal(
            barrier, inc=1, device_id=partner, device_id_type=pl.DeviceIdType.MESH
        )
    pl.semaphore_wait(barrier, len(partners))

    def half_of(at):
        return lax.rem((at + 1) // 2, 2)

    mine, theirs = half_of(x), 1 - half_of(x)
    stripes, other_stripes = pl.ds(x - odd, 2), pl.ds(NX - 2 - x + odd, 2)
    x_subs, z_subs, z_wide = x_wide.shape[1], z_part.shape[1], z_part.shape[4]

    def x_columns(to_half, s):
        return pl.ds(pl.multiple_of(to_half * halves + s * SUB, 128), SUB)

    def z_columns(to_half, s):
        return pl.ds(pl.multiple_of(to_half * halves + x_subs * SUB + s * z_wide, 128), z_wide)

    def hidden_out(d, to, to_half):
        for s in range(x_subs):
            remote(
                hid.at[:, x_columns(to_half, s)],
                x_wide.at[0, s, x],
                send_sem.at[0],
                hid_sem.at[d, s],
                tensor_0=to,
            ).start()

    for s in range(z_subs):
        remote(
            hid.at[:, z_columns(theirs, s)],
            z_part.at[0, s, x],
            send_sem.at[1],
            hid_sem.at[0, s],
            tensor_0=pair,
        ).start()
    hidden_out(1, pair, theirs)
    hidden_out(2, other, mine)
    hidden_out(3, xs[2], theirs)
    own_hidden = []
    for s in range(z_subs):
        own_hidden.append(
            pltpu.make_async_copy(
                hid.at[:, z_columns(mine, s)], z_part.at[0, s, x], own_sem.at[s]
            )
        )
    for s in range(x_subs):
        own_hidden.append(
            pltpu.make_async_copy(
                hid.at[:, x_columns(mine, s)], x_wide.at[0, s, x], own_sem.at[z_subs + s]
            )
        )
    for copy in own_hidden:
        copy.start()

    def stage_firsts(head, carry):
        away = lax.rem(head - z + nz, nz)
        for d in range(NX):
            column = pl.multiple_of((xs[d] * nz + head) * hs, 128)
            piece = firsts[:, pl.ds(column, hs)]
            if d == 0:
                fv_own[away, x] = piece
            else:
                fv_stage[d - 1, away] = piece
        return carry

    lax.fori_loop(0, nz, stage_firsts, 0)
    for d in (1, 2, 3):
        remote(
            fv_stage.at[d - 1],
            fv_own.at[:, x],
            send_sem.at[2],
            fx_sem.at[d],
            tensor_0=xs[d],
        ).start()

    share = halves // 2
    my_share = pl.multiple_of(core * share, 128)
    sibling_share = pl.multiple_of((1 - core) * share, 128)
    for p in range(3):
        remote(
            w_qkv.at[p, pl.ds(pl.multiple_of(theirs * halves + core * share, 128), share)],
            w2.at[pl.ds(my_share, share), pl.ds((3 + p) * hs, hs)],
            send_sem.at[4],
            w_sem.at[0, p],
            tensor_0=pair,
        ).start()
    own_weights = []
    for p in range(3):
        own_weights.append(
            pltpu.make_async_copy(
                w_qkv.at[p, pl.ds(pl.multiple_of(mine * halves, 128), halves)],
                w2.at[:, pl.ds(p * hs, hs)],
                local_sem.at[p],
            )
        )
    own_weights.append(
        pltpu.make_async_copy(
            w_out.at[:, pl.ds(pl.multiple_of(x * quarter, 128), quarter)],
            wo2.at[pl.ds(0, hs)],
            local_sem.at[3],
        )
    )
    for copy in own_weights:
        copy.start()

    flows = [(0, s) for s in range(x_subs)] + [(1, s) for s in range(z_subs)]

    def longer(way, n):
        return turns if (n % 2 == 0) == (way == 0) else turns - 1

    def part(n, place):
        kind, s = flows[n]
        return x_wide.at[place, s] if kind == 0 else z_part.at[place, s, stripes]

    def ring_send(n, way, step):
        source, target = (step - 1, step) if way else ((nz - step + 1) % nz, nz - step)
        remote(
            part(n, source),
            part(n, target),
            send_sem.at[3 if flows[n][0] == 0 else 5],
            ag_sem.at[way, step - 1, n],
            tensor_1=z_down if way else z_up,
        ).start()

    def to_other(n, place):
        kind, s = flows[n]
        if kind == 1:
            remote(
                z_part.at[place, s, stripes],
                z_part.at[place, s, stripes],
                send_sem.at[6],
                oz_sem.at[place, s],
                tensor_0=other,
            ).start()

    def gather_step(step):
        for n in range(len(flows)):
            for way in (0, 1):
                if step <= longer(way, n):
                    place = step if way else nz - step
                    arrived(part(n, place), ag_sem.at[way, step - 1, n])
                    if step + 1 <= longer(way, n):
                        ring_send(n, way, step + 1)
                    to_other(n, place)

    def weights_step(p):
        here = w2.at[pl.ds(my_share, share), pl.ds((3 + p) * hs, hs)]
        arrived(here, w_sem.at[0, p])
        remote(here, here, send_sem.at[7], w_sem.at[1, p], dp=1 - core).start()

    def weights_last():
        for p in range(3):
            arrived(
                w2.at[pl.ds(sibling_share, share), pl.ds((3 + p) * hs, hs)], w_sem.at[1, p]
            )
        for copy in own_weights:
            copy.wait()

    minus_turns = turns - 1

    def plus_at(step):
        return sum(turns + 1 - u for u in range(1, step))

    def minus_at(step):
        return sum(minus_turns + 1 - u for u in range(1, step))

    def firsts_step(step):
        if step == 0:
            for d in (1, 2, 3):
                arrived(fv_stage.at[d - 1], fx_sem.at[d])
            plus_src = fv_own.at[pl.ds(1, turns)]
            minus_src = fv_own.at[pl.ds(nz - minus_turns, minus_turns)]
        else:
            n_plus = turns + 1 - step
            arrived(fv_plus.at[pl.ds(plus_at(step), n_plus)], fz_sem.at[0, step - 1])
            plus_src = fv_plus.at[pl.ds(plus_at(step) + 1, n_plus - 1)] if n_plus > 1 else None
            n_minus = minus_turns + 1 - step
            minus_src = None
            if n_minus >= 1:
                arrived(fv_minus.at[pl.ds(minus_at(step), n_minus)], fz_sem.at[1, step - 1])
                if n_minus > 1:
                    minus_src = fv_minus.at[pl.ds(minus_at(step), n_minus - 1)]
        if plus_src is not None:
            remote(
                plus_src,
                fv_plus.at[pl.ds(plus_at(step + 1), turns - step)],
                send_sem.at[8],
                fz_sem.at[0, step],
                tensor_1=z_up,
            ).start()
        if minus_src is not None:
            remote(
                minus_src,
                fv_minus.at[pl.ds(minus_at(step + 1), minus_turns - step)],
                send_sem.at[9],
                fz_sem.at[1, step],
                tensor_1=z_down,
            ).start()

    for copy in own_hidden:
        copy.wait()
    for s in range(z_subs):
        arrived(z_part.at[0, s, pair], hid_sem.at[0, s])
        ring_send(x_subs + s, 0, 1)
        ring_send(x_subs + s, 1, 1)
        to_other(x_subs + s, 0)
    for s in range(x_subs):
        for d in (1, 2, 3):
            arrived(x_wide.at[0, s, x], hid_sem.at[d, s])
        ring_send(s, 0, 1)
        ring_send(s, 1, 1)
    early = max(turns - 3, 0)
    weights_after = {2: (0,), 3: (1,)}
    for step in range(1, early + 1):
        gather_step(step)
        firsts_step(step - 1)
        for p in weights_after.get(step, ()):
            weights_step(p)
    for p in range(3):
        if not any(p in done for step, done in weights_after.items() if step <= early):
            weights_step(p)
    weights_last()

    width = 3 * hs

    def place_of(i):
        return jnp.where(i % 2 == 1, (i + 1) // 2, lax.rem(nz - i // 2, nz))

    def project(i):
        place = place_of(i)
        for s in range(z_subs):
            arrived(z_part.at[place, s, other_stripes], oz_sem.at[place, s])
        lhs = jnp.concatenate(
            [x_wide[place, s].reshape(block, SUB) for s in range(x_subs)]
            + [z_part[place, s].reshape(block, z_wide) for s in range(z_subs)],
            axis=1,
        )
        term = jnp.dot(lhs, w2[...], preferred_element_type=F32)
        b_send[i] = term[:, width:].astype(BF)
        remote(
            b_send.at[i], b_recv.at[i], send_sem.at[10], b_sem.at[i], tensor_0=pair
        ).start()
        stash[i] = term[:, :width]

    def finish(i):
        arrived(b_recv.at[i], b_sem.at[i])
        total = stash[i] + b_recv[i].astype(F32)
        total = total.astype(BF).reshape(NX, rows, width)
        origin = lax.rem(z + place_of(i), nz)
        q_buf[:, origin] = total[:, :, :hs]
        k_buf[:, origin] = total[:, :, hs : 2 * hs]
        v_buf[:, origin] = total[:, :, 2 * hs :]

    my_half = pl.multiple_of(core * half, 128)

    def wo_columns(to):
        return pl.ds(pl.multiple_of(to * quarter + core * half, 128), half)

    def wo_piece(r):
        return wo2.at[pl.ds(r * hs, hs), pl.ds(my_half, half)]

    def out_weights_send():
        remote(
            w_out.at[:, wo_columns(xs[2])], wo_relay, send_sem.at[11], wo_sem.at[0], tensor_0=x_way
        ).start()
        for d, r, sem in ((1, 3, 1), (3, 1, 2)):
            remote(
                w_out.at[:, wo_columns(xs[d])],
                wo_piece(r),
                send_sem.at[11],
                wo_sem.at[sem],
                tensor_0=xs[d],
            ).start()

    def out_to_sibling(r):
        remote(
            wo_piece(r), wo_piece(r), send_sem.at[12], wo_sem.at[3 + r], dp=1 - core
        ).start()

    def out_weights_relay():
        arrived(wo_relay, wo_sem.at[0])
        remote(wo_relay, wo_piece(2), send_sem.at[13], wo_sem.at[3], tensor_0=x_way).start()

    def out_weights_direct():
        for r, sem in ((3, 1), (1, 2)):
            arrived(wo_piece(r), wo_sem.at[sem])
            out_to_sibling(r)

    def out_weights_last():
        arrived(wo_piece(2), wo_sem.at[3])
        out_to_sibling(2)

    def out_weights_wait():
        other = pl.multiple_of((1 - core) * half, 128)
        for r in (1, 2, 3):
            arrived(wo2.at[pl.ds(r * hs, hs), pl.ds(other, half)], wo_sem.at[3 + r])

    trips = nz + LAG
    late = {}
    for step in range(early + 1, turns + 1):
        at = min(2 * step - 1, 4 * (step - early) + 1)
        late.setdefault(at, []).append(functools.partial(gather_step, step))
    after_loop = []
    for step in range(early, turns + 1):
        at = 3 + 4 * (step - early)
        if at < trips:
            late.setdefault(at, []).append(functools.partial(firsts_step, step))
        else:
            after_loop.append(step)

    def trip(i, carry):
        for at, steps in late.items():

            @pl.when(i == at)
            def _(steps=steps):
                for step in steps:
                    step()

        @pl.when(i < nz)
        def _():
            project(i)

        @pl.when(i == nz)
        def _():
            out_weights_send()

        @pl.when(i >= LAG)
        def _():
            finish(i - LAG)

        return carry

    lax.fori_loop(0, trips, trip, 0)
    for step in after_loop:
        firsts_step(step)

    row = mix_index[0]
    weight_now = mix_table[0, row]
    weight_first = mix_table[1, row]

    def mix(origin, first):
        now = v_buf[:, origin].astype(F32)
        v_buf[:, origin] = (weight_now * now + weight_first * first.astype(F32)).astype(BF)

    mix(z, fv_own[0])
    for step in range(1, turns + 1):
        mix(lax.rem(z + nz - step, nz), fv_plus[plus_at(step)])
    for step in range(1, minus_turns + 1):
        mix(lax.rem(z + step, nz), fv_minus[minus_at(step) + minus_turns - step])

    scale = 1.0 / math.sqrt(hs)
    valid = lengths[0]
    stripe = nz * rows
    q_blocks = min(nz, 128 // rows)
    q_rows = q_blocks * rows

    def attend(b):
        n = (b + 1) * stripe
        keys = k_buf[0 : b + 1].reshape(n, hs)
        values = v_buf[0 : b + 1].reshape(n, hs)

        def one(t, carry):
            at = pl.ds(t * q_blocks, q_blocks)
            query = q_buf[b, at].reshape(q_rows, hs)
            scores = (
                lax.dot_general(query, keys, (((1,), (1,)), ((), ())), preferred_element_type=F32)
                * scale
            )
            col = lax.broadcasted_iota(jnp.int32, (q_rows, n), 1)
            line = b * stripe + t * q_rows + lax.broadcasted_iota(jnp.int32, (q_rows, n), 0)
            scores = jnp.where((col <= line) & (col < valid), scores, NEG_FILL)
            raised = jnp.exp(scores - jnp.max(scores, axis=1, keepdims=True))
            weights = (raised * (1.0 / jnp.sum(raised, axis=1, keepdims=True))).astype(BF)
            result = jnp.dot(weights, values, preferred_element_type=F32).astype(BF)
            att[0, at, b] = result.reshape(q_blocks, rows, hs)
            return carry

        lax.fori_loop(0, nz // q_blocks, one, 0)

    near, far = pl.ds(0, nz // 2), pl.ds(nz // 2, nz // 2)

    def att_send(b):
        remote(
            att.at[0, :, b], att.at[3, :, b], send_sem.at[14], att_sem.at[0, b], tensor_0=xs[1]
        ).start()
        remote(
            att.at[0, :, b], att.at[1, :, b], send_sem.at[15], att_sem.at[1, b], tensor_0=xs[3]
        ).start()

    def att_pass(b):
        arrived(att.at[3, :, b], att_sem.at[0, b])
        remote(
            att.at[3, near, b], att.at[2, near, b], send_sem.at[16], att_sem.at[2, b], tensor_0=xs[1]
        ).start()
        arrived(att.at[1, :, b], att_sem.at[1, b])
        remote(
            att.at[1, far, b], att.at[2, far, b], send_sem.at[17], att_sem.at[3, b], tensor_0=xs[3]
        ).start()

    attend(0)
    att_send(0)
    out_weights_relay()
    attend(1)
    att_send(1)
    att_pass(0)
    attend(2)
    att_send(2)
    att_pass(1)
    out_weights_direct()
    attend(3)
    att_send(3)
    att_pass(2)
    out_weights_last()
    rs_recv[:, 0] = jnp.zeros(rs_recv.shape[:1] + rs_recv.shape[2:], BF)
    att_pass(3)
    out_weights_wait()
    for b in range(NX):
        arrived(att.at[2, near, b], att_sem.at[2, b])
        arrived(att.at[2, far, b], att_sem.at[3, b])

    def length_of(way, s):
        return turns if (s % 2 == 0) == (way == 0) else turns - 1

    def heads_of(away):
        origin = lax.rem(z + away + nz, nz)
        return jnp.concatenate([att[r, origin].reshape(block, hs) for r in range(NX)], axis=1)

    def columns(s):
        return wo2[:, s * SUB : (s + 1) * SUB]

    def reduce_step(step, carry):
        for s in range(subs):
            for way in (0, 1):
                length = length_of(way, s)
                sign = 1 - 2 * way

                @pl.when(step <= length)
                def _(s=s, way=way, length=length, sign=sign):
                    lhs = heads_of(sign * (length - step + 1))
                    term = jnp.dot(lhs, columns(s), preferred_element_type=F32)

                    @pl.when(step > 1)
                    def _():
                        arrived(rs_recv.at[way, step - 1, s], rs_sem.at[way, step - 1, s])

                    term = term + rs_recv[way, step - 1, s].astype(F32)
                    rs_send[2 * step - 2 + way, s] = term.astype(BF)
                    remote(
                        rs_send.at[2 * step - 2 + way, s],
                        rs_recv.at[way, step, s],
                        send_sem.at[18],
                        rs_sem.at[way, step, s],
                        tensor_1=z_up if way == 0 else z_down,
                    ).start()

        return carry

    lax.fori_loop(1, turns + 1, reduce_step, 0)
    own = heads_of(0)
    for s in range(subs):
        term = jnp.dot(own, columns(s), preferred_element_type=F32)
        for way in (0, 1):
            length = length_of(way, s)
            arrived(rs_recv.at[way, length, s], rs_sem.at[way, length, s])
            term = term + rs_recv[way, length, s].astype(F32)
        fin[s] = term.astype(BF).reshape(NX, rows, SUB)
        column = pl.multiple_of(x * quarter + s * SUB, 128)
        for d in (1, 2, 3):
            remote(
                fin.at[s, xs[d]],
                out_v.at[:, pl.ds(column, SUB)],
                send_sem.at[19],
                fin_sem.at[d, s],
                tensor_0=xs[d],
            ).start()
        out_v[:, pl.ds(column, SUB)] = fin[s, x]

    n_ring = turns * 2 - 1
    arrived(x_wide.at[pl.ds(0, 3), :, 0], send_sem.at[0])
    arrived(z_part.at[0, :, 0], send_sem.at[1])
    arrived(fv_stage, send_sem.at[2])
    arrived(x_wide.at[pl.ds(0, n_ring)], send_sem.at[3])
    arrived(w2.at[pl.ds(0, share), pl.ds(0, width)], send_sem.at[4])
    arrived(z_part.at[pl.ds(0, n_ring), :, pl.ds(0, 2)], send_sem.at[5])
    arrived(z_part.at[:, :, pl.ds(0, 2)], send_sem.at[6])
    arrived(w2.at[pl.ds(0, share), pl.ds(0, width)], send_sem.at[7])
    arrived(fv_plus, send_sem.at[8])
    arrived(fv_minus, send_sem.at[9])
    arrived(b_send, send_sem.at[10])
    arrived(wo2.at[pl.ds(0, 3 * hs), pl.ds(0, half)], send_sem.at[11])
    arrived(wo2.at[pl.ds(0, 3 * hs), pl.ds(0, half)], send_sem.at[12])
    arrived(wo_relay, send_sem.at[13])
    arrived(att.at[0], send_sem.at[14])
    arrived(att.at[0], send_sem.at[15])
    arrived(att.at[0, near], send_sem.at[16])
    arrived(att.at[0, far], send_sem.at[17])
    for s in range(subs):
        for d in (1, 2, 3):
            column = pl.multiple_of(xs[NX - d] * quarter + s * SUB, 128)
            arrived(out_v.at[:, pl.ds(column, SUB)], fin_sem.at[d, s])
    arrived(rs_send.at[pl.ds(0, n_ring)], send_sem.at[18])
    arrived(fin.at[:, pl.ds(0, 3)], send_sem.at[19])
    out[...] = out_v[...]


def body(hidden_in, first_values, qkv_weight, out_weight, mix_table, mix_index, lengths, *, nz):
    rows, model = hidden_in.shape[1:]
    hs = qkv_weight.shape[2]
    quarter = model // NX
    half = quarter // 2
    halves = model // 2
    subs = quarter // SUB
    x_subs = max(1, halves * 3 // 10 // SUB)
    z_subs = 2
    z_wide = (halves - x_subs * SUB) // z_subs
    turns = nz // 2
    block = NX * rows
    vmem = pl.BlockSpec(memory_space=pltpu.VMEM)
    smem = pl.BlockSpec(memory_space=pltpu.SMEM)
    anywhere = pl.BlockSpec(memory_space=pl.ANY)
    dma = pltpu.SemaphoreType.DMA
    scratch = [
        pltpu.VMEM((nz, x_subs, NX, rows, SUB), BF),
        pltpu.VMEM((nz, z_subs, NX, rows, z_wide), BF),
        pltpu.VMEM((halves, 2 * 3 * hs), BF),
        pltpu.VMEM((NX * hs, quarter), BF),
        pltpu.VMEM((hs, half), BF),
        pltpu.VMEM((NX - 1, nz, rows, hs), BF),
        pltpu.VMEM((nz, NX, rows, hs), BF),
        pltpu.VMEM((turns * (turns + 1) // 2, NX, rows, hs), BF),
        pltpu.VMEM((turns * (turns - 1) // 2, NX, rows, hs), BF),
        pltpu.VMEM((nz, block, 3 * hs), F32),
        pltpu.VMEM((nz, block, 3 * hs), BF),
        pltpu.VMEM((nz, block, 3 * hs), BF),
        pltpu.VMEM((NX, nz, rows, hs), BF),
        pltpu.VMEM((NX, nz, rows, hs), BF),
        pltpu.VMEM((NX, nz, rows, hs), BF),
        pltpu.VMEM((NX, nz, NX, rows, hs), BF),
        pltpu.VMEM((2 * turns, subs, block, SUB), BF),
        pltpu.VMEM((2, turns + 1, subs, block, SUB), BF),
        pltpu.VMEM((subs, NX, rows, SUB), BF),
        pltpu.VMEM((rows, model), BF),
        dma((4,)),
        dma((20,)),
        dma((x_subs + z_subs,)),
        dma((NX, x_subs + z_subs)),
        dma((2, turns, x_subs + z_subs)),
        dma((nz, z_subs)),
        dma((2, 3)),
        dma((7,)),
        dma((NX,)),
        dma((2, turns)),
        dma((nz,)),
        dma((4, NX)),
        dma((2, turns + 1, subs)),
        dma((NX, subs)),
    ]
    result = pl.pallas_call(
        functools.partial(kernel, nz),
        out_shape=jax.ShapeDtypeStruct((rows, model), BF),
        in_specs=[vmem, vmem, anywhere, anywhere, smem, smem, smem],
        out_specs=vmem,
        scratch_shapes=scratch,
        compiler_params=pltpu.CompilerParams(
            collective_id=0, has_side_effects=True, vmem_limit_bytes=60 * 1024 * 1024
        ),
    )(
        hidden_in[0],
        first_values[0],
        jnp.transpose(qkv_weight, (1, 0, 2)),
        out_weight,
        mix_table.T,
        mix_index,
        lengths,
    )
    return result[None]


def solution(mesh):
    nz = mesh.shape["tensor"] // NX
    torus = Mesh(
        mesh.devices.reshape(mesh.shape["groups"], mesh.shape["dp"], NX, nz),
        ("groups", "dp", "tensor_0", "tensor_1"),
    )
    placed = (
        P(("groups", "dp"), TENSOR, None),
        P(("groups", "dp"), TENSOR, None),
        P(None, None, TENSOR),
        P(TENSOR, None),
        P(),
        P(TENSOR),
        P(("groups", "dp")),
    )
    return jax.shard_map(
        functools.partial(body, nz=nz),
        mesh=torus,
        in_specs=placed,
        out_specs=P(("groups", "dp"), TENSOR, None),
        check_vma=False,
    )
```

```python
import functools
import math

import jax
import jax.numpy as jnp
from jax import lax
from jax.experimental import pallas as pl
from jax.experimental.pallas import tpu as pltpu
from jax.sharding import Mesh
from jax.sharding import PartitionSpec as P

TENSOR = ("tensor_0", "tensor_1")
NEG_FILL = -1e30
BF = jnp.bfloat16
F32 = jnp.float32
NX = 4
SUB = 256
LAG = 3


def kernel(
    nz,
    hid,
    firsts,
    w_qkv,
    w_out,
    mix_table,
    mix_index,
    lengths,
    out,
    x_wide,
    z_part,
    w2,
    wo2,
    wo_relay,
    fv_stage,
    fv_own,
    fv_in,
    stash,
    b_send,
    b_recv,
    q_buf,
    k_buf,
    v_buf,
    att,
    rs_send,
    rs_recv,
    fin,
    local_sem,
    send_sem,
    own_sem,
    hid_sem,
    ag_sem,
    oz_sem,
    w_sem,
    wo_sem,
    fx_sem,
    fz_sem,
    b_sem,
    att_sem,
    rs_sem,
    fin_sem,
):
    rows, model = hid.shape
    hs = w_qkv.shape[2]
    quarter = model // NX
    half = quarter // 2
    halves = model // 2
    subs = quarter // SUB
    turns = nz // 2
    block = NX * rows

    x = lax.axis_index("tensor_0")
    z = lax.axis_index("tensor_1")
    core = lax.axis_index("dp")
    xs = [x] + [lax.rem(x + d, NX) for d in range(1, NX)]
    z_up = lax.rem(z + 1, nz)
    z_down = lax.rem(z + nz - 1, nz)
    x_way = lax.rem(x + 1 + 2 * core, NX)
    odd = lax.rem(x, 2)
    pair = x + 1 - 2 * odd
    other = lax.rem(x + NX - 1 + 2 * odd, NX)

    def remote(src, dst, send, recv, **where):
        return pltpu.make_async_remote_copy(
            src_ref=src,
            dst_ref=dst,
            send_sem=send,
            recv_sem=recv,
            device_id=where,
            device_id_type=pl.DeviceIdType.MESH,
        )

    def arrived(ref, sem):
        pltpu.make_async_copy(ref, ref, sem).wait()

    barrier = pltpu.get_barrier_semaphore()
    partners = [
        {"dp": 1 - core},
        {"tensor_0": xs[1]},
        {"tensor_0": xs[2]},
        {"tensor_0": xs[3]},
        {"tensor_1": z_up},
        {"tensor_1": z_down},
    ]
    for partner in partners:
        pl.semaphore_signal(
            barrier, inc=1, device_id=partner, device_id_type=pl.DeviceIdType.MESH
        )
    pl.semaphore_wait(barrier, len(partners))

    def half_of(at):
        return lax.rem((at + 1) // 2, 2)

    mine, theirs = half_of(x), 1 - half_of(x)
    stripes, other_stripes = pl.ds(x - odd, 2), pl.ds(NX - 2 - x + odd, 2)
    x_subs, z_subs, z_wide = x_wide.shape[1], z_part.shape[1], z_part.shape[4]

    def x_columns(to_half, s):
        return pl.ds(pl.multiple_of(to_half * halves + s * SUB, 128), SUB)

    def z_columns(to_half, s):
        return pl.ds(pl.multiple_of(to_half * halves + x_subs * SUB + s * z_wide, 128), z_wide)

    def hidden_out(d, to, to_half):
        for s in range(x_subs):
            remote(
                hid.at[:, x_columns(to_half, s)],
                x_wide.at[0, s, x],
                send_sem.at[0],
                hid_sem.at[d, s],
                tensor_0=to,
            ).start()

    for s in range(z_subs):
        remote(
            hid.at[:, z_columns(theirs, s)],
            z_part.at[0, s, x],
            send_sem.at[1],
            hid_sem.at[0, s],
            tensor_0=pair,
        ).start()
    hidden_out(1, pair, theirs)
    hidden_out(2, other, mine)
    hidden_out(3, xs[2], theirs)
    own_hidden = []
    for s in range(z_subs):
        own_hidden.append(
            pltpu.make_async_copy(
                hid.at[:, z_columns(mine, s)], z_part.at[0, s, x], own_sem.at[s]
            )
        )
    for s in range(x_subs):
        own_hidden.append(
            pltpu.make_async_copy(
                hid.at[:, x_columns(mine, s)], x_wide.at[0, s, x], own_sem.at[z_subs + s]
            )
        )
    for copy in own_hidden:
        copy.start()

    def stage_firsts(head, carry):
        away = lax.rem(head - z + nz, nz)
        for d in range(NX):
            column = pl.multiple_of((xs[d] * nz + head) * hs, 128)
            piece = firsts[:, pl.ds(column, hs)]
            if d == 0:
                fv_own[away, x] = piece
            else:
                fv_stage[d - 1, away] = piece
        return carry

    lax.fori_loop(0, nz, stage_firsts, 0)
    for d in (1, 2, 3):
        remote(
            fv_stage.at[d - 1],
            fv_own.at[:, x],
            send_sem.at[2],
            fx_sem.at[d],
            tensor_0=xs[d],
        ).start()

    share = halves // 2
    my_share = pl.multiple_of(core * share, 128)
    sibling_share = pl.multiple_of((1 - core) * share, 128)
    for p in range(3):
        remote(
            w_qkv.at[p, pl.ds(pl.multiple_of(theirs * halves + core * share, 128), share)],
            w2.at[pl.ds(my_share, share), pl.ds((3 + p) * hs, hs)],
            send_sem.at[4],
            w_sem.at[0, p],
            tensor_0=pair,
        ).start()
    own_weights = []
    for p in range(3):
        own_weights.append(
            pltpu.make_async_copy(
                w_qkv.at[p, pl.ds(pl.multiple_of(mine * halves, 128), halves)],
                w2.at[:, pl.ds(p * hs, hs)],
                local_sem.at[p],
            )
        )
    own_weights.append(
        pltpu.make_async_copy(
            w_out.at[:, pl.ds(pl.multiple_of(x * quarter, 128), quarter)],
            wo2.at[pl.ds(0, hs)],
            local_sem.at[3],
        )
    )
    for copy in own_weights:
        copy.start()

    my_half = pl.multiple_of(core * half, 128)

    def wo_columns(to):
        return pl.ds(pl.multiple_of(to * quarter + core * half, 128), half)

    def wo_piece(r):
        return wo2.at[pl.ds(r * hs, hs), pl.ds(my_half, half)]

    def out_weights_send():
        remote(
            w_out.at[:, wo_columns(xs[2])], wo_relay, send_sem.at[11], wo_sem.at[0], tensor_0=x_way
        ).start()
        for d, r, sem in ((1, 3, 1), (3, 1, 2)):
            remote(
                w_out.at[:, wo_columns(xs[d])],
                wo_piece(r),
                send_sem.at[11],
                wo_sem.at[sem],
                tensor_0=xs[d],
            ).start()

    def out_to_sibling(r):
        remote(
            wo_piece(r), wo_piece(r), send_sem.at[12], wo_sem.at[3 + r], dp=1 - core
        ).start()

    def out_weights_relay():
        arrived(wo_relay, wo_sem.at[0])
        remote(wo_relay, wo_piece(2), send_sem.at[13], wo_sem.at[3], tensor_0=x_way).start()

    def out_weights_direct():
        for r, sem in ((3, 1), (1, 2)):
            arrived(wo_piece(r), wo_sem.at[sem])
            out_to_sibling(r)

    def out_weights_last():
        arrived(wo_piece(2), wo_sem.at[3])
        out_to_sibling(2)

    def out_weights_wait():
        other = pl.multiple_of((1 - core) * half, 128)
        for r in (1, 2, 3):
            arrived(wo2.at[pl.ds(r * hs, hs), pl.ds(other, half)], wo_sem.at[3 + r])

    out_weights_send()

    flows = [(0, s) for s in range(x_subs)] + [(1, s) for s in range(z_subs)]

    def longer(way, n):
        return turns if (n % 2 == 0) == (way == 0) else turns - 1

    def part(n, place):
        kind, s = flows[n]
        return x_wide.at[place, s] if kind == 0 else z_part.at[place, s, stripes]

    def ring_send(n, way, step):
        source, target = (step - 1, step) if way else ((nz - step + 1) % nz, nz - step)
        remote(
            part(n, source),
            part(n, target),
            send_sem.at[3 if flows[n][0] == 0 else 5],
            ag_sem.at[way, step - 1, n],
            tensor_1=z_down if way else z_up,
        ).start()

    def to_other(n, place):
        kind, s = flows[n]
        if kind == 1:
            remote(
                z_part.at[place, s, stripes],
                z_part.at[place, s, stripes],
                send_sem.at[6],
                oz_sem.at[place, s],
                tensor_0=other,
            ).start()

    def gather_step(step):
        for n in range(len(flows)):
            for way in (0, 1):
                if step <= longer(way, n):
                    place = step if way else nz - step
                    arrived(part(n, place), ag_sem.at[way, step - 1, n])
                    if step + 1 <= longer(way, n):
                        ring_send(n, way, step + 1)
                    to_other(n, place)

    def weights_step(p):
        here = w2.at[pl.ds(my_share, share), pl.ds((3 + p) * hs, hs)]
        arrived(here, w_sem.at[0, p])
        remote(here, here, send_sem.at[7], w_sem.at[1, p], dp=1 - core).start()

    def weights_last():
        for p in range(3):
            arrived(
                w2.at[pl.ds(sibling_share, share), pl.ds((3 + p) * hs, hs)], w_sem.at[1, p]
            )
        for copy in own_weights:
            copy.wait()

    def firsts_step(step):
        if step == 1:
            for d in (1, 2, 3):
                arrived(fv_stage.at[d - 1], fx_sem.at[d])
        for away in sorted({step, nz - step}):
            remote(
                fv_own.at[away],
                fv_in.at[nz - away],
                send_sem.at[8],
                fz_sem.at[nz - away],
                tensor_1=lax.rem(z + away, nz),
            ).start()

    for copy in own_hidden:
        copy.wait()
    for s in range(z_subs):
        arrived(z_part.at[0, s, pair], hid_sem.at[0, s])
        ring_send(x_subs + s, 0, 1)
        ring_send(x_subs + s, 1, 1)
        to_other(x_subs + s, 0)
    for s in range(x_subs):
        for d in (1, 2, 3):
            arrived(x_wide.at[0, s, x], hid_sem.at[d, s])
        ring_send(s, 0, 1)
        ring_send(s, 1, 1)
    early = max(turns - 4, 0)
    weights_after = {2: (0,), 3: (1,)}
    for step in range(1, early + 1):
        gather_step(step)
        firsts_step(step)
        for p in weights_after.get(step, ()):
            weights_step(p)
    for p in range(3):
        if not any(p in done for step, done in weights_after.items() if step <= early):
            weights_step(p)
    weights_last()

    width = 3 * hs

    def place_of(i):
        return jnp.where(i % 2 == 1, (i + 1) // 2, lax.rem(nz - i // 2, nz))

    def project(i):
        place = place_of(i)
        for s in range(z_subs):
            arrived(z_part.at[place, s, other_stripes], oz_sem.at[place, s])
        lhs = jnp.concatenate(
            [x_wide[place, s].reshape(block, SUB) for s in range(x_subs)]
            + [z_part[place, s].reshape(block, z_wide) for s in range(z_subs)],
            axis=1,
        )
        term = jnp.dot(lhs, w2[...], preferred_element_type=F32)
        b_send[i] = term[:, width:].astype(BF)
        remote(
            b_send.at[i], b_recv.at[i], send_sem.at[10], b_sem.at[i], tensor_0=pair
        ).start()
        stash[i] = term[:, :width]

    def finish(i):
        arrived(b_recv.at[i], b_sem.at[i])
        total = stash[i] + b_recv[i].astype(F32)
        total = total.astype(BF).reshape(NX, rows, width)
        origin = lax.rem(z + place_of(i), nz)
        q_buf[:, origin] = total[:, :, :hs]
        k_buf[:, origin] = total[:, :, hs : 2 * hs]
        v_buf[:, origin] = total[:, :, 2 * hs :]

    trips = nz + LAG
    late = {}

    def at_trip(i, *steps):
        late.setdefault(min(i, trips - 1), []).extend(steps)

    for step, at in zip(range(early + 1, turns + 1), (0, 3, 8, 13)):
        at_trip(
            min(at, 2 * step - 1),
            functools.partial(gather_step, step),
            functools.partial(firsts_step, step),
        )
    at_trip(4, out_weights_relay)
    at_trip(6, out_weights_direct)
    at_trip(12, out_weights_last)

    def trip(i, carry):
        for at, steps in late.items():

            @pl.when(i == at)
            def _(steps=steps):
                for step in steps:
                    step()

        @pl.when(i < nz)
        def _():
            project(i)

        @pl.when(i >= LAG)
        def _():
            finish(i - LAG)

        return carry

    lax.fori_loop(0, trips, trip, 0)
    out_weights_wait()

    row = mix_index[0]
    weight_now = mix_table[0, row]
    weight_first = mix_table[1, row]

    def mix(origin, first):
        now = v_buf[:, origin].astype(F32)
        v_buf[:, origin] = (weight_now * now + weight_first * first.astype(F32)).astype(BF)

    mix(z, fv_own[0])
    for away in range(1, nz):
        arrived(fv_in.at[away], fz_sem.at[away])
        mix(lax.rem(z + away, nz), fv_in[away])

    scale = 1.0 / math.sqrt(hs)
    valid = lengths[0]
    stripe = nz * rows
    q_blocks = min(nz, 128 // rows)
    q_rows = q_blocks * rows

    def attend(b):
        n = (b + 1) * stripe
        keys = k_buf[0 : b + 1].reshape(n, hs)
        values = v_buf[0 : b + 1].reshape(n, hs)

        def one(t, carry):
            at = pl.ds(t * q_blocks, q_blocks)
            query = q_buf[b, at].reshape(q_rows, hs)
            scores = (
                lax.dot_general(query, keys, (((1,), (1,)), ((), ())), preferred_element_type=F32)
                * scale
            )
            col = lax.broadcasted_iota(jnp.int32, (q_rows, n), 1)
            line = b * stripe + t * q_rows + lax.broadcasted_iota(jnp.int32, (q_rows, n), 0)
            scores = jnp.where((col <= line) & (col < valid), scores, NEG_FILL)
            raised = jnp.exp(scores - jnp.max(scores, axis=1, keepdims=True))
            weights = (raised * (1.0 / jnp.sum(raised, axis=1, keepdims=True))).astype(BF)
            result = jnp.dot(weights, values, preferred_element_type=F32).astype(BF)
            att[0, at, b] = result.reshape(q_blocks, rows, hs)
            return carry

        lax.fori_loop(0, nz // q_blocks, one, 0)

    near, far = pl.ds(0, nz // 2), pl.ds(nz // 2, nz // 2)

    def att_send(b):
        remote(
            att.at[0, :, b], att.at[3, :, b], send_sem.at[14], att_sem.at[0, b], tensor_0=xs[1]
        ).start()
        remote(
            att.at[0, :, b], att.at[1, :, b], send_sem.at[15], att_sem.at[1, b], tensor_0=xs[3]
        ).start()

    def att_pass(b):
        arrived(att.at[3, :, b], att_sem.at[0, b])
        remote(
            att.at[3, near, b], att.at[2, near, b], send_sem.at[16], att_sem.at[2, b], tensor_0=xs[1]
        ).start()
        arrived(att.at[1, :, b], att_sem.at[1, b])
        remote(
            att.at[1, far, b], att.at[2, far, b], send_sem.at[17], att_sem.at[3, b], tensor_0=xs[3]
        ).start()

    attend(0)
    att_send(0)
    attend(1)
    att_send(1)
    att_pass(0)
    attend(2)
    att_send(2)
    att_pass(1)
    attend(3)
    att_send(3)
    att_pass(2)
    rs_recv[:, 0] = jnp.zeros(rs_recv.shape[:1] + rs_recv.shape[2:], BF)
    att_pass(3)
    for b in range(NX):
        arrived(att.at[2, near, b], att_sem.at[2, b])
        arrived(att.at[2, far, b], att_sem.at[3, b])

    def length_of(way, s):
        return turns if (s % 2 == 0) == (way == 0) else turns - 1

    def heads_of(away):
        origin = lax.rem(z + away + nz, nz)
        return jnp.concatenate([att[r, origin].reshape(block, hs) for r in range(NX)], axis=1)

    def columns(s):
        return wo2[:, s * SUB : (s + 1) * SUB]

    def reduce_step(step, carry):
        for s in range(subs):
            for way in (0, 1):
                length = length_of(way, s)
                sign = 1 - 2 * way

                @pl.when(step <= length)
                def _(s=s, way=way, length=length, sign=sign):
                    lhs = heads_of(sign * (length - step + 1))
                    term = jnp.dot(lhs, columns(s), preferred_element_type=F32)

                    @pl.when(step > 1)
                    def _():
                        arrived(rs_recv.at[way, step - 1, s], rs_sem.at[way, step - 1, s])

                    term = term + rs_recv[way, step - 1, s].astype(F32)
                    rs_send[2 * step - 2 + way, s] = term.astype(BF)
                    remote(
                        rs_send.at[2 * step - 2 + way, s],
                        rs_recv.at[way, step, s],
                        send_sem.at[18],
                        rs_sem.at[way, step, s],
                        tensor_1=z_up if way == 0 else z_down,
                    ).start()

        return carry

    lax.fori_loop(1, turns + 1, reduce_step, 0)
    own = heads_of(0)
    for s in range(subs):
        term = jnp.dot(own, columns(s), preferred_element_type=F32)
        for way in (0, 1):
            length = length_of(way, s)
            arrived(rs_recv.at[way, length, s], rs_sem.at[way, length, s])
            term = term + rs_recv[way, length, s].astype(F32)
        fin[s] = term.astype(BF).reshape(NX, rows, SUB)
        column = pl.multiple_of(x * quarter + s * SUB, 128)
        for d in (1, 2, 3):
            remote(
                fin.at[s, xs[d]],
                out.at[:, pl.ds(column, SUB)],
                send_sem.at[19],
                fin_sem.at[d, s],
                tensor_0=xs[d],
            ).start()
        pltpu.make_async_copy(
            fin.at[s, x], out.at[:, pl.ds(column, SUB)], fin_sem.at[0, s]
        ).start()

    n_ring = turns * 2 - 1
    arrived(x_wide.at[pl.ds(0, 3), :, 0], send_sem.at[0])
    arrived(z_part.at[0, :, 0], send_sem.at[1])
    arrived(fv_stage, send_sem.at[2])
    arrived(x_wide.at[pl.ds(0, n_ring)], send_sem.at[3])
    arrived(w2.at[pl.ds(0, share), pl.ds(0, width)], send_sem.at[4])
    arrived(z_part.at[pl.ds(0, n_ring), :, pl.ds(0, 2)], send_sem.at[5])
    arrived(z_part.at[:, :, pl.ds(0, 2)], send_sem.at[6])
    arrived(w2.at[pl.ds(0, share), pl.ds(0, width)], send_sem.at[7])
    arrived(fv_own.at[pl.ds(1, nz - 1)], send_sem.at[8])
    arrived(b_send, send_sem.at[10])
    arrived(wo2.at[pl.ds(0, 3 * hs), pl.ds(0, half)], send_sem.at[11])
    arrived(wo2.at[pl.ds(0, 3 * hs), pl.ds(0, half)], send_sem.at[12])
    arrived(wo_relay, send_sem.at[13])
    arrived(att.at[0], send_sem.at[14])
    arrived(att.at[0], send_sem.at[15])
    arrived(att.at[0, near], send_sem.at[16])
    arrived(att.at[0, far], send_sem.at[17])
    for s in range(subs):
        for d in range(NX):
            arrived(fin.at[s, x], fin_sem.at[d, s])
    arrived(rs_send.at[pl.ds(0, n_ring)], send_sem.at[18])
    arrived(fin.at[:, pl.ds(0, 3)], send_sem.at[19])


def body(hidden_in, first_values, qkv_weight, out_weight, mix_table, mix_index, lengths, *, nz):
    rows, model = hidden_in.shape[1:]
    hs = qkv_weight.shape[2]
    quarter = model // NX
    half = quarter // 2
    halves = model // 2
    subs = quarter // SUB
    x_subs = max(1, halves * 3 // 10 // SUB)
    z_subs = 2
    z_wide = (halves - x_subs * SUB) // z_subs
    turns = nz // 2
    block = NX * rows
    vmem = pl.BlockSpec(memory_space=pltpu.VMEM)
    smem = pl.BlockSpec(memory_space=pltpu.SMEM)
    anywhere = pl.BlockSpec(memory_space=pl.ANY)
    dma = pltpu.SemaphoreType.DMA
    scratch = [
        pltpu.VMEM((nz, x_subs, NX, rows, SUB), BF),
        pltpu.VMEM((nz, z_subs, NX, rows, z_wide), BF),
        pltpu.VMEM((halves, 2 * 3 * hs), BF),
        pltpu.VMEM((NX * hs, quarter), BF),
        pltpu.VMEM((hs, half), BF),
        pltpu.VMEM((NX - 1, nz, rows, hs), BF),
        pltpu.VMEM((nz, NX, rows, hs), BF),
        pltpu.VMEM((nz, NX, rows, hs), BF),
        pltpu.VMEM((nz, block, 3 * hs), F32),
        pltpu.VMEM((nz, block, 3 * hs), BF),
        pltpu.VMEM((nz, block, 3 * hs), BF),
        pltpu.VMEM((NX, nz, rows, hs), BF),
        pltpu.VMEM((NX, nz, rows, hs), BF),
        pltpu.VMEM((NX, nz, rows, hs), BF),
        pltpu.VMEM((NX, nz, NX, rows, hs), BF),
        pltpu.VMEM((2 * turns, subs, block, SUB), BF),
        pltpu.VMEM((2, turns + 1, subs, block, SUB), BF),
        pltpu.VMEM((subs, NX, rows, SUB), BF),
        dma((4,)),
        dma((20,)),
        dma((x_subs + z_subs,)),
        dma((NX, x_subs + z_subs)),
        dma((2, turns, x_subs + z_subs)),
        dma((nz, z_subs)),
        dma((2, 3)),
        dma((7,)),
        dma((NX,)),
        dma((nz,)),
        dma((nz,)),
        dma((4, NX)),
        dma((2, turns + 1, subs)),
        dma((NX, subs)),
    ]
    result = pl.pallas_call(
        functools.partial(kernel, nz),
        out_shape=jax.ShapeDtypeStruct((rows, model), BF),
        in_specs=[vmem, vmem, anywhere, anywhere, smem, smem, smem],
        out_specs=anywhere,
        scratch_shapes=scratch,
        compiler_params=pltpu.CompilerParams(
            collective_id=0, has_side_effects=True, vmem_limit_bytes=60 * 1024 * 1024
        ),
    )(
        hidden_in[0],
        first_values[0],
        jnp.transpose(qkv_weight, (1, 0, 2)),
        out_weight,
        mix_table.T,
        mix_index,
        lengths,
    )
    return result[None]


def solution(mesh):
    nz = mesh.shape["tensor"] // NX
    torus = Mesh(
        mesh.devices.reshape(mesh.shape["groups"], mesh.shape["dp"], NX, nz),
        ("groups", "dp", "tensor_0", "tensor_1"),
    )
    placed = (
        P(("groups", "dp"), TENSOR, None),
        P(("groups", "dp"), TENSOR, None),
        P(None, None, TENSOR),
        P(TENSOR, None),
        P(),
        P(TENSOR),
        P(("groups", "dp")),
    )
    return jax.shard_map(
        functools.partial(body, nz=nz),
        mesh=torus,
        in_specs=placed,
        out_specs=P(("groups", "dp"), TENSOR, None),
        check_vma=False,
    )
```

```python
import functools
import math

import jax
import jax.numpy as jnp
from jax import lax
from jax.experimental import pallas as pl
from jax.experimental.pallas import tpu as pltpu
from jax.sharding import Mesh
from jax.sharding import PartitionSpec as P

TENSOR = ("tensor_0", "tensor_1")
NEG_FILL = -1e30
BF = jnp.bfloat16
F32 = jnp.float32
NX = 4
SUB = 256
LAG = 3


def kernel(
    nz,
    hid,
    firsts,
    w_qkv,
    w_out,
    mix_table,
    mix_index,
    lengths,
    out,
    x_wide,
    z_part,
    w2,
    wo2,
    wo_relay,
    fv_stage,
    fv_own,
    fv_in,
    stash,
    b_send,
    b_recv,
    q_buf,
    k_buf,
    v_buf,
    att,
    rs_send,
    rs_recv,
    fin,
    local_sem,
    send_sem,
    own_sem,
    hid_sem,
    ag_sem,
    oz_sem,
    w_sem,
    wo_sem,
    fx_sem,
    fz_sem,
    b_sem,
    att_sem,
    rs_sem,
    fin_sem,
):
    rows, model = hid.shape
    hs = w_qkv.shape[2]
    quarter = model // NX
    half = quarter // 2
    halves = model // 2
    subs = quarter // SUB
    turns = nz // 2
    block = NX * rows

    x = lax.axis_index("tensor_0")
    z = lax.axis_index("tensor_1")
    core = lax.axis_index("dp")
    xs = [x] + [lax.rem(x + d, NX) for d in range(1, NX)]
    z_up = lax.rem(z + 1, nz)
    z_down = lax.rem(z + nz - 1, nz)
    x_way = lax.rem(x + 1 + 2 * core, NX)
    odd = lax.rem(x, 2)
    pair = x + 1 - 2 * odd
    other = lax.rem(x + NX - 1 + 2 * odd, NX)

    def remote(src, dst, send, recv, **where):
        return pltpu.make_async_remote_copy(
            src_ref=src,
            dst_ref=dst,
            send_sem=send,
            recv_sem=recv,
            device_id=where,
            device_id_type=pl.DeviceIdType.MESH,
        )

    def arrived(ref, sem):
        pltpu.make_async_copy(ref, ref, sem).wait()

    barrier = pltpu.get_barrier_semaphore()
    partners = [
        {"dp": 1 - core},
        {"tensor_0": xs[1]},
        {"tensor_0": xs[2]},
        {"tensor_0": xs[3]},
        {"tensor_1": z_up},
        {"tensor_1": z_down},
    ]
    for partner in partners:
        pl.semaphore_signal(
            barrier, inc=1, device_id=partner, device_id_type=pl.DeviceIdType.MESH
        )
    pl.semaphore_wait(barrier, len(partners))

    def half_of(at):
        return lax.rem((at + 1) // 2, 2)

    mine, theirs = half_of(x), 1 - half_of(x)
    stripes, other_stripes = pl.ds(x - odd, 2), pl.ds(NX - 2 - x + odd, 2)
    x_subs, z_subs, z_wide = x_wide.shape[1], z_part.shape[1], z_part.shape[4]

    def x_columns(to_half, s):
        return pl.ds(pl.multiple_of(to_half * halves + s * SUB, 128), SUB)

    def z_columns(to_half, s):
        return pl.ds(pl.multiple_of(to_half * halves + x_subs * SUB + s * z_wide, 128), z_wide)

    def hidden_out(d, to, to_half):
        for s in range(x_subs):
            remote(
                hid.at[:, x_columns(to_half, s)],
                x_wide.at[0, s, x],
                send_sem.at[0],
                hid_sem.at[d, s],
                tensor_0=to,
            ).start()

    for s in range(z_subs):
        remote(
            hid.at[:, z_columns(theirs, s)],
            z_part.at[0, s, x],
            send_sem.at[1],
            hid_sem.at[0, s],
            tensor_0=pair,
        ).start()
    hidden_out(1, pair, theirs)
    hidden_out(2, other, mine)
    hidden_out(3, xs[2], theirs)
    own_hidden = []
    for s in range(z_subs):
        own_hidden.append(
            pltpu.make_async_copy(
                hid.at[:, z_columns(mine, s)], z_part.at[0, s, x], own_sem.at[s]
            )
        )
    for s in range(x_subs):
        own_hidden.append(
            pltpu.make_async_copy(
                hid.at[:, x_columns(mine, s)], x_wide.at[0, s, x], own_sem.at[z_subs + s]
            )
        )
    for copy in own_hidden:
        copy.start()

    def stage_firsts(head, carry):
        away = lax.rem(head - z + nz, nz)
        for d in range(NX):
            column = pl.multiple_of((xs[d] * nz + head) * hs, 128)
            piece = firsts[:, pl.ds(column, hs)]
            if d == 0:
                fv_own[away, x] = piece
            else:
                fv_stage[d - 1, away] = piece
        return carry

    lax.fori_loop(0, nz, stage_firsts, 0)
    for d in (1, 2, 3):
        remote(
            fv_stage.at[d - 1],
            fv_own.at[:, x],
            send_sem.at[2],
            fx_sem.at[d],
            tensor_0=xs[d],
        ).start()

    share = halves // 2
    my_share = pl.multiple_of(core * share, 128)
    sibling_share = pl.multiple_of((1 - core) * share, 128)
    for p in range(3):
        remote(
            w_qkv.at[p, pl.ds(pl.multiple_of(theirs * halves + core * share, 128), share)],
            w2.at[pl.ds(my_share, share), pl.ds((3 + p) * hs, hs)],
            send_sem.at[4],
            w_sem.at[0, p],
            tensor_0=pair,
        ).start()
    own_weights = []
    for p in range(3):
        own_weights.append(
            pltpu.make_async_copy(
                w_qkv.at[p, pl.ds(pl.multiple_of(mine * halves, 128), halves)],
                w2.at[:, pl.ds(p * hs, hs)],
                local_sem.at[p],
            )
        )
    own_weights.append(
        pltpu.make_async_copy(
            w_out.at[:, pl.ds(pl.multiple_of(x * quarter, 128), quarter)],
            wo2.at[pl.ds(0, hs)],
            local_sem.at[3],
        )
    )
    for copy in own_weights:
        copy.start()

    my_half = pl.multiple_of(core * half, 128)

    def wo_columns(to):
        return pl.ds(pl.multiple_of(to * quarter + core * half, 128), half)

    def wo_piece(r):
        return wo2.at[pl.ds(r * hs, hs), pl.ds(my_half, half)]

    def out_weights_send():
        remote(
            w_out.at[:, wo_columns(xs[2])], wo_relay, send_sem.at[11], wo_sem.at[0], tensor_0=x_way
        ).start()
        for d, r, sem in ((1, 3, 1), (3, 1, 2)):
            remote(
                w_out.at[:, wo_columns(xs[d])],
                wo_piece(r),
                send_sem.at[11],
                wo_sem.at[sem],
                tensor_0=xs[d],
            ).start()

    def out_to_sibling(r):
        remote(
            wo_piece(r), wo_piece(r), send_sem.at[12], wo_sem.at[3 + r], dp=1 - core
        ).start()

    def out_weights_relay():
        arrived(wo_relay, wo_sem.at[0])
        remote(wo_relay, wo_piece(2), send_sem.at[13], wo_sem.at[3], tensor_0=x_way).start()

    def out_weights_direct():
        for r, sem in ((3, 1), (1, 2)):
            arrived(wo_piece(r), wo_sem.at[sem])
            out_to_sibling(r)

    def out_weights_last():
        arrived(wo_piece(2), wo_sem.at[3])
        out_to_sibling(2)

    def out_weights_wait():
        other = pl.multiple_of((1 - core) * half, 128)
        for r in (1, 2, 3):
            arrived(wo2.at[pl.ds(r * hs, hs), pl.ds(other, half)], wo_sem.at[3 + r])

    out_weights_send()

    flows = [(0, s) for s in range(x_subs)] + [(1, s) for s in range(z_subs)]

    def longer(way, n):
        return turns if (n % 2 == 0) == (way == 0) else turns - 1

    def part(n, place):
        kind, s = flows[n]
        return x_wide.at[place, s] if kind == 0 else z_part.at[place, s, stripes]

    def ring_send(n, way, step):
        source, target = (step - 1, step) if way else ((nz - step + 1) % nz, nz - step)
        remote(
            part(n, source),
            part(n, target),
            send_sem.at[3 if flows[n][0] == 0 else 5],
            ag_sem.at[way, step - 1, n],
            tensor_1=z_down if way else z_up,
        ).start()

    def to_other(n, place):
        kind, s = flows[n]
        if kind == 1:
            remote(
                z_part.at[place, s, stripes],
                z_part.at[place, s, stripes],
                send_sem.at[6],
                oz_sem.at[place, s],
                tensor_0=other,
            ).start()

    def gather_step(step):
        for n in range(len(flows)):
            for way in (0, 1):
                if step <= longer(way, n):
                    place = step if way else nz - step
                    arrived(part(n, place), ag_sem.at[way, step - 1, n])
                    if step + 1 <= longer(way, n):
                        ring_send(n, way, step + 1)
                    to_other(n, place)

    def weights_step(p):
        here = w2.at[pl.ds(my_share, share), pl.ds((3 + p) * hs, hs)]
        arrived(here, w_sem.at[0, p])
        remote(here, here, send_sem.at[7], w_sem.at[1, p], dp=1 - core).start()

    def weights_last():
        for p in range(3):
            arrived(
                w2.at[pl.ds(sibling_share, share), pl.ds((3 + p) * hs, hs)], w_sem.at[1, p]
            )
        for copy in own_weights:
            copy.wait()

    def firsts_step(step):
        if step == 1:
            for d in (1, 2, 3):
                arrived(fv_stage.at[d - 1], fx_sem.at[d])
        for away in sorted({step, nz - step}):
            remote(
                fv_own.at[away],
                fv_in.at[nz - away],
                send_sem.at[8],
                fz_sem.at[nz - away],
                tensor_1=lax.rem(z + away, nz),
            ).start()

    for copy in own_hidden:
        copy.wait()
    for s in range(z_subs):
        arrived(z_part.at[0, s, pair], hid_sem.at[0, s])
        ring_send(x_subs + s, 0, 1)
        ring_send(x_subs + s, 1, 1)
        to_other(x_subs + s, 0)
    for s in range(x_subs):
        for d in (1, 2, 3):
            arrived(x_wide.at[0, s, x], hid_sem.at[d, s])
        ring_send(s, 0, 1)
        ring_send(s, 1, 1)
    early = max(turns - 3, 0)
    weights_after = {2: (0,), 3: (1,), 4: (2,)}
    for step in range(1, early + 1):
        gather_step(step)
        firsts_step(step)
        for p in weights_after.get(step, ()):
            weights_step(p)
    for p in range(3):
        if not any(p in done for step, done in weights_after.items() if step <= early):
            weights_step(p)
    weights_last()

    width = 3 * hs

    def place_of(i):
        return jnp.where(i % 2 == 1, (i + 1) // 2, lax.rem(nz - i // 2, nz))

    def project(i):
        place = place_of(i)
        for s in range(z_subs):
            arrived(z_part.at[place, s, other_stripes], oz_sem.at[place, s])
        lhs = jnp.concatenate(
            [x_wide[place, s].reshape(block, SUB) for s in range(x_subs)]
            + [z_part[place, s].reshape(block, z_wide) for s in range(z_subs)],
            axis=1,
        )
        term = jnp.dot(lhs, w2[...], preferred_element_type=F32)
        b_send[i] = term[:, width:].astype(BF)
        remote(
            b_send.at[i], b_recv.at[i], send_sem.at[10], b_sem.at[i], tensor_0=pair
        ).start()
        stash[i] = term[:, :width]

    def finish(i):
        arrived(b_recv.at[i], b_sem.at[i])
        total = stash[i] + b_recv[i].astype(F32)
        total = total.astype(BF).reshape(NX, rows, width)
        origin = lax.rem(z + place_of(i), nz)
        q_buf[:, origin] = total[:, :, :hs]
        k_buf[:, origin] = total[:, :, hs : 2 * hs]
        v_buf[:, origin] = total[:, :, 2 * hs :]

    trips = nz + LAG
    late = {}

    def at_trip(i, *steps):
        late.setdefault(min(i, trips - 1), []).extend(steps)

    for step, at in zip(range(early + 1, turns + 1), (2, 7, 12)):
        at_trip(
            min(at, 2 * step - 1),
            functools.partial(gather_step, step),
            functools.partial(firsts_step, step),
        )
    at_trip(4, out_weights_relay)
    at_trip(6, out_weights_direct)
    at_trip(12, out_weights_last)

    def trip(i, carry):
        for at, steps in late.items():

            @pl.when(i == at)
            def _(steps=steps):
                for step in steps:
                    step()

        @pl.when(i < nz)
        def _():
            project(i)

        @pl.when(i >= LAG)
        def _():
            finish(i - LAG)

        return carry

    lax.fori_loop(0, trips, trip, 0)
    out_weights_wait()

    row = mix_index[0]
    weight_now = mix_table[0, row]
    weight_first = mix_table[1, row]

    def mix(origin, first):
        now = v_buf[:, origin].astype(F32)
        v_buf[:, origin] = (weight_now * now + weight_first * first.astype(F32)).astype(BF)

    mix(z, fv_own[0])
    for away in range(1, nz):
        arrived(fv_in.at[away], fz_sem.at[away])
        mix(lax.rem(z + away, nz), fv_in[away])

    scale = 1.0 / math.sqrt(hs)
    valid = lengths[0]
    stripe = nz * rows
    q_blocks = min(nz, 128 // rows)
    q_rows = q_blocks * rows

    def attend(b):
        n = (b + 1) * stripe
        keys = k_buf[0 : b + 1].reshape(n, hs)
        values = v_buf[0 : b + 1].reshape(n, hs)

        def one(t, carry):
            at = pl.ds(t * q_blocks, q_blocks)
            query = q_buf[b, at].reshape(q_rows, hs)
            scores = (
                lax.dot_general(query, keys, (((1,), (1,)), ((), ())), preferred_element_type=F32)
                * scale
            )
            col = lax.broadcasted_iota(jnp.int32, (q_rows, n), 1)
            line = b * stripe + t * q_rows + lax.broadcasted_iota(jnp.int32, (q_rows, n), 0)
            scores = jnp.where((col <= line) & (col < valid), scores, NEG_FILL)
            raised = jnp.exp(scores - jnp.max(scores, axis=1, keepdims=True))
            weights = (raised * (1.0 / jnp.sum(raised, axis=1, keepdims=True))).astype(BF)
            result = jnp.dot(weights, values, preferred_element_type=F32).astype(BF)
            att[0, at, b] = result.reshape(q_blocks, rows, hs)
            return carry

        lax.fori_loop(0, nz // q_blocks, one, 0)

    near, far = pl.ds(0, nz // 2), pl.ds(nz // 2, nz // 2)

    def att_send(b):
        remote(
            att.at[0, :, b], att.at[3, :, b], send_sem.at[14], att_sem.at[0, b], tensor_0=xs[1]
        ).start()
        remote(
            att.at[0, :, b], att.at[1, :, b], send_sem.at[15], att_sem.at[1, b], tensor_0=xs[3]
        ).start()

    def att_pass(b):
        arrived(att.at[3, :, b], att_sem.at[0, b])
        remote(
            att.at[3, near, b], att.at[2, near, b], send_sem.at[16], att_sem.at[2, b], tensor_0=xs[1]
        ).start()
        arrived(att.at[1, :, b], att_sem.at[1, b])
        remote(
            att.at[1, far, b], att.at[2, far, b], send_sem.at[17], att_sem.at[3, b], tensor_0=xs[3]
        ).start()

    attend(0)
    att_send(0)
    attend(1)
    att_send(1)
    att_pass(0)
    attend(2)
    att_send(2)
    att_pass(1)
    attend(3)
    att_send(3)
    att_pass(2)
    rs_recv[:, 0] = jnp.zeros(rs_recv.shape[:1] + rs_recv.shape[2:], BF)
    att_pass(3)
    for b in range(NX):
        arrived(att.at[2, near, b], att_sem.at[2, b])
        arrived(att.at[2, far, b], att_sem.at[3, b])

    def length_of(way, s):
        return turns if (s % 2 == 0) == (way == 0) else turns - 1

    def heads_of(away):
        origin = lax.rem(z + away + nz, nz)
        return jnp.concatenate([att[r, origin].reshape(block, hs) for r in range(NX)], axis=1)

    def columns(s):
        return wo2[:, s * SUB : (s + 1) * SUB]

    def reduce_step(step, carry):
        for s in range(subs):
            for way in (0, 1):
                length = length_of(way, s)
                sign = 1 - 2 * way

                @pl.when(step <= length)
                def _(s=s, way=way, length=length, sign=sign):
                    lhs = heads_of(sign * (length - step + 1))
                    term = jnp.dot(lhs, columns(s), preferred_element_type=F32)

                    @pl.when(step > 1)
                    def _():
                        arrived(rs_recv.at[way, step - 1, s], rs_sem.at[way, step - 1, s])

                    term = term + rs_recv[way, step - 1, s].astype(F32)
                    rs_send[2 * step - 2 + way, s] = term.astype(BF)
                    remote(
                        rs_send.at[2 * step - 2 + way, s],
                        rs_recv.at[way, step, s],
                        send_sem.at[18],
                        rs_sem.at[way, step, s],
                        tensor_1=z_up if way == 0 else z_down,
                    ).start()

        return carry

    lax.fori_loop(1, turns + 1, reduce_step, 0)
    own = heads_of(0)
    for s in range(subs):
        term = jnp.dot(own, columns(s), preferred_element_type=F32)
        for way in (0, 1):
            length = length_of(way, s)
            arrived(rs_recv.at[way, length, s], rs_sem.at[way, length, s])
            term = term + rs_recv[way, length, s].astype(F32)
        fin[s] = term.astype(BF).reshape(NX, rows, SUB)
        column = pl.multiple_of(x * quarter + s * SUB, 128)
        for d in (1, 2, 3):
            remote(
                fin.at[s, xs[d]],
                out.at[:, pl.ds(column, SUB)],
                send_sem.at[19],
                fin_sem.at[d, s],
                tensor_0=xs[d],
            ).start()
        pltpu.make_async_copy(
            fin.at[s, x], out.at[:, pl.ds(column, SUB)], fin_sem.at[0, s]
        ).start()

    n_ring = turns * 2 - 1
    arrived(x_wide.at[pl.ds(0, 3), :, 0], send_sem.at[0])
    arrived(z_part.at[0, :, 0], send_sem.at[1])
    arrived(fv_stage, send_sem.at[2])
    arrived(x_wide.at[pl.ds(0, n_ring)], send_sem.at[3])
    arrived(w2.at[pl.ds(0, share), pl.ds(0, width)], send_sem.at[4])
    arrived(z_part.at[pl.ds(0, n_ring), :, pl.ds(0, 2)], send_sem.at[5])
    arrived(z_part.at[:, :, pl.ds(0, 2)], send_sem.at[6])
    arrived(w2.at[pl.ds(0, share), pl.ds(0, width)], send_sem.at[7])
    arrived(fv_own.at[pl.ds(1, nz - 1)], send_sem.at[8])
    arrived(b_send, send_sem.at[10])
    arrived(wo2.at[pl.ds(0, 3 * hs), pl.ds(0, half)], send_sem.at[11])
    arrived(wo2.at[pl.ds(0, 3 * hs), pl.ds(0, half)], send_sem.at[12])
    arrived(wo_relay, send_sem.at[13])
    arrived(att.at[0], send_sem.at[14])
    arrived(att.at[0], send_sem.at[15])
    arrived(att.at[0, near], send_sem.at[16])
    arrived(att.at[0, far], send_sem.at[17])
    for s in range(subs):
        for d in range(NX):
            arrived(fin.at[s, x], fin_sem.at[d, s])
    arrived(rs_send.at[pl.ds(0, n_ring)], send_sem.at[18])
    arrived(fin.at[:, pl.ds(0, 3)], send_sem.at[19])


def body(hidden_in, first_values, qkv_weight, out_weight, mix_table, mix_index, lengths, *, nz):
    rows, model = hidden_in.shape[1:]
    hs = qkv_weight.shape[2]
    quarter = model // NX
    half = quarter // 2
    halves = model // 2
    subs = quarter // SUB
    x_subs = max(1, halves * 3 // 10 // SUB)
    z_subs = 2
    z_wide = (halves - x_subs * SUB) // z_subs
    turns = nz // 2
    block = NX * rows
    vmem = pl.BlockSpec(memory_space=pltpu.VMEM)
    smem = pl.BlockSpec(memory_space=pltpu.SMEM)
    anywhere = pl.BlockSpec(memory_space=pl.ANY)
    dma = pltpu.SemaphoreType.DMA
    scratch = [
        pltpu.VMEM((nz, x_subs, NX, rows, SUB), BF),
        pltpu.VMEM((nz, z_subs, NX, rows, z_wide), BF),
        pltpu.VMEM((halves, 2 * 3 * hs), BF),
        pltpu.VMEM((NX * hs, quarter), BF),
        pltpu.VMEM((hs, half), BF),
        pltpu.VMEM((NX - 1, nz, rows, hs), BF),
        pltpu.VMEM((nz, NX, rows, hs), BF),
        pltpu.VMEM((nz, NX, rows, hs), BF),
        pltpu.VMEM((nz, block, 3 * hs), F32),
        pltpu.VMEM((nz, block, 3 * hs), BF),
        pltpu.VMEM((nz, block, 3 * hs), BF),
        pltpu.VMEM((NX, nz, rows, hs), BF),
        pltpu.VMEM((NX, nz, rows, hs), BF),
        pltpu.VMEM((NX, nz, rows, hs), BF),
        pltpu.VMEM((NX, nz, NX, rows, hs), BF),
        pltpu.VMEM((2 * turns, subs, block, SUB), BF),
        pltpu.VMEM((2, turns + 1, subs, block, SUB), BF),
        pltpu.VMEM((subs, NX, rows, SUB), BF),
        dma((4,)),
        dma((20,)),
        dma((x_subs + z_subs,)),
        dma((NX, x_subs + z_subs)),
        dma((2, turns, x_subs + z_subs)),
        dma((nz, z_subs)),
        dma((2, 3)),
        dma((7,)),
        dma((NX,)),
        dma((nz,)),
        dma((nz,)),
        dma((4, NX)),
        dma((2, turns + 1, subs)),
        dma((NX, subs)),
    ]
    result = pl.pallas_call(
        functools.partial(kernel, nz),
        out_shape=jax.ShapeDtypeStruct((rows, model), BF),
        in_specs=[vmem, vmem, anywhere, anywhere, smem, smem, smem],
        out_specs=anywhere,
        scratch_shapes=scratch,
        compiler_params=pltpu.CompilerParams(
            collective_id=0, has_side_effects=True, vmem_limit_bytes=60 * 1024 * 1024
        ),
    )(
        hidden_in[0],
        first_values[0],
        jnp.transpose(qkv_weight, (1, 0, 2)),
        out_weight,
        mix_table.T,
        mix_index,
        lengths,
    )
    return result[None]


def solution(mesh):
    nz = mesh.shape["tensor"] // NX
    torus = Mesh(
        mesh.devices.reshape(mesh.shape["groups"], mesh.shape["dp"], NX, nz),
        ("groups", "dp", "tensor_0", "tensor_1"),
    )
    placed = (
        P(("groups", "dp"), TENSOR, None),
        P(("groups", "dp"), TENSOR, None),
        P(None, None, TENSOR),
        P(TENSOR, None),
        P(),
        P(TENSOR),
        P(("groups", "dp")),
    )
    return jax.shard_map(
        functools.partial(body, nz=nz),
        mesh=torus,
        in_specs=placed,
        out_specs=P(("groups", "dp"), TENSOR, None),
        check_vma=False,
    )
```

```python
import functools
import math

import jax
import jax.numpy as jnp
from jax import lax
from jax.experimental import pallas as pl
from jax.experimental.pallas import tpu as pltpu
from jax.sharding import Mesh
from jax.sharding import PartitionSpec as P

TENSOR = ("tensor_0", "tensor_1")
NEG_FILL = -1e30
BF = jnp.bfloat16
F32 = jnp.float32
NX = 4
SUB = 256
LAG = 3


def kernel(
    nz,
    hid,
    firsts,
    w_qkv,
    w_out,
    mix_table,
    mix_index,
    lengths,
    out,
    x_wide,
    z_part,
    w2,
    wo2,
    wo_relay,
    fv_stage,
    fv_own,
    fv_in,
    stash,
    b_send,
    b_recv,
    q_buf,
    k_buf,
    v_buf,
    att,
    rs_send,
    rs_recv,
    own_term,
    fin,
    local_sem,
    send_sem,
    own_sem,
    hid_sem,
    ag_sem,
    oz_sem,
    w_sem,
    wo_sem,
    fx_sem,
    fz_sem,
    b_sem,
    att_sem,
    rs_sem,
    fin_sem,
):
    rows, model = hid.shape
    hs = w_qkv.shape[2]
    quarter = model // NX
    half = quarter // 2
    halves = model // 2
    subs = quarter // SUB
    turns = nz // 2
    block = NX * rows

    x = lax.axis_index("tensor_0")
    z = lax.axis_index("tensor_1")
    core = lax.axis_index("dp")
    xs = [x] + [lax.rem(x + d, NX) for d in range(1, NX)]
    z_up = lax.rem(z + 1, nz)
    z_down = lax.rem(z + nz - 1, nz)
    x_way = lax.rem(x + 1 + 2 * core, NX)
    odd = lax.rem(x, 2)
    pair = x + 1 - 2 * odd
    other = lax.rem(x + NX - 1 + 2 * odd, NX)

    def remote(src, dst, send, recv, **where):
        return pltpu.make_async_remote_copy(
            src_ref=src,
            dst_ref=dst,
            send_sem=send,
            recv_sem=recv,
            device_id=where,
            device_id_type=pl.DeviceIdType.MESH,
        )

    def arrived(ref, sem):
        pltpu.make_async_copy(ref, ref, sem).wait()

    barrier = pltpu.get_barrier_semaphore()
    partners = [
        {"dp": 1 - core},
        {"tensor_0": xs[1]},
        {"tensor_0": xs[2]},
        {"tensor_0": xs[3]},
        {"tensor_1": z_up},
        {"tensor_1": z_down},
    ]
    for partner in partners:
        pl.semaphore_signal(
            barrier, inc=1, device_id=partner, device_id_type=pl.DeviceIdType.MESH
        )
    pl.semaphore_wait(barrier, len(partners))

    def half_of(at):
        return lax.rem((at + 1) // 2, 2)

    mine, theirs = half_of(x), 1 - half_of(x)
    stripes, other_stripes = pl.ds(x - odd, 2), pl.ds(NX - 2 - x + odd, 2)
    x_subs, z_subs, z_wide = x_wide.shape[1], z_part.shape[1], z_part.shape[4]

    def x_columns(to_half, s):
        return pl.ds(pl.multiple_of(to_half * halves + s * SUB, 128), SUB)

    def z_columns(to_half, s):
        return pl.ds(pl.multiple_of(to_half * halves + x_subs * SUB + s * z_wide, 128), z_wide)

    def hidden_out(d, to, to_half):
        for s in range(x_subs):
            remote(
                hid.at[:, x_columns(to_half, s)],
                x_wide.at[0, s, x],
                send_sem.at[0],
                hid_sem.at[d, s],
                tensor_0=to,
            ).start()

    for s in range(z_subs):
        remote(
            hid.at[:, z_columns(theirs, s)],
            z_part.at[0, s, x],
            send_sem.at[1],
            hid_sem.at[0, s],
            tensor_0=pair,
        ).start()
    hidden_out(1, pair, theirs)
    hidden_out(2, other, mine)
    hidden_out(3, xs[2], theirs)
    own_hidden = []
    for s in range(z_subs):
        own_hidden.append(
            pltpu.make_async_copy(
                hid.at[:, z_columns(mine, s)], z_part.at[0, s, x], own_sem.at[s]
            )
        )
    for s in range(x_subs):
        own_hidden.append(
            pltpu.make_async_copy(
                hid.at[:, x_columns(mine, s)], x_wide.at[0, s, x], own_sem.at[z_subs + s]
            )
        )
    for copy in own_hidden:
        copy.start()

    def stage_firsts(head, carry):
        away = lax.rem(head - z + nz, nz)
        for d in range(NX):
            column = pl.multiple_of((xs[d] * nz + head) * hs, 128)
            piece = firsts[:, pl.ds(column, hs)]
            if d == 0:
                fv_own[away, x] = piece
            else:
                fv_stage[d - 1, away] = piece
        return carry

    lax.fori_loop(0, nz, stage_firsts, 0)
    for d in (1, 2, 3):
        remote(
            fv_stage.at[d - 1],
            fv_own.at[:, x],
            send_sem.at[2],
            fx_sem.at[d],
            tensor_0=xs[d],
        ).start()

    share = halves // 2
    my_share = pl.multiple_of(core * share, 128)
    sibling_share = pl.multiple_of((1 - core) * share, 128)
    for p in range(3):
        remote(
            w_qkv.at[p, pl.ds(pl.multiple_of(theirs * halves + core * share, 128), share)],
            w2.at[pl.ds(my_share, share), pl.ds((3 + p) * hs, hs)],
            send_sem.at[4],
            w_sem.at[0, p],
            tensor_0=pair,
        ).start()
    own_weights = []
    for p in range(3):
        own_weights.append(
            pltpu.make_async_copy(
                w_qkv.at[p, pl.ds(pl.multiple_of(mine * halves, 128), halves)],
                w2.at[:, pl.ds(p * hs, hs)],
                local_sem.at[p],
            )
        )
    own_weights.append(
        pltpu.make_async_copy(
            w_out.at[:, pl.ds(pl.multiple_of(x * quarter, 128), quarter)],
            wo2.at[pl.ds(0, hs)],
            local_sem.at[3],
        )
    )
    for copy in own_weights:
        copy.start()

    my_half = pl.multiple_of(core * half, 128)

    def wo_columns(to):
        return pl.ds(pl.multiple_of(to * quarter + core * half, 128), half)

    def wo_piece(r):
        return wo2.at[pl.ds(r * hs, hs), pl.ds(my_half, half)]

    def out_weights_send():
        remote(
            w_out.at[:, wo_columns(xs[2])], wo_relay, send_sem.at[11], wo_sem.at[0], tensor_0=x_way
        ).start()
        for d, r, sem in ((1, 3, 1), (3, 1, 2)):
            remote(
                w_out.at[:, wo_columns(xs[d])],
                wo_piece(r),
                send_sem.at[11],
                wo_sem.at[sem],
                tensor_0=xs[d],
            ).start()

    def out_to_sibling(r):
        remote(
            wo_piece(r), wo_piece(r), send_sem.at[12], wo_sem.at[3 + r], dp=1 - core
        ).start()

    def out_weights_relay():
        arrived(wo_relay, wo_sem.at[0])
        remote(wo_relay, wo_piece(2), send_sem.at[13], wo_sem.at[3], tensor_0=x_way).start()

    def out_weights_direct():
        for r, sem in ((3, 1), (1, 2)):
            arrived(wo_piece(r), wo_sem.at[sem])
            out_to_sibling(r)

    def out_weights_last():
        arrived(wo_piece(2), wo_sem.at[3])
        out_to_sibling(2)

    def out_weights_wait():
        other = pl.multiple_of((1 - core) * half, 128)
        for r in (1, 2, 3):
            arrived(wo2.at[pl.ds(r * hs, hs), pl.ds(other, half)], wo_sem.at[3 + r])

    out_weights_send()

    flows = [(0, s) for s in range(x_subs)] + [(1, s) for s in range(z_subs)]

    def longer(way, n):
        return turns if (n % 2 == 0) == (way == 0) else turns - 1

    def part(n, place):
        kind, s = flows[n]
        return x_wide.at[place, s] if kind == 0 else z_part.at[place, s, stripes]

    def ring_send(n, way, step):
        source, target = (step - 1, step) if way else ((nz - step + 1) % nz, nz - step)
        remote(
            part(n, source),
            part(n, target),
            send_sem.at[3 if flows[n][0] == 0 else 5],
            ag_sem.at[way, step - 1, n],
            tensor_1=z_down if way else z_up,
        ).start()

    def to_other(n, place):
        kind, s = flows[n]
        if kind == 1:
            remote(
                z_part.at[place, s, stripes],
                z_part.at[place, s, stripes],
                send_sem.at[6],
                oz_sem.at[place, s],
                tensor_0=other,
            ).start()

    def gather_step(step):
        for n in range(len(flows)):
            for way in (0, 1):
                if step <= longer(way, n):
                    place = step if way else nz - step
                    arrived(part(n, place), ag_sem.at[way, step - 1, n])
                    if step + 1 <= longer(way, n):
                        ring_send(n, way, step + 1)
                    to_other(n, place)

    def weights_step(p):
        here = w2.at[pl.ds(my_share, share), pl.ds((3 + p) * hs, hs)]
        arrived(here, w_sem.at[0, p])
        remote(here, here, send_sem.at[7], w_sem.at[1, p], dp=1 - core).start()

    def weights_last():
        for p in range(3):
            arrived(
                w2.at[pl.ds(sibling_share, share), pl.ds((3 + p) * hs, hs)], w_sem.at[1, p]
            )
        for copy in own_weights:
            copy.wait()

    def firsts_step(step):
        if step == 1:
            for d in (1, 2, 3):
                arrived(fv_stage.at[d - 1], fx_sem.at[d])
        for away in sorted({step, nz - step}):
            remote(
                fv_own.at[away],
                fv_in.at[nz - away],
                send_sem.at[8],
                fz_sem.at[nz - away],
                tensor_1=lax.rem(z + away, nz),
            ).start()

    for copy in own_hidden:
        copy.wait()
    for s in range(z_subs):
        arrived(z_part.at[0, s, pair], hid_sem.at[0, s])
        ring_send(x_subs + s, 0, 1)
        ring_send(x_subs + s, 1, 1)
        to_other(x_subs + s, 0)
    for s in range(x_subs):
        for d in (1, 2, 3):
            arrived(x_wide.at[0, s, x], hid_sem.at[d, s])
        ring_send(s, 0, 1)
        ring_send(s, 1, 1)
    early = max(turns - 3, 0)
    weights_after = {2: (0,), 3: (1,), 4: (2,)}
    for step in range(1, early + 1):
        gather_step(step)
        for p in weights_after.get(step, ()):
            weights_step(p)
    for p in range(3):
        if not any(p in done for step, done in weights_after.items() if step <= early):
            weights_step(p)
    weights_last()

    width = 3 * hs

    def place_of(i):
        return jnp.where(i % 2 == 1, (i + 1) // 2, lax.rem(nz - i // 2, nz))

    def project(i):
        place = place_of(i)
        for s in range(z_subs):
            arrived(z_part.at[place, s, other_stripes], oz_sem.at[place, s])
        lhs = jnp.concatenate(
            [x_wide[place, s].reshape(block, SUB) for s in range(x_subs)]
            + [z_part[place, s].reshape(block, z_wide) for s in range(z_subs)],
            axis=1,
        )
        term = jnp.dot(lhs, w2[...], preferred_element_type=F32)
        b_send[i] = term[:, width:].astype(BF)
        remote(
            b_send.at[i], b_recv.at[i], send_sem.at[10], b_sem.at[i], tensor_0=pair
        ).start()
        stash[i] = term[:, :width]

    def finish(i):
        arrived(b_recv.at[i], b_sem.at[i])
        total = stash[i] + b_recv[i].astype(F32)
        total = total.astype(BF).reshape(NX, rows, width)
        origin = lax.rem(z + place_of(i), nz)
        q_buf[:, origin] = total[:, :, :hs]
        k_buf[:, origin] = total[:, :, hs : 2 * hs]
        v_buf[:, origin] = total[:, :, 2 * hs :]

    trips = nz + LAG
    late = {}

    def at_trip(i, *steps):
        late.setdefault(min(i, trips - 1), []).extend(steps)

    for step, at in zip(range(early + 1, turns + 1), (2, 7, 12)):
        at_trip(min(at, 2 * step - 1), functools.partial(gather_step, step))
        if step == turns:
            at_trip(
                min(at, 2 * step - 1),
                *(functools.partial(firsts_step, away) for away in range(1, turns + 1)),
            )
    at_trip(4, out_weights_relay)
    at_trip(6, out_weights_direct)
    at_trip(12, out_weights_last)

    def trip(i, carry):
        for at, steps in late.items():

            @pl.when(i == at)
            def _(steps=steps):
                for step in steps:
                    step()

        @pl.when(i < nz)
        def _():
            project(i)

        @pl.when(i >= LAG)
        def _():
            finish(i - LAG)

        return carry

    lax.fori_loop(0, trips, trip, 0)
    out_weights_wait()

    row = mix_index[0]
    weight_now = mix_table[0, row]
    weight_first = mix_table[1, row]

    def mix(origin, first):
        now = v_buf[:, origin].astype(F32)
        v_buf[:, origin] = (weight_now * now + weight_first * first.astype(F32)).astype(BF)

    mix(z, fv_own[0])
    for away in range(1, nz):
        arrived(fv_in.at[away], fz_sem.at[away])
        mix(lax.rem(z + away, nz), fv_in[away])

    scale = 1.0 / math.sqrt(hs)
    valid = lengths[0]
    stripe = nz * rows
    q_blocks = min(nz, 128 // rows)
    q_rows = q_blocks * rows

    def attend(b):
        n = (b + 1) * stripe
        keys = k_buf[0 : b + 1].reshape(n, hs)
        values = v_buf[0 : b + 1].reshape(n, hs)

        def one(t, carry):
            at = pl.ds(t * q_blocks, q_blocks)
            query = q_buf[b, at].reshape(q_rows, hs)
            scores = (
                lax.dot_general(query, keys, (((1,), (1,)), ((), ())), preferred_element_type=F32)
                * scale
            )
            col = lax.broadcasted_iota(jnp.int32, (q_rows, n), 1)
            line = b * stripe + t * q_rows + lax.broadcasted_iota(jnp.int32, (q_rows, n), 0)
            scores = jnp.where((col <= line) & (col < valid), scores, NEG_FILL)
            raised = jnp.exp(scores - jnp.max(scores, axis=1, keepdims=True))
            weights = (raised * (1.0 / jnp.sum(raised, axis=1, keepdims=True))).astype(BF)
            result = jnp.dot(weights, values, preferred_element_type=F32).astype(BF)
            att[0, at, b] = result.reshape(q_blocks, rows, hs)
            return carry

        lax.fori_loop(0, nz // q_blocks, one, 0)

    near, far = pl.ds(0, nz // 2), pl.ds(nz // 2, nz // 2)

    def att_send(b):
        remote(
            att.at[0, :, b], att.at[3, :, b], send_sem.at[14], att_sem.at[0, b], tensor_0=xs[1]
        ).start()
        remote(
            att.at[0, :, b], att.at[1, :, b], send_sem.at[15], att_sem.at[1, b], tensor_0=xs[3]
        ).start()

    def att_pass(b):
        arrived(att.at[3, :, b], att_sem.at[0, b])
        remote(
            att.at[3, near, b], att.at[2, near, b], send_sem.at[16], att_sem.at[2, b], tensor_0=xs[1]
        ).start()
        arrived(att.at[1, :, b], att_sem.at[1, b])
        remote(
            att.at[1, far, b], att.at[2, far, b], send_sem.at[17], att_sem.at[3, b], tensor_0=xs[3]
        ).start()

    for b in range(NX):
        attend(b)
        att_send(b)
    rs_recv[:, 0] = jnp.zeros(rs_recv.shape[:1] + rs_recv.shape[2:], BF)
    for b in range(NX):
        att_pass(b)
    for b in range(NX):
        arrived(att.at[2, near, b], att_sem.at[2, b])
        arrived(att.at[2, far, b], att_sem.at[3, b])

    def length_of(way, s):
        return turns if (s % 2 == 0) == (way == 0) else turns - 1

    def heads_of(away):
        origin = lax.rem(z + away + nz, nz)
        return jnp.concatenate([att[r, origin].reshape(block, hs) for r in range(NX)], axis=1)

    def columns(s):
        return wo2[:, s * SUB : (s + 1) * SUB]

    def own_terms(step):
        for s in range(subs):
            for way in (0, 1):
                length = length_of(way, s)

                @pl.when(step <= length)
                def _(s=s, way=way, length=length):
                    lhs = heads_of((1 - 2 * way) * (length - step + 1))
                    own_term[way, s] = jnp.dot(lhs, columns(s), preferred_element_type=F32)

    def out_columns(s):
        return pl.ds(pl.multiple_of(x * quarter + s * SUB, 128), SUB)

    def reduce_step(step, carry):
        for s in range(subs):
            for way in (0, 1):
                length = length_of(way, s)
                z_next = z_down if way else z_up
                slot = 2 * step - 2 + way

                @pl.when(step <= length)
                def _(s=s, way=way, z_next=z_next, slot=slot, length=length):
                    @pl.when(step > 1)
                    def _():
                        arrived(rs_recv.at[way, step - 1, s], rs_sem.at[way, step - 1, s])

                    term = own_term[way, s] + rs_recv[way, step - 1, s].reshape(
                        block, SUB
                    ).astype(F32)
                    rs_send[slot, s] = term.astype(BF).reshape(NX, rows, SUB)

                    @pl.when(step < length)
                    def _():
                        remote(
                            rs_send.at[slot, s],
                            rs_recv.at[way, step, s],
                            send_sem.at[18],
                            rs_sem.at[way, step, s],
                            tensor_1=z_next,
                        ).start()

                    @pl.when(step == length)
                    def _():
                        for d in range(NX):
                            remote(
                                rs_send.at[slot, s, xs[d]],
                                out.at[1 + way, :, out_columns(s)],
                                send_sem.at[18],
                                fin_sem.at[1 + way, d, s],
                                tensor_0=xs[d],
                                tensor_1=z_next,
                            ).start()

        @pl.when(step < turns)
        def _():
            own_terms(step + 1)

        return carry

    own_terms(1)
    lax.fori_loop(1, turns + 1, reduce_step, 0)
    own = heads_of(0)
    for s in range(subs):
        term = jnp.dot(own, columns(s), preferred_element_type=F32)
        fin[s] = term.astype(BF).reshape(NX, rows, SUB)
        for d in (1, 2, 3):
            remote(
                fin.at[s, xs[d]],
                out.at[0, :, out_columns(s)],
                send_sem.at[19],
                fin_sem.at[0, d, s],
                tensor_0=xs[d],
            ).start()
        pltpu.make_async_copy(
            fin.at[s, x], out.at[0, :, out_columns(s)], fin_sem.at[0, 0, s]
        ).start()

    n_ring = turns * 2 - 1
    arrived(x_wide.at[pl.ds(0, 3), :, 0], send_sem.at[0])
    arrived(z_part.at[0, :, 0], send_sem.at[1])
    arrived(fv_stage, send_sem.at[2])
    arrived(x_wide.at[pl.ds(0, n_ring)], send_sem.at[3])
    arrived(w2.at[pl.ds(0, share), pl.ds(0, width)], send_sem.at[4])
    arrived(z_part.at[pl.ds(0, n_ring), :, pl.ds(0, 2)], send_sem.at[5])
    arrived(z_part.at[:, :, pl.ds(0, 2)], send_sem.at[6])
    arrived(w2.at[pl.ds(0, share), pl.ds(0, width)], send_sem.at[7])
    arrived(fv_own.at[pl.ds(1, nz - 1)], send_sem.at[8])
    arrived(b_send, send_sem.at[10])
    arrived(wo2.at[pl.ds(0, 3 * hs), pl.ds(0, half)], send_sem.at[11])
    arrived(wo2.at[pl.ds(0, 3 * hs), pl.ds(0, half)], send_sem.at[12])
    arrived(wo_relay, send_sem.at[13])
    arrived(att.at[0], send_sem.at[14])
    arrived(att.at[0], send_sem.at[15])
    arrived(att.at[0, near], send_sem.at[16])
    arrived(att.at[0, far], send_sem.at[17])
    for s in range(subs):
        for d in range(NX):
            for piece in range(3):
                arrived(fin.at[s, x], fin_sem.at[piece, d, s])
    arrived(rs_send.at[pl.ds(0, n_ring)], send_sem.at[18])
    arrived(fin.at[:, pl.ds(0, 3)], send_sem.at[19])


def body(hidden_in, first_values, qkv_weight, out_weight, mix_table, mix_index, lengths, *, nz):
    rows, model = hidden_in.shape[1:]
    hs = qkv_weight.shape[2]
    quarter = model // NX
    half = quarter // 2
    halves = model // 2
    subs = quarter // SUB
    x_subs = max(1, halves * 4 // 10 // SUB)
    z_subs = 2
    z_wide = (halves - x_subs * SUB) // z_subs
    turns = nz // 2
    block = NX * rows
    vmem = pl.BlockSpec(memory_space=pltpu.VMEM)
    smem = pl.BlockSpec(memory_space=pltpu.SMEM)
    anywhere = pl.BlockSpec(memory_space=pl.ANY)
    dma = pltpu.SemaphoreType.DMA
    scratch = [
        pltpu.VMEM((nz, x_subs, NX, rows, SUB), BF),
        pltpu.VMEM((nz, z_subs, NX, rows, z_wide), BF),
        pltpu.VMEM((halves, 2 * 3 * hs), BF),
        pltpu.VMEM((NX * hs, quarter), BF),
        pltpu.VMEM((hs, half), BF),
        pltpu.VMEM((NX - 1, nz, rows, hs), BF),
        pltpu.VMEM((nz, NX, rows, hs), BF),
        pltpu.VMEM((nz, NX, rows, hs), BF),
        pltpu.VMEM((nz, block, 3 * hs), F32),
        pltpu.VMEM((nz, block, 3 * hs), BF),
        pltpu.VMEM((nz, block, 3 * hs), BF),
        pltpu.VMEM((NX, nz, rows, hs), BF),
        pltpu.VMEM((NX, nz, rows, hs), BF),
        pltpu.VMEM((NX, nz, rows, hs), BF),
        pltpu.VMEM((NX, nz, NX, rows, hs), BF),
        pltpu.VMEM((2 * turns, subs, NX, rows, SUB), BF),
        pltpu.VMEM((2, turns, subs, NX, rows, SUB), BF),
        pltpu.VMEM((2, subs, block, SUB), F32),
        pltpu.VMEM((subs, NX, rows, SUB), BF),
        dma((4,)),
        dma((20,)),
        dma((x_subs + z_subs,)),
        dma((NX, x_subs + z_subs)),
        dma((2, turns, x_subs + z_subs)),
        dma((nz, z_subs)),
        dma((2, 3)),
        dma((7,)),
        dma((NX,)),
        dma((nz,)),
        dma((nz,)),
        dma((4, NX)),
        dma((2, turns, subs)),
        dma((3, NX, subs)),
    ]
    result = pl.pallas_call(
        functools.partial(kernel, nz),
        out_shape=jax.ShapeDtypeStruct((3, rows, model), BF),
        in_specs=[vmem, vmem, anywhere, anywhere, smem, smem, smem],
        out_specs=anywhere,
        scratch_shapes=scratch,
        compiler_params=pltpu.CompilerParams(
            collective_id=0, has_side_effects=True, vmem_limit_bytes=60 * 1024 * 1024
        ),
    )(
        hidden_in[0],
        first_values[0],
        jnp.transpose(qkv_weight, (1, 0, 2)),
        out_weight,
        mix_table.T,
        mix_index,
        lengths,
    )
    first, second, third = (piece.astype(F32) for piece in result)
    return (first + second + third).astype(BF)[None]


def solution(mesh):
    nz = mesh.shape["tensor"] // NX
    torus = Mesh(
        mesh.devices.reshape(mesh.shape["groups"], mesh.shape["dp"], NX, nz),
        ("groups", "dp", "tensor_0", "tensor_1"),
    )
    placed = (
        P(("groups", "dp"), TENSOR, None),
        P(("groups", "dp"), TENSOR, None),
        P(None, None, TENSOR),
        P(TENSOR, None),
        P(),
        P(TENSOR),
        P(("groups", "dp")),
    )
    return jax.shard_map(
        functools.partial(body, nz=nz),
        mesh=torus,
        in_specs=placed,
        out_specs=P(("groups", "dp"), TENSOR, None),
        check_vma=False,
    )
```

```python
import functools
import math

import jax
import jax.numpy as jnp
from jax import lax
from jax.experimental import pallas as pl
from jax.experimental.pallas import tpu as pltpu
from jax.sharding import Mesh
from jax.sharding import PartitionSpec as P

TENSOR = ("tensor_0", "tensor_1")
NEG_FILL = -1e30
BF = jnp.bfloat16
F32 = jnp.float32
NX = 4
SUB = 256
LAG = 3


def kernel(
    nz,
    hid,
    firsts,
    w_qkv,
    w_out,
    mix_table,
    mix_index,
    lengths,
    out,
    x_wide,
    z_part,
    w2,
    wo2,
    wo_relay,
    fv_stage,
    fv_own,
    fv_in,
    stash,
    b_send,
    b_recv,
    q_buf,
    k_buf,
    v_buf,
    att,
    rs_send,
    rs_recv,
    own_term,
    fin,
    local_sem,
    send_sem,
    own_sem,
    hid_sem,
    ag_sem,
    oz_sem,
    w_sem,
    wo_sem,
    fx_sem,
    fz_sem,
    b_sem,
    att_sem,
    rs_sem,
    fin_sem,
):
    rows, model = hid.shape
    hs = w_qkv.shape[2]
    quarter = model // NX
    half = quarter // 2
    halves = model // 2
    subs = quarter // SUB
    turns = nz // 2
    block = NX * rows

    x = lax.axis_index("tensor_0")
    z = lax.axis_index("tensor_1")
    core = lax.axis_index("dp")
    xs = [x] + [lax.rem(x + d, NX) for d in range(1, NX)]
    z_up = lax.rem(z + 1, nz)
    z_down = lax.rem(z + nz - 1, nz)
    x_way = lax.rem(x + 1 + 2 * core, NX)
    odd = lax.rem(x, 2)
    pair = x + 1 - 2 * odd
    other = lax.rem(x + NX - 1 + 2 * odd, NX)

    def remote(src, dst, send, recv, **where):
        return pltpu.make_async_remote_copy(
            src_ref=src,
            dst_ref=dst,
            send_sem=send,
            recv_sem=recv,
            device_id=where,
            device_id_type=pl.DeviceIdType.MESH,
        )

    def arrived(ref, sem):
        pltpu.make_async_copy(ref, ref, sem).wait()

    barrier = pltpu.get_barrier_semaphore()
    partners = [
        {"dp": 1 - core},
        {"tensor_0": xs[1]},
        {"tensor_0": xs[2]},
        {"tensor_0": xs[3]},
        {"tensor_1": z_up},
        {"tensor_1": z_down},
    ]
    for partner in partners:
        pl.semaphore_signal(
            barrier, inc=1, device_id=partner, device_id_type=pl.DeviceIdType.MESH
        )
    pl.semaphore_wait(barrier, len(partners))

    def half_of(at):
        return lax.rem((at + 1) // 2, 2)

    mine, theirs = half_of(x), 1 - half_of(x)
    stripes, other_stripes = pl.ds(x - odd, 2), pl.ds(NX - 2 - x + odd, 2)
    x_subs, z_subs, z_wide = x_wide.shape[1], z_part.shape[1], z_part.shape[4]

    def x_columns(to_half, s):
        return pl.ds(pl.multiple_of(to_half * halves + s * SUB, 128), SUB)

    def z_columns(to_half, s):
        return pl.ds(pl.multiple_of(to_half * halves + x_subs * SUB + s * z_wide, 128), z_wide)

    def hidden_out(d, to, to_half):
        for s in range(x_subs):
            remote(
                hid.at[:, x_columns(to_half, s)],
                x_wide.at[0, s, x],
                send_sem.at[0],
                hid_sem.at[d, s],
                tensor_0=to,
            ).start()

    for s in range(z_subs):
        remote(
            hid.at[:, z_columns(theirs, s)],
            z_part.at[0, s, x],
            send_sem.at[1],
            hid_sem.at[0, s],
            tensor_0=pair,
        ).start()
    hidden_out(1, pair, theirs)
    hidden_out(2, other, mine)
    hidden_out(3, xs[2], theirs)
    own_hidden = []
    for s in range(z_subs):
        own_hidden.append(
            pltpu.make_async_copy(
                hid.at[:, z_columns(mine, s)], z_part.at[0, s, x], own_sem.at[s]
            )
        )
    for s in range(x_subs):
        own_hidden.append(
            pltpu.make_async_copy(
                hid.at[:, x_columns(mine, s)], x_wide.at[0, s, x], own_sem.at[z_subs + s]
            )
        )
    for copy in own_hidden:
        copy.start()

    def stage_firsts(head, carry):
        away = lax.rem(head - z + nz, nz)
        for d in range(NX):
            column = pl.multiple_of((xs[d] * nz + head) * hs, 128)
            piece = firsts[:, pl.ds(column, hs)]
            if d == 0:
                fv_own[away, x] = piece
            else:
                fv_stage[d - 1, away] = piece
        return carry

    lax.fori_loop(0, nz, stage_firsts, 0)
    for d in (1, 2, 3):
        remote(
            fv_stage.at[d - 1],
            fv_own.at[:, x],
            send_sem.at[2],
            fx_sem.at[d],
            tensor_0=xs[d],
        ).start()

    share = halves // 2
    my_share = pl.multiple_of(core * share, 128)
    sibling_share = pl.multiple_of((1 - core) * share, 128)
    for p in range(3):
        remote(
            w_qkv.at[p, pl.ds(pl.multiple_of(theirs * halves + core * share, 128), share)],
            w2.at[pl.ds(my_share, share), pl.ds((3 + p) * hs, hs)],
            send_sem.at[4],
            w_sem.at[0, p],
            tensor_0=pair,
        ).start()
    own_weights = []
    for p in range(3):
        own_weights.append(
            pltpu.make_async_copy(
                w_qkv.at[p, pl.ds(pl.multiple_of(mine * halves, 128), halves)],
                w2.at[:, pl.ds(p * hs, hs)],
                local_sem.at[p],
            )
        )
    own_weights.append(
        pltpu.make_async_copy(
            w_out.at[:, pl.ds(pl.multiple_of(x * quarter, 128), quarter)],
            wo2.at[pl.ds(0, hs)],
            local_sem.at[3],
        )
    )
    for copy in own_weights:
        copy.start()

    my_half = pl.multiple_of(core * half, 128)

    def wo_columns(to):
        return pl.ds(pl.multiple_of(to * quarter + core * half, 128), half)

    def wo_piece(r):
        return wo2.at[pl.ds(r * hs, hs), pl.ds(my_half, half)]

    def out_weights_send():
        remote(
            w_out.at[:, wo_columns(xs[2])], wo_relay, send_sem.at[11], wo_sem.at[0], tensor_0=x_way
        ).start()
        for d, r, sem in ((1, 3, 1), (3, 1, 2)):
            remote(
                w_out.at[:, wo_columns(xs[d])],
                wo_piece(r),
                send_sem.at[11],
                wo_sem.at[sem],
                tensor_0=xs[d],
            ).start()

    def out_to_sibling(r):
        remote(
            wo_piece(r), wo_piece(r), send_sem.at[12], wo_sem.at[3 + r], dp=1 - core
        ).start()

    def out_weights_relay():
        arrived(wo_relay, wo_sem.at[0])
        remote(wo_relay, wo_piece(2), send_sem.at[13], wo_sem.at[3], tensor_0=x_way).start()

    def out_weights_direct():
        for r, sem in ((3, 1), (1, 2)):
            arrived(wo_piece(r), wo_sem.at[sem])
            out_to_sibling(r)

    def out_weights_last():
        arrived(wo_piece(2), wo_sem.at[3])
        out_to_sibling(2)

    def out_weights_wait():
        other = pl.multiple_of((1 - core) * half, 128)
        for r in (1, 2, 3):
            arrived(wo2.at[pl.ds(r * hs, hs), pl.ds(other, half)], wo_sem.at[3 + r])

    out_weights_send()

    flows = [(0, s) for s in range(x_subs)] + [(1, s) for s in range(z_subs)]

    def longer(way, n):
        return turns if (n % 2 == 0) == (way == 0) else turns - 1

    def part(n, place):
        kind, s = flows[n]
        return x_wide.at[place, s] if kind == 0 else z_part.at[place, s, stripes]

    def ring_send(n, way, step):
        source, target = (step - 1, step) if way else ((nz - step + 1) % nz, nz - step)
        remote(
            part(n, source),
            part(n, target),
            send_sem.at[3 if flows[n][0] == 0 else 5],
            ag_sem.at[way, step - 1, n],
            tensor_1=z_down if way else z_up,
        ).start()

    def to_other(n, place):
        kind, s = flows[n]
        if kind == 1:
            remote(
                z_part.at[place, s, stripes],
                z_part.at[place, s, stripes],
                send_sem.at[6],
                oz_sem.at[place, s],
                tensor_0=other,
            ).start()

    def gather_step(step):
        for n in range(len(flows)):
            for way in (0, 1):
                if step <= longer(way, n):
                    place = step if way else nz - step
                    arrived(part(n, place), ag_sem.at[way, step - 1, n])
                    if step + 1 <= longer(way, n):
                        ring_send(n, way, step + 1)
                    to_other(n, place)

    def weights_step(p):
        here = w2.at[pl.ds(my_share, share), pl.ds((3 + p) * hs, hs)]
        arrived(here, w_sem.at[0, p])
        remote(here, here, send_sem.at[7], w_sem.at[1, p], dp=1 - core).start()

    def weights_last():
        for p in range(3):
            arrived(
                w2.at[pl.ds(sibling_share, share), pl.ds((3 + p) * hs, hs)], w_sem.at[1, p]
            )
        for copy in own_weights:
            copy.wait()

    def firsts_step(step):
        if step == 1:
            for d in (1, 2, 3):
                arrived(fv_stage.at[d - 1], fx_sem.at[d])
        for away in sorted({step, nz - step}):
            remote(
                fv_own.at[away],
                fv_in.at[nz - away],
                send_sem.at[8],
                fz_sem.at[nz - away],
                tensor_1=lax.rem(z + away, nz),
            ).start()

    for copy in own_hidden:
        copy.wait()
    for s in range(z_subs):
        arrived(z_part.at[0, s, pair], hid_sem.at[0, s])
        ring_send(x_subs + s, 0, 1)
        ring_send(x_subs + s, 1, 1)
        to_other(x_subs + s, 0)
    for s in range(x_subs):
        for d in (1, 2, 3):
            arrived(x_wide.at[0, s, x], hid_sem.at[d, s])
        ring_send(s, 0, 1)
        ring_send(s, 1, 1)
    early = max(turns - 3, 0)
    weights_after = {2: (0,), 3: (1,), 4: (2,)}
    for step in range(1, early + 1):
        gather_step(step)
        for p in weights_after.get(step, ()):
            weights_step(p)
    for p in range(3):
        if not any(p in done for step, done in weights_after.items() if step <= early):
            weights_step(p)
    weights_last()

    width = 3 * hs

    def place_of(i):
        return jnp.where(i % 2 == 1, (i + 1) // 2, lax.rem(nz - i // 2, nz))

    def project(i):
        place = place_of(i)
        for s in range(z_subs):
            arrived(z_part.at[place, s, other_stripes], oz_sem.at[place, s])
        lhs = jnp.concatenate(
            [x_wide[place, s].reshape(block, SUB) for s in range(x_subs)]
            + [z_part[place, s].reshape(block, z_wide) for s in range(z_subs)],
            axis=1,
        )
        term = jnp.dot(lhs, w2[...], preferred_element_type=F32)
        b_send[i] = term[:, width:].astype(BF)
        remote(
            b_send.at[i], b_recv.at[i], send_sem.at[10], b_sem.at[i], tensor_0=pair
        ).start()
        stash[i] = term[:, :width]

    def finish(i):
        arrived(b_recv.at[i], b_sem.at[i])
        total = stash[i] + b_recv[i].astype(F32)
        total = total.astype(BF).reshape(NX, rows, width)
        origin = lax.rem(z + place_of(i), nz)
        q_buf[:, origin] = total[:, :, :hs]
        k_buf[:, origin] = total[:, :, hs : 2 * hs]
        v_buf[:, origin] = total[:, :, 2 * hs :]

    trips = nz + LAG
    late = {}

    def at_trip(i, *steps):
        late.setdefault(min(i, trips - 1), []).extend(steps)

    for step, at in zip(range(early + 1, turns + 1), (2, 7, 12)):
        at_trip(min(at, 2 * step - 1), functools.partial(gather_step, step))
        if step == turns:
            at_trip(
                min(at, 2 * step - 1),
                *(functools.partial(firsts_step, away) for away in range(1, turns + 1)),
            )
    at_trip(4, out_weights_relay)
    at_trip(6, out_weights_direct)
    at_trip(12, out_weights_last)

    def trip(i, carry):
        for at, steps in late.items():

            @pl.when(i == at)
            def _(steps=steps):
                for step in steps:
                    step()

        @pl.when(i < nz)
        def _():
            project(i)

        @pl.when(i >= LAG)
        def _():
            finish(i - LAG)

        return carry

    lax.fori_loop(0, trips, trip, 0)
    out_weights_wait()

    row = mix_index[0]
    weight_now = mix_table[0, row]
    weight_first = mix_table[1, row]

    def mix(origin, first):
        now = v_buf[:, origin].astype(F32)
        v_buf[:, origin] = (weight_now * now + weight_first * first.astype(F32)).astype(BF)

    mix(z, fv_own[0])
    for away in range(1, nz):
        arrived(fv_in.at[away], fz_sem.at[away])
        mix(lax.rem(z + away, nz), fv_in[away])

    scale = 1.0 / math.sqrt(hs)
    valid = lengths[0]
    stripe = nz * rows
    q_blocks = min(nz, 128 // rows)
    q_rows = q_blocks * rows

    def attend(b):
        n = (b + 1) * stripe
        keys = k_buf[0 : b + 1].reshape(n, hs)
        values = v_buf[0 : b + 1].reshape(n, hs)

        def one(t, carry):
            at = pl.ds(t * q_blocks, q_blocks)
            query = q_buf[b, at].reshape(q_rows, hs)
            scores = (
                lax.dot_general(query, keys, (((1,), (1,)), ((), ())), preferred_element_type=F32)
                * scale
            )
            col = lax.broadcasted_iota(jnp.int32, (q_rows, n), 1)
            line = b * stripe + t * q_rows + lax.broadcasted_iota(jnp.int32, (q_rows, n), 0)
            scores = jnp.where((col <= line) & (col < valid), scores, NEG_FILL)
            raised = jnp.exp(scores - jnp.max(scores, axis=1, keepdims=True))
            weights = (raised * (1.0 / jnp.sum(raised, axis=1, keepdims=True))).astype(BF)
            result = jnp.dot(weights, values, preferred_element_type=F32).astype(BF)
            att[0, at, b] = result.reshape(q_blocks, rows, hs)
            return carry

        lax.fori_loop(0, nz // q_blocks, one, 0)

    near, far = pl.ds(0, nz // 2), pl.ds(nz // 2, nz // 2)

    def att_send(b):
        remote(
            att.at[0, :, b], att.at[3, :, b], send_sem.at[14], att_sem.at[0, b], tensor_0=xs[1]
        ).start()
        remote(
            att.at[0, :, b], att.at[1, :, b], send_sem.at[15], att_sem.at[1, b], tensor_0=xs[3]
        ).start()

    def att_pass(b):
        arrived(att.at[3, :, b], att_sem.at[0, b])
        remote(
            att.at[3, near, b], att.at[2, near, b], send_sem.at[16], att_sem.at[2, b], tensor_0=xs[1]
        ).start()
        arrived(att.at[1, :, b], att_sem.at[1, b])
        remote(
            att.at[1, far, b], att.at[2, far, b], send_sem.at[17], att_sem.at[3, b], tensor_0=xs[3]
        ).start()

    my_columns = pl.ds(pl.multiple_of(x * quarter, 128), quarter)

    def length_of(way, b):
        return turns if (b % 2 == 0) == (way == 0) else turns - 1

    def ready(b):
        arrived(att.at[2, near, b], att_sem.at[2, b])
        arrived(att.at[2, far, b], att_sem.at[3, b])
        lhs = jnp.concatenate([att[r, :, b].reshape(stripe, hs) for r in range(NX)], axis=1)
        for s in range(subs):
            column = slice(s * SUB, (s + 1) * SUB)
            term = jnp.dot(lhs, wo2[:, column], preferred_element_type=F32)
            own_term[b, :, :, column] = term.reshape(nz, rows, SUB)
        fin[b] = own_term[b, z].astype(BF)

    def reduce_step(b, step):
        for way in (0, 1):
            length = length_of(way, b)
            slot = (2 * b + way) * turns + step
            z_next = z_down if way else z_up

            def one(b=b, way=way, length=length, slot=slot, z_next=z_next):
                target = lax.rem(z + (1 - 2 * way) * (length - step + 1) + nz, nz)
                term = own_term[b, target]
                if not (isinstance(step, int) and step == 1):
                    arrived(rs_recv.at[slot - 1], rs_sem.at[slot - 1])
                    term = term + rs_recv[slot - 1].astype(F32)
                rs_send[slot - 1] = term.astype(BF)

                def go_on():
                    remote(
                        rs_send.at[slot - 1],
                        rs_recv.at[slot],
                        send_sem.at[18],
                        rs_sem.at[slot],
                        tensor_1=z_next,
                    ).start()

                def deliver():
                    remote(
                        rs_send.at[slot - 1],
                        out.at[1 + way, :, my_columns],
                        send_sem.at[18],
                        fin_sem.at[1 + way, lax.rem(b - x + NX, NX)],
                        tensor_0=jnp.int32(b),
                        tensor_1=z_next,
                    ).start()

                if isinstance(step, int):
                    (go_on if step < length else deliver)()
                else:
                    pl.when(step < length)(go_on)
                    pl.when(step == length)(deliver)

            if isinstance(step, int):
                if step <= length:
                    one()
            else:
                pl.when(step <= length)(one)

    for b in range(NX):
        attend(b)
        att_send(b)
    att_pass(0)
    for b in range(NX):
        if b + 1 < NX:
            att_pass(b + 1)
        ready(b)
        for back in range(b + 1):
            reduce_step(b - back, 1 + back)
    for d in (1, 2, 3):
        remote(
            fin.at[xs[d]],
            out.at[0, :, my_columns],
            send_sem.at[19],
            fin_sem.at[0, d],
            tensor_0=xs[d],
        ).start()
    pltpu.make_async_copy(fin.at[x], out.at[0, :, my_columns], fin_sem.at[0, 0]).start()

    def reduce_round(step, carry):
        for b in reversed(range(NX)):
            reduce_step(b, step + NX - 1 - b)
        return carry

    lax.fori_loop(2, turns + 1, reduce_round, 0)

    n_ring = turns * 2 - 1
    arrived(x_wide.at[pl.ds(0, 3), :, 0], send_sem.at[0])
    arrived(z_part.at[0, :, 0], send_sem.at[1])
    arrived(fv_stage, send_sem.at[2])
    arrived(x_wide.at[pl.ds(0, n_ring)], send_sem.at[3])
    arrived(w2.at[pl.ds(0, share), pl.ds(0, width)], send_sem.at[4])
    arrived(z_part.at[pl.ds(0, n_ring), :, pl.ds(0, 2)], send_sem.at[5])
    arrived(z_part.at[:, :, pl.ds(0, 2)], send_sem.at[6])
    arrived(w2.at[pl.ds(0, share), pl.ds(0, width)], send_sem.at[7])
    arrived(fv_own.at[pl.ds(1, nz - 1)], send_sem.at[8])
    arrived(b_send, send_sem.at[10])
    arrived(wo2.at[pl.ds(0, 3 * hs), pl.ds(0, half)], send_sem.at[11])
    arrived(wo2.at[pl.ds(0, 3 * hs), pl.ds(0, half)], send_sem.at[12])
    arrived(wo_relay, send_sem.at[13])
    arrived(att.at[0], send_sem.at[14])
    arrived(att.at[0], send_sem.at[15])
    arrived(att.at[0, near], send_sem.at[16])
    arrived(att.at[0, far], send_sem.at[17])
    for d in range(NX):
        for piece in range(3):
            arrived(fin.at[0], fin_sem.at[piece, d])
    arrived(rs_send.at[pl.ds(0, NX * n_ring)], send_sem.at[18])
    arrived(fin.at[pl.ds(0, 3)], send_sem.at[19])


def body(hidden_in, first_values, qkv_weight, out_weight, mix_table, mix_index, lengths, *, nz):
    rows, model = hidden_in.shape[1:]
    hs = qkv_weight.shape[2]
    quarter = model // NX
    half = quarter // 2
    halves = model // 2
    subs = quarter // SUB
    x_subs = max(1, halves * 4 // 10 // SUB)
    z_subs = 2
    z_wide = (halves - x_subs * SUB) // z_subs
    turns = nz // 2
    block = NX * rows
    vmem = pl.BlockSpec(memory_space=pltpu.VMEM)
    smem = pl.BlockSpec(memory_space=pltpu.SMEM)
    anywhere = pl.BlockSpec(memory_space=pl.ANY)
    dma = pltpu.SemaphoreType.DMA
    scratch = [
        pltpu.VMEM((nz, x_subs, NX, rows, SUB), BF),
        pltpu.VMEM((nz, z_subs, NX, rows, z_wide), BF),
        pltpu.VMEM((halves, 2 * 3 * hs), BF),
        pltpu.VMEM((NX * hs, quarter), BF),
        pltpu.VMEM((hs, half), BF),
        pltpu.VMEM((NX - 1, nz, rows, hs), BF),
        pltpu.VMEM((nz, NX, rows, hs), BF),
        pltpu.VMEM((nz, NX, rows, hs), BF),
        pltpu.VMEM((nz, block, 3 * hs), F32),
        pltpu.VMEM((nz, block, 3 * hs), BF),
        pltpu.VMEM((nz, block, 3 * hs), BF),
        pltpu.VMEM((NX, nz, rows, hs), BF),
        pltpu.VMEM((NX, nz, rows, hs), BF),
        pltpu.VMEM((NX, nz, rows, hs), BF),
        pltpu.VMEM((NX, nz, NX, rows, hs), BF),
        pltpu.VMEM((NX * 2 * turns, rows, quarter), BF),
        pltpu.VMEM((NX * 2 * turns, rows, quarter), BF),
        pltpu.VMEM((NX, nz, rows, quarter), F32),
        pltpu.VMEM((NX, rows, quarter), BF),
        dma((4,)),
        dma((20,)),
        dma((x_subs + z_subs,)),
        dma((NX, x_subs + z_subs)),
        dma((2, turns, x_subs + z_subs)),
        dma((nz, z_subs)),
        dma((2, 3)),
        dma((7,)),
        dma((NX,)),
        dma((nz,)),
        dma((nz,)),
        dma((4, NX)),
        dma((NX * 2 * turns,)),
        dma((3, NX)),
    ]
    result = pl.pallas_call(
        functools.partial(kernel, nz),
        out_shape=jax.ShapeDtypeStruct((3, rows, model), BF),
        in_specs=[vmem, vmem, anywhere, anywhere, smem, smem, smem],
        out_specs=anywhere,
        scratch_shapes=scratch,
        compiler_params=pltpu.CompilerParams(
            collective_id=0, has_side_effects=True, vmem_limit_bytes=60 * 1024 * 1024
        ),
    )(
        hidden_in[0],
        first_values[0],
        jnp.transpose(qkv_weight, (1, 0, 2)),
        out_weight,
        mix_table.T,
        mix_index,
        lengths,
    )
    first, second, third = (piece.astype(F32) for piece in result)
    return (first + second + third).astype(BF)[None]


def solution(mesh):
    nz = mesh.shape["tensor"] // NX
    torus = Mesh(
        mesh.devices.reshape(mesh.shape["groups"], mesh.shape["dp"], NX, nz),
        ("groups", "dp", "tensor_0", "tensor_1"),
    )
    placed = (
        P(("groups", "dp"), TENSOR, None),
        P(("groups", "dp"), TENSOR, None),
        P(None, None, TENSOR),
        P(TENSOR, None),
        P(),
        P(TENSOR),
        P(("groups", "dp")),
    )
    return jax.shard_map(
        functools.partial(body, nz=nz),
        mesh=torus,
        in_specs=placed,
        out_specs=P(("groups", "dp"), TENSOR, None),
        check_vma=False,
    )
```

```python
import functools
import math

import jax
import jax.numpy as jnp
from jax import lax
from jax.experimental import pallas as pl
from jax.experimental.pallas import tpu as pltpu
from jax.sharding import Mesh
from jax.sharding import PartitionSpec as P

TENSOR = ("tensor_0", "tensor_1")
NEG_FILL = -1e30
BF = jnp.bfloat16
F32 = jnp.float32
NX = 4
SUB = 256
LAG = 3


def kernel(
    nz,
    hid,
    firsts,
    w_qkv,
    w_out,
    mix_table,
    mix_index,
    lengths,
    out,
    x_wide,
    z_part,
    w2,
    wo2,
    wo_relay,
    fv_stage,
    fv_own,
    fv_in,
    stash,
    b_send,
    b_recv,
    q_buf,
    k_buf,
    v_buf,
    att,
    rs_send,
    rs_recv,
    own_term,
    fin,
    local_sem,
    send_sem,
    own_sem,
    hid_sem,
    ag_sem,
    oz_sem,
    w_sem,
    wo_sem,
    fx_sem,
    fz_sem,
    b_sem,
    att_sem,
    rs_sem,
    fin_sem,
):
    rows, model = hid.shape
    hs = w_qkv.shape[2]
    quarter = model // NX
    half = quarter // 2
    halves = model // 2
    subs = quarter // SUB
    turns = nz // 2
    block = NX * rows

    x = lax.axis_index("tensor_0")
    z = lax.axis_index("tensor_1")
    core = lax.axis_index("dp")
    xs = [x] + [lax.rem(x + d, NX) for d in range(1, NX)]
    z_up = lax.rem(z + 1, nz)
    z_down = lax.rem(z + nz - 1, nz)
    x_way = lax.rem(x + 1 + 2 * core, NX)
    odd = lax.rem(x, 2)
    pair = x + 1 - 2 * odd
    other = lax.rem(x + NX - 1 + 2 * odd, NX)

    def remote(src, dst, send, recv, **where):
        return pltpu.make_async_remote_copy(
            src_ref=src,
            dst_ref=dst,
            send_sem=send,
            recv_sem=recv,
            device_id=where,
            device_id_type=pl.DeviceIdType.MESH,
        )

    def arrived(ref, sem):
        pltpu.make_async_copy(ref, ref, sem).wait()

    barrier = pltpu.get_barrier_semaphore()
    partners = [
        {"dp": 1 - core},
        {"tensor_0": xs[1]},
        {"tensor_0": xs[2]},
        {"tensor_0": xs[3]},
        {"tensor_1": z_up},
        {"tensor_1": z_down},
    ]
    for partner in partners:
        pl.semaphore_signal(
            barrier, inc=1, device_id=partner, device_id_type=pl.DeviceIdType.MESH
        )
    pl.semaphore_wait(barrier, len(partners))

    def half_of(at):
        return lax.rem((at + 1) // 2, 2)

    mine, theirs = half_of(x), 1 - half_of(x)
    stripes, other_stripes = pl.ds(x - odd, 2), pl.ds(NX - 2 - x + odd, 2)
    x_subs, z_subs, z_wide = x_wide.shape[1], z_part.shape[1], z_part.shape[4]

    def x_columns(to_half, s):
        return pl.ds(pl.multiple_of(to_half * halves + s * SUB, 128), SUB)

    def z_columns(to_half, s):
        return pl.ds(pl.multiple_of(to_half * halves + x_subs * SUB + s * z_wide, 128), z_wide)

    def hidden_out(d, to, to_half):
        for s in range(x_subs):
            remote(
                hid.at[:, x_columns(to_half, s)],
                x_wide.at[0, s, x],
                send_sem.at[0],
                hid_sem.at[d],
                tensor_0=to,
            ).start()

    for s in range(z_subs):
        remote(
            hid.at[:, z_columns(theirs, s)],
            z_part.at[0, s, x],
            send_sem.at[1],
            hid_sem.at[0],
            tensor_0=pair,
        ).start()
    hidden_out(1, pair, theirs)
    hidden_out(2, other, mine)
    hidden_out(3, xs[2], theirs)
    for s in range(z_subs):
        pltpu.make_async_copy(
            hid.at[:, z_columns(mine, s)], z_part.at[0, s, x], own_sem.at[0]
        ).start()
    for s in range(x_subs):
        pltpu.make_async_copy(
            hid.at[:, x_columns(mine, s)], x_wide.at[0, s, x], own_sem.at[1]
        ).start()

    flows = [(0, s, min(2, x_subs - s)) for s in range(0, x_subs, 2)]
    flows += [(1, s, 1) for s in range(z_subs)]

    def longer(way, n):
        return turns if (n % 2 == 0) == (way == 0) else turns - 1

    def part(n, place):
        kind, s, count = flows[n]
        if kind == 0:
            return x_wide.at[place, pl.ds(s, count)]
        return z_part.at[place, s, stripes]

    def ring_send(n, way, step, source, target):
        remote(
            source,
            target,
            send_sem.at[3 if flows[n][0] == 0 else 5],
            ag_sem.at[way, step - 1, n],
            tensor_1=z_down if way else z_up,
        ).start()

    def other_send(place, s, source, target):
        remote(source, target, send_sem.at[6], oz_sem.at[place], tensor_0=other).start()

    for n, (kind, first, count) in enumerate(flows):
        for s in range(first, first + count):
            for way in (0, 1):
                target = 1 if way else nz - 1
                if kind == 0:
                    ring_send(n, way, 1, hid.at[:, x_columns(mine, s)], x_wide.at[target, s, x])
                else:
                    ring_send(n, way, 1, hid.at[:, z_columns(mine, s)], z_part.at[target, s, x])
            if kind == 1:
                other_send(0, s, hid.at[:, z_columns(mine, s)], z_part.at[0, s, x])

    def stage_firsts(head, carry):
        away = lax.rem(head - z + nz, nz)
        for d in range(NX):
            column = pl.multiple_of((xs[d] * nz + head) * hs, 128)
            piece = firsts[:, pl.ds(column, hs)]
            if d == 0:
                fv_own[away, x] = piece
            else:
                fv_stage[d - 1, away] = piece
        return carry

    lax.fori_loop(0, nz, stage_firsts, 0)
    for d in (1, 2, 3):
        remote(
            fv_stage.at[d - 1],
            fv_own.at[:, x],
            send_sem.at[2],
            fx_sem.at[0],
            tensor_0=xs[d],
        ).start()

    share = halves // 2
    my_share = pl.multiple_of(core * share, 128)
    sibling_share = pl.multiple_of((1 - core) * share, 128)
    for p in range(3):
        remote(
            w_qkv.at[p, pl.ds(pl.multiple_of(theirs * halves + core * share, 128), share)],
            w2.at[pl.ds(my_share, share), pl.ds((3 + p) * hs, hs)],
            send_sem.at[4],
            w_sem.at[0, p],
            tensor_0=pair,
        ).start()
    own_weights = []
    for p in range(3):
        own_weights.append(
            pltpu.make_async_copy(
                w_qkv.at[p, pl.ds(pl.multiple_of(mine * halves, 128), halves)],
                w2.at[:, pl.ds(p * hs, hs)],
                local_sem.at[0],
            )
        )
    own_weights.append(
        pltpu.make_async_copy(
            w_out.at[:, pl.ds(pl.multiple_of(x * quarter, 128), quarter)],
            wo2.at[pl.ds(0, hs)],
            local_sem.at[1],
        )
    )
    for copy in own_weights:
        copy.start()

    my_half = pl.multiple_of(core * half, 128)

    def wo_columns(to):
        return pl.ds(pl.multiple_of(to * quarter + core * half, 128), half)

    def wo_piece(r):
        return wo2.at[pl.ds(pl.multiple_of(r * hs, hs), hs), pl.ds(my_half, half)]

    from_pair, from_other = 1 + 2 * odd, 3 - 2 * odd

    def out_weights_send():
        remote(
            w_out.at[:, wo_columns(pair)], wo_piece(from_other), send_sem.at[11], wo_sem.at[1], tensor_0=pair
        ).start()
        remote(
            w_out.at[:, wo_columns(xs[2])], wo_relay, send_sem.at[11], wo_sem.at[0], tensor_0=pair
        ).start()

    def out_weights_late():
        remote(
            w_out.at[:, wo_columns(other)], wo_piece(from_pair), send_sem.at[11], wo_sem.at[2], tensor_0=other
        ).start()
        arrived(wo_relay, wo_sem.at[0])
        remote(wo_relay, wo_piece(2), send_sem.at[13], wo_sem.at[3], tensor_0=other).start()

    def out_to_sibling(r, sem):
        arrived(wo_piece(r), wo_sem.at[sem])
        remote(
            wo_piece(r), wo_piece(r), send_sem.at[12], wo_sem.at[3 + sem], dp=1 - core
        ).start()

    def out_weights_wait():
        for sem in (1, 2, 3):
            arrived(wo_piece(0), wo_sem.at[3 + sem])

    out_weights_send()

    def gather_step(step):
        for n in range(len(flows)):
            for way in (0, 1):
                if step <= longer(way, n):
                    place = step if way else nz - step
                    arrived(part(n, place), ag_sem.at[way, step - 1, n])
                    if step + 1 <= longer(way, n):
                        onward = step + 1 if way else nz - step - 1
                        ring_send(n, way, step + 1, part(n, place), part(n, onward))
                    if flows[n][0] == 1:
                        other_send(place, flows[n][1], part(n, place), part(n, place))

    def weights_step(p):
        here = w2.at[pl.ds(my_share, share), pl.ds((3 + p) * hs, hs)]
        arrived(here, w_sem.at[0, p])
        remote(here, here, send_sem.at[7], w_sem.at[1, p], dp=1 - core).start()

    def weights_last():
        for p in range(3):
            arrived(
                w2.at[pl.ds(sibling_share, share), pl.ds((3 + p) * hs, hs)], w_sem.at[1, p]
            )
        arrived(w2.at[:, pl.ds(0, 3 * hs)], local_sem.at[0])
        arrived(wo2.at[pl.ds(0, hs)], local_sem.at[1])

    def firsts_step(step):
        if step == 1:
            arrived(fv_stage, fx_sem.at[0])
        for away in sorted({step, nz - step}):
            remote(
                fv_own.at[away],
                fv_in.at[nz - away],
                send_sem.at[8],
                fz_sem.at[0],
                tensor_1=lax.rem(z + away, nz),
            ).start()

    arrived(z_part.at[0, :, x], hid_sem.at[0])
    for n, (kind, first, count) in enumerate(flows):
        if kind == 1:
            piece = z_part.at[0, first, pair]
            ring_send(n, 0, 1, piece, z_part.at[nz - 1, first, pair])
            ring_send(n, 1, 1, piece, z_part.at[1, first, pair])
            other_send(0, first, piece, piece)
    for d in (1, 2, 3):
        arrived(x_wide.at[0, :, x], hid_sem.at[d])
    for n, (kind, first, count) in enumerate(flows):
        if kind == 0:
            for d in (1, 2, 3):
                at = pl.ds(first, count)
                piece = x_wide.at[0, at, xs[d]]
                ring_send(n, 0, 1, piece, x_wide.at[nz - 1, at, xs[d]])
                ring_send(n, 1, 1, piece, x_wide.at[1, at, xs[d]])
    arrived(z_part.at[0, :, x], own_sem.at[0])
    arrived(x_wide.at[0, :, x], own_sem.at[1])
    early = max(turns - 3, 0)
    weights_after = {2: (0,), 3: (1,), 4: (2,)}
    for step in range(1, early + 1):
        gather_step(step)
        for p in weights_after.get(step, ()):
            weights_step(p)
    for p in range(3):
        if not any(p in done for step, done in weights_after.items() if step <= early):
            weights_step(p)
    weights_last()

    width = 3 * hs

    def place_of(i):
        return jnp.where(i % 2 == 1, (i + 1) // 2, lax.rem(nz - i // 2, nz))

    def project(i):
        place = place_of(i)
        arrived(z_part.at[place, :, other_stripes], oz_sem.at[place])
        lhs = jnp.concatenate(
            [x_wide[place, s].reshape(block, SUB) for s in range(x_subs)]
            + [z_part[place, s].reshape(block, z_wide) for s in range(z_subs)],
            axis=1,
        )
        term = jnp.dot(lhs, w2[...], preferred_element_type=F32)
        b_send[i] = term[:, width:].astype(BF)
        remote(
            b_send.at[i], b_recv.at[i], send_sem.at[10], b_sem.at[i], tensor_0=pair
        ).start()
        stash[i] = term[:, :width]

    def finish(i):
        arrived(b_recv.at[i], b_sem.at[i])
        total = stash[i] + b_recv[i].astype(F32)
        total = total.astype(BF).reshape(NX, rows, width)
        origin = lax.rem(z + place_of(i), nz)
        q_buf[:, origin] = total[:, :, :hs]
        k_buf[:, origin] = total[:, :, hs : 2 * hs]
        v_buf[:, origin] = total[:, :, 2 * hs :]

    trips = nz + LAG
    late = {}

    def at_trip(i, *steps):
        late.setdefault(min(i, trips - 1), []).extend(steps)

    for step, at in zip(range(early + 1, turns + 1), (2, 7, 12)):
        at_trip(min(at, 2 * step - 1), functools.partial(gather_step, step))
        if step == turns:
            at_trip(
                min(at, 2 * step - 1),
                *(functools.partial(firsts_step, away) for away in range(1, turns + 1)),
            )
    at_trip(12, out_weights_late)
    at_trip(12, functools.partial(out_to_sibling, from_pair, 1))

    def trip(i, carry):
        for at, steps in late.items():

            @pl.when(i == at)
            def _(steps=steps):
                for step in steps:
                    step()

        @pl.when(i < nz)
        def _():
            project(i)

        @pl.when(i >= LAG)
        def _():
            finish(i - LAG)

        return carry

    lax.fori_loop(0, trips, trip, 0)
    row = mix_index[0]
    weight_now = mix_table[0, row]
    weight_first = mix_table[1, row]

    def mix(origin, first):
        now = v_buf[:, origin].astype(F32)
        v_buf[:, origin] = (weight_now * now + weight_first * first.astype(F32)).astype(BF)

    mix(z, fv_own[0])
    arrived(fv_in.at[pl.ds(1, nz - 1)], fz_sem.at[0])
    for away in range(1, nz):
        mix(lax.rem(z + away, nz), fv_in[away])

    scale = 1.0 / math.sqrt(hs)
    valid = lengths[0]
    stripe = nz * rows
    q_blocks = min(nz, 128 // rows)
    q_rows = q_blocks * rows

    def attend(b):
        n = (b + 1) * stripe
        keys = k_buf[0 : b + 1].reshape(n, hs)
        values = v_buf[0 : b + 1].reshape(n, hs)

        def one(t, carry):
            at = pl.ds(t * q_blocks, q_blocks)
            query = q_buf[b, at].reshape(q_rows, hs)
            scores = (
                lax.dot_general(query, keys, (((1,), (1,)), ((), ())), preferred_element_type=F32)
                * scale
            )
            col = lax.broadcasted_iota(jnp.int32, (q_rows, n), 1)
            line = b * stripe + t * q_rows + lax.broadcasted_iota(jnp.int32, (q_rows, n), 0)
            scores = jnp.where((col <= line) & (col < valid), scores, NEG_FILL)
            raised = jnp.exp(scores - jnp.max(scores, axis=1, keepdims=True))
            weights = (raised * (1.0 / jnp.sum(raised, axis=1, keepdims=True))).astype(BF)
            result = jnp.dot(weights, values, preferred_element_type=F32).astype(BF)
            att[0, at, b] = result.reshape(q_blocks, rows, hs)
            return carry

        lax.fori_loop(0, nz // q_blocks, one, 0)

    near, far = pl.ds(0, nz // 2), pl.ds(nz // 2, nz // 2)

    def att_send(b):
        remote(
            att.at[0, :, b], att.at[3, :, b], send_sem.at[14], att_sem.at[0, b], tensor_0=xs[1]
        ).start()
        remote(
            att.at[0, :, b], att.at[1, :, b], send_sem.at[15], att_sem.at[1, b], tensor_0=xs[3]
        ).start()

    def att_pass(b):
        arrived(att.at[3, :, b], att_sem.at[0, b])
        remote(
            att.at[3, near, b], att.at[2, near, b], send_sem.at[16], att_sem.at[2, b], tensor_0=xs[1]
        ).start()
        arrived(att.at[1, :, b], att_sem.at[1, b])
        remote(
            att.at[1, far, b], att.at[2, far, b], send_sem.at[17], att_sem.at[2, b], tensor_0=xs[3]
        ).start()

    my_columns = pl.ds(pl.multiple_of(x * quarter, 128), quarter)

    def length_of(way, b):
        return turns if (b % 2 == 0) == (way == 0) else turns - 1

    def ready(b):
        arrived(att.at[2, :, b], att_sem.at[2, b])
        lhs = jnp.concatenate([att[r, :, b].reshape(stripe, hs) for r in range(NX)], axis=1)
        for s in range(subs):
            column = slice(s * SUB, (s + 1) * SUB)
            term = jnp.dot(lhs, wo2[:, column], preferred_element_type=F32)
            own_term[b, :, :, column] = term.reshape(nz, rows, SUB)
        fin[b] = own_term[b, z].astype(BF)

    def reduce_step(b, step):
        for way in (0, 1):
            length = length_of(way, b)
            slot = (2 * b + way) * turns + step
            z_next = z_down if way else z_up

            def one(b=b, way=way, length=length, slot=slot, z_next=z_next):
                target = lax.rem(z + (1 - 2 * way) * (length - step + 1) + nz, nz)
                term = own_term[b, target]
                if not (isinstance(step, int) and step == 1):
                    arrived(rs_recv.at[slot - 1], rs_sem.at[slot - 1])
                    term = term + rs_recv[slot - 1].astype(F32)
                rs_send[slot - 1] = term.astype(BF)

                def go_on():
                    remote(
                        rs_send.at[slot - 1],
                        rs_recv.at[slot],
                        send_sem.at[18],
                        rs_sem.at[slot],
                        tensor_1=z_next,
                    ).start()

                def deliver():
                    remote(
                        rs_send.at[slot - 1],
                        out.at[1 + way, :, my_columns],
                        send_sem.at[18],
                        fin_sem.at[0],
                        tensor_0=jnp.int32(b),
                        tensor_1=z_next,
                    ).start()

                if isinstance(step, int):
                    (go_on if step < length else deliver)()
                else:
                    pl.when(step < length)(go_on)
                    pl.when(step == length)(deliver)

            if isinstance(step, int):
                if step <= length:
                    one()
            else:
                pl.when(step <= length)(one)

    for b in range(NX):
        attend(b)
        att_send(b)
    out_to_sibling(from_other, 2)
    out_to_sibling(2, 3)
    att_pass(0)
    out_weights_wait()
    for b in range(NX):
        if b + 1 < NX:
            att_pass(b + 1)
        ready(b)
        for back in range(b + 1):
            reduce_step(b - back, 1 + back)
    for d in (1, 2, 3):
        remote(
            fin.at[xs[d]],
            out.at[0, :, my_columns],
            send_sem.at[19],
            fin_sem.at[0],
            tensor_0=xs[d],
        ).start()
    pltpu.make_async_copy(fin.at[x], out.at[0, :, my_columns], fin_sem.at[0]).start()

    def reduce_round(step, carry):
        for b in reversed(range(NX)):
            reduce_step(b, step + NX - 1 - b)
        return carry

    lax.fori_loop(2, turns + 1, reduce_round, 0)

    n_ring = turns * 2 - 1
    arrived(x_wide.at[pl.ds(0, 3), :, 0], send_sem.at[0])
    arrived(z_part.at[0, :, 0], send_sem.at[1])
    arrived(fv_stage, send_sem.at[2])
    arrived(x_wide.at[pl.ds(0, n_ring)], send_sem.at[3])
    arrived(w2.at[pl.ds(0, share), pl.ds(0, width)], send_sem.at[4])
    arrived(z_part.at[pl.ds(0, n_ring), :, pl.ds(0, 2)], send_sem.at[5])
    arrived(z_part.at[:, :, pl.ds(0, 2)], send_sem.at[6])
    arrived(w2.at[pl.ds(0, share), pl.ds(0, width)], send_sem.at[7])
    arrived(fv_own.at[pl.ds(1, nz - 1)], send_sem.at[8])
    arrived(b_send, send_sem.at[10])
    arrived(wo2.at[pl.ds(0, 3 * hs), pl.ds(0, half)], send_sem.at[11])
    arrived(wo2.at[pl.ds(0, 3 * hs), pl.ds(0, half)], send_sem.at[12])
    arrived(wo_relay, send_sem.at[13])
    arrived(att.at[0], send_sem.at[14])
    arrived(att.at[0], send_sem.at[15])
    arrived(att.at[0, near], send_sem.at[16])
    arrived(att.at[0, far], send_sem.at[17])
    arrived(rs_recv.at[pl.ds(0, 3 * NX)], fin_sem.at[0])
    arrived(rs_send.at[pl.ds(0, NX * n_ring)], send_sem.at[18])
    arrived(fin.at[pl.ds(0, 3)], send_sem.at[19])


def body(hidden_in, first_values, qkv_weight, out_weight, mix_table, mix_index, lengths, *, nz):
    rows, model = hidden_in.shape[1:]
    hs = qkv_weight.shape[2]
    quarter = model // NX
    half = quarter // 2
    halves = model // 2
    subs = quarter // SUB
    x_subs = max(1, halves * 3 // 10 // SUB)
    z_subs = 2
    z_wide = (halves - x_subs * SUB) // z_subs
    turns = nz // 2
    block = NX * rows
    vmem = pl.BlockSpec(memory_space=pltpu.VMEM)
    smem = pl.BlockSpec(memory_space=pltpu.SMEM)
    anywhere = pl.BlockSpec(memory_space=pl.ANY)
    dma = pltpu.SemaphoreType.DMA
    scratch = [
        pltpu.VMEM((nz, x_subs, NX, rows, SUB), BF),
        pltpu.VMEM((nz, z_subs, NX, rows, z_wide), BF),
        pltpu.VMEM((halves, 2 * 3 * hs), BF),
        pltpu.VMEM((NX * hs, quarter), BF),
        pltpu.VMEM((hs, half), BF),
        pltpu.VMEM((NX - 1, nz, rows, hs), BF),
        pltpu.VMEM((nz, NX, rows, hs), BF),
        pltpu.VMEM((nz, NX, rows, hs), BF),
        pltpu.VMEM((nz, block, 3 * hs), F32),
        pltpu.VMEM((nz, block, 3 * hs), BF),
        pltpu.VMEM((nz, block, 3 * hs), BF),
        pltpu.VMEM((NX, nz, rows, hs), BF),
        pltpu.VMEM((NX, nz, rows, hs), BF),
        pltpu.VMEM((NX, nz, rows, hs), BF),
        pltpu.VMEM((NX, nz, NX, rows, hs), BF),
        pltpu.VMEM((NX * 2 * turns, rows, quarter), BF),
        pltpu.VMEM((NX * 2 * turns, rows, quarter), BF),
        pltpu.VMEM((NX, nz, rows, quarter), F32),
        pltpu.VMEM((NX, rows, quarter), BF),
        dma((2,)),
        dma((20,)),
        dma((2,)),
        dma((NX,)),
        dma((2, turns, (x_subs + 1) // 2 + z_subs)),
        dma((nz,)),
        dma((2, 3)),
        dma((7,)),
        dma((1,)),
        dma((1,)),
        dma((nz,)),
        dma((3, NX)),
        dma((NX * 2 * turns,)),
        dma((1,)),
    ]
    result = pl.pallas_call(
        functools.partial(kernel, nz),
        out_shape=jax.ShapeDtypeStruct((3, rows, model), BF),
        in_specs=[vmem, vmem, anywhere, anywhere, smem, smem, smem],
        out_specs=anywhere,
        scratch_shapes=scratch,
        compiler_params=pltpu.CompilerParams(
            collective_id=0, has_side_effects=True, vmem_limit_bytes=60 * 1024 * 1024
        ),
    )(
        hidden_in[0],
        first_values[0],
        jnp.transpose(qkv_weight, (1, 0, 2)),
        out_weight,
        mix_table.T,
        mix_index,
        lengths,
    )
    first, second, third = (piece.astype(F32) for piece in result)
    return (first + second + third).astype(BF)[None]


def solution(mesh):
    nz = mesh.shape["tensor"] // NX
    torus = Mesh(
        mesh.devices.reshape(mesh.shape["groups"], mesh.shape["dp"], NX, nz),
        ("groups", "dp", "tensor_0", "tensor_1"),
    )
    placed = (
        P(("groups", "dp"), TENSOR, None),
        P(("groups", "dp"), TENSOR, None),
        P(None, None, TENSOR),
        P(TENSOR, None),
        P(),
        P(TENSOR),
        P(("groups", "dp")),
    )
    return jax.shard_map(
        functools.partial(body, nz=nz),
        mesh=torus,
        in_specs=placed,
        out_specs=P(("groups", "dp"), TENSOR, None),
        check_vma=False,
    )
```

```python
import functools
import math

import jax
import jax.numpy as jnp
from jax import lax
from jax.experimental import pallas as pl
from jax.experimental.pallas import tpu as pltpu
from jax.sharding import Mesh
from jax.sharding import PartitionSpec as P

TENSOR = ("tensor_0", "tensor_1")
NEG_FILL = -1e30
BF = jnp.bfloat16
F32 = jnp.float32
NX = 4
SUB = 256
LAG = 3


def kernel(
    nz,
    hid,
    firsts,
    w_qkv,
    w_out,
    mix_table,
    mix_index,
    lengths,
    out,
    x_wide,
    z_part,
    w2,
    wo2,
    wo_relay,
    fv_stage,
    fv_own,
    fv_in,
    stash,
    b_send,
    b_recv,
    q_buf,
    k_buf,
    v_buf,
    att,
    rs_send,
    rs_recv,
    own_term,
    fin,
    local_sem,
    send_sem,
    own_sem,
    hid_sem,
    ag_sem,
    oz_sem,
    w_sem,
    wo_sem,
    fx_sem,
    fz_sem,
    b_sem,
    att_sem,
    rs_sem,
    fin_sem,
):
    rows, model = hid.shape
    hs = w_qkv.shape[2]
    quarter = model // NX
    half = quarter // 2
    halves = model // 2
    subs = quarter // SUB
    turns = nz // 2
    block = NX * rows

    x = lax.axis_index("tensor_0")
    z = lax.axis_index("tensor_1")
    core = lax.axis_index("dp")
    xs = [x] + [lax.rem(x + d, NX) for d in range(1, NX)]
    z_up = lax.rem(z + 1, nz)
    z_down = lax.rem(z + nz - 1, nz)
    x_way = lax.rem(x + 1 + 2 * core, NX)
    odd = lax.rem(x, 2)
    pair = x + 1 - 2 * odd
    other = lax.rem(x + NX - 1 + 2 * odd, NX)

    def remote(src, dst, send, recv, **where):
        return pltpu.make_async_remote_copy(
            src_ref=src,
            dst_ref=dst,
            send_sem=send,
            recv_sem=recv,
            device_id=where,
            device_id_type=pl.DeviceIdType.MESH,
        )

    def arrived(ref, sem):
        pltpu.make_async_copy(ref, ref, sem).wait()

    barrier = pltpu.get_barrier_semaphore()
    partners = [
        {"dp": 1 - core},
        {"tensor_0": xs[1]},
        {"tensor_0": xs[2]},
        {"tensor_0": xs[3]},
        {"tensor_1": z_up},
        {"tensor_1": z_down},
    ]
    for partner in partners:
        pl.semaphore_signal(
            barrier, inc=1, device_id=partner, device_id_type=pl.DeviceIdType.MESH
        )
    pl.semaphore_wait(barrier, len(partners))

    def half_of(at):
        return lax.rem((at + 1) // 2, 2)

    mine, theirs = half_of(x), 1 - half_of(x)
    stripes, other_stripes = pl.ds(x - odd, 2), pl.ds(NX - 2 - x + odd, 2)
    x_subs, z_subs, z_wide = x_wide.shape[1], z_part.shape[1], z_part.shape[4]

    def x_columns(to_half, s):
        return pl.ds(pl.multiple_of(to_half * halves + s * SUB, 128), SUB)

    def z_columns(to_half, s):
        return pl.ds(pl.multiple_of(to_half * halves + x_subs * SUB + s * z_wide, 128), z_wide)

    def hidden_out(d, to, to_half):
        for s in range(x_subs):
            remote(
                hid.at[:, x_columns(to_half, s)],
                x_wide.at[0, s, x],
                send_sem.at[0],
                hid_sem.at[d],
                tensor_0=to,
            ).start()

    for s in range(z_subs):
        remote(
            hid.at[:, z_columns(theirs, s)],
            z_part.at[0, s, x],
            send_sem.at[1],
            hid_sem.at[0],
            tensor_0=pair,
        ).start()
    hidden_out(1, pair, theirs)
    hidden_out(2, other, mine)
    hidden_out(3, xs[2], theirs)
    for s in range(z_subs):
        pltpu.make_async_copy(
            hid.at[:, z_columns(mine, s)], z_part.at[0, s, x], own_sem.at[0]
        ).start()
    for s in range(x_subs):
        pltpu.make_async_copy(
            hid.at[:, x_columns(mine, s)], x_wide.at[0, s, x], own_sem.at[1]
        ).start()

    flows = [(0, s, min(2, x_subs - s)) for s in range(0, x_subs, 2)]
    flows += [(1, s, 1) for s in range(z_subs)]

    def longer(way, n):
        return turns if (n % 2 == 0) == (way == 0) else turns - 1

    def part(n, place):
        kind, s, count = flows[n]
        if kind == 0:
            return x_wide.at[place, pl.ds(s, count)]
        return z_part.at[place, s, stripes]

    def ring_send(n, way, step, source, target):
        remote(
            source,
            target,
            send_sem.at[3 if flows[n][0] == 0 else 5],
            ag_sem.at[way, step - 1, n],
            tensor_1=z_down if way else z_up,
        ).start()

    def other_send(place, s, source, target):
        remote(source, target, send_sem.at[6], oz_sem.at[place], tensor_0=other).start()

    for n, (kind, first, count) in enumerate(flows):
        for s in range(first, first + count):
            for way in (0, 1):
                target = 1 if way else nz - 1
                if kind == 0:
                    ring_send(n, way, 1, hid.at[:, x_columns(mine, s)], x_wide.at[target, s, x])
                else:
                    ring_send(n, way, 1, hid.at[:, z_columns(mine, s)], z_part.at[target, s, x])
            if kind == 1:
                other_send(0, s, hid.at[:, z_columns(mine, s)], z_part.at[0, s, x])

    def stage_firsts(head, carry):
        away = lax.rem(head - z + nz, nz)
        for d in range(NX):
            column = pl.multiple_of((xs[d] * nz + head) * hs, 128)
            piece = firsts[:, pl.ds(column, hs)]
            if d == 0:
                fv_own[away, x] = piece
            else:
                fv_stage[d - 1, away] = piece
        return carry

    lax.fori_loop(0, nz, stage_firsts, 0)
    for d in (1, 2, 3):
        remote(
            fv_stage.at[d - 1],
            fv_own.at[:, x],
            send_sem.at[2],
            fx_sem.at[0],
            tensor_0=xs[d],
        ).start()

    share = halves // 2
    my_share = pl.multiple_of(core * share, 128)
    sibling_share = pl.multiple_of((1 - core) * share, 128)
    for p in range(3):
        remote(
            w_qkv.at[p, pl.ds(pl.multiple_of(theirs * halves + core * share, 128), share)],
            w2.at[pl.ds(my_share, share), pl.ds((3 + p) * hs, hs)],
            send_sem.at[4],
            w_sem.at[0, p],
            tensor_0=pair,
        ).start()
    own_weights = []
    for p in range(3):
        own_weights.append(
            pltpu.make_async_copy(
                w_qkv.at[p, pl.ds(pl.multiple_of(mine * halves, 128), halves)],
                w2.at[:, pl.ds(p * hs, hs)],
                local_sem.at[0],
            )
        )
    own_weights.append(
        pltpu.make_async_copy(
            w_out.at[:, pl.ds(pl.multiple_of(x * quarter, 128), quarter)],
            wo2.at[pl.ds(0, hs)],
            local_sem.at[1],
        )
    )
    for copy in own_weights:
        copy.start()

    my_half = pl.multiple_of(core * half, 128)

    def wo_columns(to):
        return pl.ds(pl.multiple_of(to * quarter + core * half, 128), half)

    def wo_piece(r):
        return wo2.at[pl.ds(pl.multiple_of(r * hs, hs), hs), pl.ds(my_half, half)]

    from_pair, from_other = 1 + 2 * odd, 3 - 2 * odd

    def out_weights_send():
        remote(
            w_out.at[:, wo_columns(pair)], wo_piece(from_other), send_sem.at[11], wo_sem.at[1], tensor_0=pair
        ).start()
        remote(
            w_out.at[:, wo_columns(xs[2])], wo_relay, send_sem.at[11], wo_sem.at[0], tensor_0=pair
        ).start()

    def out_weights_late():
        remote(
            w_out.at[:, wo_columns(other)], wo_piece(from_pair), send_sem.at[11], wo_sem.at[2], tensor_0=other
        ).start()
        arrived(wo_relay, wo_sem.at[0])
        remote(wo_relay, wo_piece(2), send_sem.at[13], wo_sem.at[3], tensor_0=other).start()

    def out_to_sibling(r, sem):
        arrived(wo_piece(r), wo_sem.at[sem])
        remote(
            wo_piece(r), wo_piece(r), send_sem.at[12], wo_sem.at[3 + sem], dp=1 - core
        ).start()

    def out_weights_wait():
        for sem in (1, 2, 3):
            arrived(wo_piece(0), wo_sem.at[3 + sem])

    out_weights_send()

    def gather_step(step):
        for n in range(len(flows)):
            for way in (0, 1):
                if step <= longer(way, n):
                    place = step if way else nz - step
                    arrived(part(n, place), ag_sem.at[way, step - 1, n])
                    if step + 1 <= longer(way, n):
                        onward = step + 1 if way else nz - step - 1
                        ring_send(n, way, step + 1, part(n, place), part(n, onward))
                    if flows[n][0] == 1:
                        other_send(place, flows[n][1], part(n, place), part(n, place))

    def weights_step(p):
        here = w2.at[pl.ds(my_share, share), pl.ds((3 + p) * hs, hs)]
        arrived(here, w_sem.at[0, p])
        remote(here, here, send_sem.at[7], w_sem.at[1, p], dp=1 - core).start()

    def weights_last():
        for p in range(3):
            arrived(
                w2.at[pl.ds(sibling_share, share), pl.ds((3 + p) * hs, hs)], w_sem.at[1, p]
            )
        arrived(w2.at[:, pl.ds(0, 3 * hs)], local_sem.at[0])
        arrived(wo2.at[pl.ds(0, hs)], local_sem.at[1])

    def firsts_step(step):
        if step == 1:
            arrived(fv_stage, fx_sem.at[0])
        for away in sorted({step, nz - step}):
            remote(
                fv_own.at[away],
                fv_in.at[nz - away],
                send_sem.at[8],
                fz_sem.at[0],
                tensor_1=lax.rem(z + away, nz),
            ).start()

    arrived(z_part.at[0, :, x], hid_sem.at[0])
    for n, (kind, first, count) in enumerate(flows):
        if kind == 1:
            piece = z_part.at[0, first, pair]
            ring_send(n, 0, 1, piece, z_part.at[nz - 1, first, pair])
            ring_send(n, 1, 1, piece, z_part.at[1, first, pair])
            other_send(0, first, piece, piece)
    for d in (1, 2, 3):
        arrived(x_wide.at[0, :, x], hid_sem.at[d])
    for n, (kind, first, count) in enumerate(flows):
        if kind == 0:
            for d in (1, 2, 3):
                at = pl.ds(first, count)
                piece = x_wide.at[0, at, xs[d]]
                ring_send(n, 0, 1, piece, x_wide.at[nz - 1, at, xs[d]])
                ring_send(n, 1, 1, piece, x_wide.at[1, at, xs[d]])
    arrived(z_part.at[0, :, x], own_sem.at[0])
    arrived(x_wide.at[0, :, x], own_sem.at[1])
    early = max(turns - 3, 0)
    weights_after = {2: (0,), 3: (1,), 4: (2,)}
    for step in range(1, early + 1):
        gather_step(step)
        for p in weights_after.get(step, ()):
            weights_step(p)
    for p in range(3):
        if not any(p in done for step, done in weights_after.items() if step <= early):
            weights_step(p)
    weights_last()

    width = 3 * hs

    def place_of(i):
        return jnp.where(i % 2 == 1, (i + 1) // 2, lax.rem(nz - i // 2, nz))

    def project(i):
        place = place_of(i)
        arrived(z_part.at[place, :, other_stripes], oz_sem.at[place])
        lhs = jnp.concatenate(
            [x_wide[place, s].reshape(block, SUB) for s in range(x_subs)]
            + [z_part[place, s].reshape(block, z_wide) for s in range(z_subs)],
            axis=1,
        )
        term = jnp.dot(lhs, w2[...], preferred_element_type=F32)
        b_send[i] = term[:, width:].astype(BF)
        remote(
            b_send.at[i], b_recv.at[i], send_sem.at[10], b_sem.at[i], tensor_0=pair
        ).start()
        stash[i] = term[:, :width]

    def finish(i):
        arrived(b_recv.at[i], b_sem.at[i])
        total = stash[i] + b_recv[i].astype(F32)
        total = total.astype(BF).reshape(NX, rows, width)
        origin = lax.rem(z + place_of(i), nz)
        q_buf[:, origin] = total[:, :, :hs]
        k_buf[:, origin] = total[:, :, hs : 2 * hs]
        v_buf[:, origin] = total[:, :, 2 * hs :]

    trips = nz + LAG
    late = {}

    def at_trip(i, *steps):
        late.setdefault(min(i, trips - 1), []).extend(steps)

    for step, at in zip(range(early + 1, turns + 1), (2, 7, 12)):
        at_trip(min(at, 2 * step - 1), functools.partial(gather_step, step))
        if step == turns:
            at_trip(
                min(at, 2 * step - 1),
                *(functools.partial(firsts_step, away) for away in range(1, turns + 1)),
            )
    at_trip(12, out_weights_late)
    at_trip(12, functools.partial(out_to_sibling, from_pair, 1))

    def trip(i, carry):
        for at, steps in late.items():

            @pl.when(i == at)
            def _(steps=steps):
                for step in steps:
                    step()

        @pl.when(i < nz)
        def _():
            project(i)

        @pl.when(i >= LAG)
        def _():
            finish(i - LAG)

        return carry

    lax.fori_loop(0, trips, trip, 0)
    row = mix_index[0]
    weight_now = mix_table[0, row]
    weight_first = mix_table[1, row]

    def mix(origin, first):
        now = v_buf[:, origin].astype(F32)
        v_buf[:, origin] = (weight_now * now + weight_first * first.astype(F32)).astype(BF)

    mix(z, fv_own[0])
    arrived(fv_in.at[pl.ds(1, nz - 1)], fz_sem.at[0])
    for away in range(1, nz):
        mix(lax.rem(z + away, nz), fv_in[away])

    scale = 1.0 / math.sqrt(hs)
    valid = lengths[0]
    stripe = nz * rows
    q_blocks = min(nz, 128 // rows)
    q_rows = q_blocks * rows

    def attend(b):
        n = (b + 1) * stripe
        keys = k_buf[0 : b + 1].reshape(n, hs)
        values = v_buf[0 : b + 1].reshape(n, hs)

        def one(t, carry):
            at = pl.ds(t * q_blocks, q_blocks)
            query = q_buf[b, at].reshape(q_rows, hs)
            scores = (
                lax.dot_general(query, keys, (((1,), (1,)), ((), ())), preferred_element_type=F32)
                * scale
            )
            col = lax.broadcasted_iota(jnp.int32, (q_rows, n), 1)
            line = b * stripe + t * q_rows + lax.broadcasted_iota(jnp.int32, (q_rows, n), 0)
            scores = jnp.where((col <= line) & (col < valid), scores, NEG_FILL)
            raised = jnp.exp(scores - jnp.max(scores, axis=1, keepdims=True))
            weights = (raised * (1.0 / jnp.sum(raised, axis=1, keepdims=True))).astype(BF)
            result = jnp.dot(weights, values, preferred_element_type=F32).astype(BF)
            att[0, at, b] = result.reshape(q_blocks, rows, hs)
            return carry

        lax.fori_loop(0, nz // q_blocks, one, 0)

    near, far = pl.ds(0, nz // 2), pl.ds(nz // 2, nz // 2)

    def att_send(b):
        remote(
            att.at[0, :, b], att.at[3, :, b], send_sem.at[14], att_sem.at[0, b], tensor_0=xs[1]
        ).start()
        remote(
            att.at[0, :, b], att.at[1, :, b], send_sem.at[15], att_sem.at[1, b], tensor_0=xs[3]
        ).start()

    def att_pass(b):
        arrived(att.at[3, :, b], att_sem.at[0, b])
        remote(
            att.at[3, near, b], att.at[2, near, b], send_sem.at[16], att_sem.at[2, b], tensor_0=xs[1]
        ).start()
        arrived(att.at[1, :, b], att_sem.at[1, b])
        remote(
            att.at[1, far, b], att.at[2, far, b], send_sem.at[17], att_sem.at[2, b], tensor_0=xs[3]
        ).start()

    my_columns = pl.ds(pl.multiple_of(x * quarter, 128), quarter)

    def length_of(way, b):
        return turns if (b % 2 == 0) == (way == 0) else turns - 1

    def ready(b):
        arrived(att.at[2, :, b], att_sem.at[2, b])
        lhs = jnp.concatenate([att[r, :, b].reshape(stripe, hs) for r in range(NX)], axis=1)
        for s in range(subs):
            column = slice(s * SUB, (s + 1) * SUB)
            term = jnp.dot(lhs, wo2[:, column], preferred_element_type=F32)
            own_term[b, :, :, column] = term.reshape(nz, rows, SUB)
        fin[b] = own_term[b, z].astype(BF)

    def reduce_step(b, step):
        for way in (0, 1):
            length = length_of(way, b)
            slot = (2 * b + way) * turns + step
            z_next = z_down if way else z_up

            def one(b=b, way=way, length=length, slot=slot, z_next=z_next):
                target = lax.rem(z + (1 - 2 * way) * (length - step + 1) + nz, nz)
                term = own_term[b, target]
                if not (isinstance(step, int) and step == 1):
                    arrived(rs_recv.at[slot - 1], rs_sem.at[slot - 1])
                    term = term + rs_recv[slot - 1].astype(F32)
                rs_send[slot - 1] = term.astype(BF)

                def go_on():
                    remote(
                        rs_send.at[slot - 1],
                        rs_recv.at[slot],
                        send_sem.at[18],
                        rs_sem.at[slot],
                        tensor_1=z_next,
                    ).start()

                def deliver():
                    remote(
                        rs_send.at[slot - 1],
                        out.at[1 + way, :, my_columns],
                        send_sem.at[18],
                        fin_sem.at[0],
                        tensor_0=jnp.int32(b),
                        tensor_1=z_next,
                    ).start()

                if isinstance(step, int):
                    (go_on if step < length else deliver)()
                else:
                    pl.when(step < length)(go_on)
                    pl.when(step == length)(deliver)

            if isinstance(step, int):
                if step <= length:
                    one()
            else:
                pl.when(step <= length)(one)

    for b in range(NX):
        attend(b)
        att_send(b)
    out_to_sibling(from_other, 2)
    out_to_sibling(2, 3)
    for b in range(NX):
        att_pass(b)
    out_weights_wait()
    for b in range(NX):
        ready(b)
        reduce_step(b, 1)
    for d in (1, 2, 3):
        remote(
            fin.at[xs[d]],
            out.at[0, :, my_columns],
            send_sem.at[19],
            fin_sem.at[0],
            tensor_0=xs[d],
        ).start()
    pltpu.make_async_copy(fin.at[x], out.at[0, :, my_columns], fin_sem.at[0]).start()

    def reduce_round(step, carry):
        for b in range(NX):
            reduce_step(b, step)
        return carry

    lax.fori_loop(2, turns + 1, reduce_round, 0)

    n_ring = turns * 2 - 1
    arrived(x_wide.at[pl.ds(0, 3), :, 0], send_sem.at[0])
    arrived(z_part.at[0, :, 0], send_sem.at[1])
    arrived(fv_stage, send_sem.at[2])
    arrived(x_wide.at[pl.ds(0, n_ring)], send_sem.at[3])
    arrived(w2.at[pl.ds(0, share), pl.ds(0, width)], send_sem.at[4])
    arrived(z_part.at[pl.ds(0, n_ring), :, pl.ds(0, 2)], send_sem.at[5])
    arrived(z_part.at[:, :, pl.ds(0, 2)], send_sem.at[6])
    arrived(w2.at[pl.ds(0, share), pl.ds(0, width)], send_sem.at[7])
    arrived(fv_own.at[pl.ds(1, nz - 1)], send_sem.at[8])
    arrived(b_send, send_sem.at[10])
    arrived(wo2.at[pl.ds(0, 3 * hs), pl.ds(0, half)], send_sem.at[11])
    arrived(wo2.at[pl.ds(0, 3 * hs), pl.ds(0, half)], send_sem.at[12])
    arrived(wo_relay, send_sem.at[13])
    arrived(att.at[0], send_sem.at[14])
    arrived(att.at[0], send_sem.at[15])
    arrived(att.at[0, near], send_sem.at[16])
    arrived(att.at[0, far], send_sem.at[17])
    arrived(rs_recv.at[pl.ds(0, 3 * NX)], fin_sem.at[0])
    arrived(rs_send.at[pl.ds(0, NX * n_ring)], send_sem.at[18])
    arrived(fin.at[pl.ds(0, 3)], send_sem.at[19])


def body(hidden_in, first_values, qkv_weight, out_weight, mix_table, mix_index, lengths, *, nz):
    rows, model = hidden_in.shape[1:]
    hs = qkv_weight.shape[2]
    quarter = model // NX
    half = quarter // 2
    halves = model // 2
    subs = quarter // SUB
    x_subs = max(1, halves * 3 // 10 // SUB)
    z_subs = 2
    z_wide = (halves - x_subs * SUB) // z_subs
    turns = nz // 2
    block = NX * rows
    vmem = pl.BlockSpec(memory_space=pltpu.VMEM)
    smem = pl.BlockSpec(memory_space=pltpu.SMEM)
    anywhere = pl.BlockSpec(memory_space=pl.ANY)
    dma = pltpu.SemaphoreType.DMA
    scratch = [
        pltpu.VMEM((nz, x_subs, NX, rows, SUB), BF),
        pltpu.VMEM((nz, z_subs, NX, rows, z_wide), BF),
        pltpu.VMEM((halves, 2 * 3 * hs), BF),
        pltpu.VMEM((NX * hs, quarter), BF),
        pltpu.VMEM((hs, half), BF),
        pltpu.VMEM((NX - 1, nz, rows, hs), BF),
        pltpu.VMEM((nz, NX, rows, hs), BF),
        pltpu.VMEM((nz, NX, rows, hs), BF),
        pltpu.VMEM((nz, block, 3 * hs), F32),
        pltpu.VMEM((nz, block, 3 * hs), BF),
        pltpu.VMEM((nz, block, 3 * hs), BF),
        pltpu.VMEM((NX, nz, rows, hs), BF),
        pltpu.VMEM((NX, nz, rows, hs), BF),
        pltpu.VMEM((NX, nz, rows, hs), BF),
        pltpu.VMEM((NX, nz, NX, rows, hs), BF),
        pltpu.VMEM((NX * 2 * turns, rows, quarter), BF),
        pltpu.VMEM((NX * 2 * turns, rows, quarter), BF),
        pltpu.VMEM((NX, nz, rows, quarter), F32),
        pltpu.VMEM((NX, rows, quarter), BF),
        dma((2,)),
        dma((20,)),
        dma((2,)),
        dma((NX,)),
        dma((2, turns, (x_subs + 1) // 2 + z_subs)),
        dma((nz,)),
        dma((2, 3)),
        dma((7,)),
        dma((1,)),
        dma((1,)),
        dma((nz,)),
        dma((3, NX)),
        dma((NX * 2 * turns,)),
        dma((1,)),
    ]
    result = pl.pallas_call(
        functools.partial(kernel, nz),
        out_shape=jax.ShapeDtypeStruct((3, rows, model), BF),
        in_specs=[vmem, vmem, anywhere, anywhere, smem, smem, smem],
        out_specs=anywhere,
        scratch_shapes=scratch,
        compiler_params=pltpu.CompilerParams(
            collective_id=0, has_side_effects=True, vmem_limit_bytes=60 * 1024 * 1024
        ),
    )(
        hidden_in[0],
        first_values[0],
        jnp.transpose(qkv_weight, (1, 0, 2)),
        out_weight,
        mix_table.T,
        mix_index,
        lengths,
    )
    first, second, third = (piece.astype(F32) for piece in result)
    return (first + second + third).astype(BF)[None]


def solution(mesh):
    nz = mesh.shape["tensor"] // NX
    torus = Mesh(
        mesh.devices.reshape(mesh.shape["groups"], mesh.shape["dp"], NX, nz),
        ("groups", "dp", "tensor_0", "tensor_1"),
    )
    placed = (
        P(("groups", "dp"), TENSOR, None),
        P(("groups", "dp"), TENSOR, None),
        P(None, None, TENSOR),
        P(TENSOR, None),
        P(),
        P(TENSOR),
        P(("groups", "dp")),
    )
    return jax.shard_map(
        functools.partial(body, nz=nz),
        mesh=torus,
        in_specs=placed,
        out_specs=P(("groups", "dp"), TENSOR, None),
        check_vma=False,
    )
```

```python
import functools
import math

import jax
import jax.numpy as jnp
from jax import lax
from jax.experimental import pallas as pl
from jax.experimental.pallas import tpu as pltpu
from jax.sharding import Mesh
from jax.sharding import PartitionSpec as P

TENSOR = ("tensor_0", "tensor_1")
NEG_FILL = -1e30
BF = jnp.bfloat16
F32 = jnp.float32
NX = 4
SUB = 256
LAG = 3


def kernel(
    nz,
    hid_in,
    firsts_in,
    w_qkv,
    w_out,
    table_in,
    index_in,
    lengths_in,
    out,
    hid,
    firsts,
    mix_table,
    mix_index,
    lengths,
    load_sem,
    x_wide,
    z_part,
    w2,
    wo2,
    wo_relay,
    fv_stage,
    fv_own,
    fv_in,
    stash,
    b_send,
    b_recv,
    q_buf,
    k_buf,
    v_buf,
    att,
    rs_send,
    rs_recv,
    own_term,
    fin,
    local_sem,
    send_sem,
    own_sem,
    hid_sem,
    ag_sem,
    oz_sem,
    w_sem,
    wo_sem,
    fx_sem,
    fz_sem,
    b_sem,
    att_sem,
    rs_sem,
    fin_sem,
):
    rows, model = hid.shape
    hs = w_qkv.shape[2]
    quarter = model // NX
    half = quarter // 2
    halves = model // 2
    subs = quarter // SUB
    turns = nz // 2
    block = NX * rows

    x = lax.axis_index("tensor_0")
    z = lax.axis_index("tensor_1")
    core = lax.axis_index("dp")
    xs = [x] + [lax.rem(x + d, NX) for d in range(1, NX)]
    z_up = lax.rem(z + 1, nz)
    z_down = lax.rem(z + nz - 1, nz)
    x_way = lax.rem(x + 1 + 2 * core, NX)
    odd = lax.rem(x, 2)
    pair = x + 1 - 2 * odd
    other = lax.rem(x + NX - 1 + 2 * odd, NX)

    def remote(src, dst, send, recv, **where):
        return pltpu.make_async_remote_copy(
            src_ref=src,
            dst_ref=dst,
            send_sem=send,
            recv_sem=recv,
            device_id=where,
            device_id_type=pl.DeviceIdType.MESH,
        )

    def arrived(ref, sem):
        pltpu.make_async_copy(ref, ref, sem).wait()

    barrier = pltpu.get_barrier_semaphore()
    partners = [
        {"dp": 1 - core},
        {"tensor_0": xs[1]},
        {"tensor_0": xs[2]},
        {"tensor_0": xs[3]},
        {"tensor_1": z_up},
        {"tensor_1": z_down},
    ]
    for partner in partners:
        pl.semaphore_signal(
            barrier, inc=1, device_id=partner, device_id_type=pl.DeviceIdType.MESH
        )
    loads = [
        pltpu.make_async_copy(source, target, load_sem.at[n])
        for n, (source, target) in enumerate(
            (
                (hid_in, hid),
                (firsts_in, firsts),
                (table_in, mix_table),
                (index_in, mix_index),
                (lengths_in, lengths),
            )
        )
    ]
    for load in loads:
        load.start()
    pl.semaphore_wait(barrier, len(partners))
    loads[0].wait()

    def half_of(at):
        return lax.rem((at + 1) // 2, 2)

    mine, theirs = half_of(x), 1 - half_of(x)
    stripes, other_stripes = pl.ds(x - odd, 2), pl.ds(NX - 2 - x + odd, 2)
    x_subs, z_subs, z_wide = x_wide.shape[1], z_part.shape[1], z_part.shape[4]

    def x_columns(to_half, s):
        return pl.ds(pl.multiple_of(to_half * halves + s * SUB, 128), SUB)

    def z_columns(to_half, s):
        return pl.ds(pl.multiple_of(to_half * halves + x_subs * SUB + s * z_wide, 128), z_wide)

    def hidden_out(d, to, to_half):
        for s in range(x_subs):
            remote(
                hid.at[:, x_columns(to_half, s)],
                x_wide.at[0, s, x],
                send_sem.at[0],
                hid_sem.at[d],
                tensor_0=to,
            ).start()

    for s in range(z_subs):
        remote(
            hid.at[:, z_columns(theirs, s)],
            z_part.at[0, s, x],
            send_sem.at[1],
            hid_sem.at[0],
            tensor_0=pair,
        ).start()
    hidden_out(1, pair, theirs)
    hidden_out(2, other, mine)
    hidden_out(3, xs[2], theirs)
    for s in range(z_subs):
        pltpu.make_async_copy(
            hid.at[:, z_columns(mine, s)], z_part.at[0, s, x], own_sem.at[0]
        ).start()
    for s in range(x_subs):
        pltpu.make_async_copy(
            hid.at[:, x_columns(mine, s)], x_wide.at[0, s, x], own_sem.at[1]
        ).start()

    flows = [(0, s, min(2, x_subs - s)) for s in range(0, x_subs, 2)]
    flows += [(1, s, 1) for s in range(z_subs)]

    def longer(way, n):
        return turns if (n % 2 == 0) == (way == 0) else turns - 1

    def part(n, place):
        kind, s, count = flows[n]
        if kind == 0:
            return x_wide.at[place, pl.ds(s, count)]
        return z_part.at[place, s, stripes]

    def ring_send(n, way, step, source, target):
        remote(
            source,
            target,
            send_sem.at[3 if flows[n][0] == 0 else 5],
            ag_sem.at[way, step - 1, n],
            tensor_1=z_down if way else z_up,
        ).start()

    def other_send(place, s, source, target):
        remote(source, target, send_sem.at[6], oz_sem.at[place], tensor_0=other).start()

    for n, (kind, first, count) in enumerate(flows):
        for s in range(first, first + count):
            for way in (0, 1):
                target = 1 if way else nz - 1
                if kind == 0:
                    ring_send(n, way, 1, hid.at[:, x_columns(mine, s)], x_wide.at[target, s, x])
                else:
                    ring_send(n, way, 1, hid.at[:, z_columns(mine, s)], z_part.at[target, s, x])
            if kind == 1:
                other_send(0, s, hid.at[:, z_columns(mine, s)], z_part.at[0, s, x])

    def stage_firsts(head, carry):
        away = lax.rem(head - z + nz, nz)
        for d in range(NX):
            column = pl.multiple_of((xs[d] * nz + head) * hs, 128)
            piece = firsts[:, pl.ds(column, hs)]
            if d == 0:
                fv_own[away, x] = piece
            else:
                fv_stage[d - 1, away] = piece
        return carry

    loads[1].wait()
    lax.fori_loop(0, nz, stage_firsts, 0)
    for d in (1, 2, 3):
        remote(
            fv_stage.at[d - 1],
            fv_own.at[:, x],
            send_sem.at[2],
            fx_sem.at[0],
            tensor_0=xs[d],
        ).start()

    share = halves // 2
    my_share = pl.multiple_of(core * share, 128)
    sibling_share = pl.multiple_of((1 - core) * share, 128)
    for p in range(3):
        remote(
            w_qkv.at[p, pl.ds(pl.multiple_of(theirs * halves + core * share, 128), share)],
            w2.at[pl.ds(my_share, share), pl.ds((3 + p) * hs, hs)],
            send_sem.at[4],
            w_sem.at[0, p],
            tensor_0=pair,
        ).start()
    own_weights = []
    for p in range(3):
        own_weights.append(
            pltpu.make_async_copy(
                w_qkv.at[p, pl.ds(pl.multiple_of(mine * halves, 128), halves)],
                w2.at[:, pl.ds(p * hs, hs)],
                local_sem.at[0],
            )
        )
    own_weights.append(
        pltpu.make_async_copy(
            w_out.at[:, pl.ds(pl.multiple_of(x * quarter, 128), quarter)],
            wo2.at[pl.ds(0, hs)],
            local_sem.at[1],
        )
    )
    for copy in own_weights:
        copy.start()

    my_half = pl.multiple_of(core * half, 128)

    def wo_columns(to):
        return pl.ds(pl.multiple_of(to * quarter + core * half, 128), half)

    def wo_piece(r):
        return wo2.at[pl.ds(pl.multiple_of(r * hs, hs), hs), pl.ds(my_half, half)]

    from_pair, from_other = 1 + 2 * odd, 3 - 2 * odd

    def out_weights_send():
        remote(
            w_out.at[:, wo_columns(pair)], wo_piece(from_other), send_sem.at[11], wo_sem.at[1], tensor_0=pair
        ).start()
        remote(
            w_out.at[:, wo_columns(xs[2])], wo_relay, send_sem.at[11], wo_sem.at[0], tensor_0=pair
        ).start()

    def out_weights_late():
        remote(
            w_out.at[:, wo_columns(other)], wo_piece(from_pair), send_sem.at[11], wo_sem.at[2], tensor_0=other
        ).start()
        arrived(wo_relay, wo_sem.at[0])
        remote(wo_relay, wo_piece(2), send_sem.at[13], wo_sem.at[3], tensor_0=other).start()

    def out_to_sibling(r, sem):
        arrived(wo_piece(r), wo_sem.at[sem])
        remote(
            wo_piece(r), wo_piece(r), send_sem.at[12], wo_sem.at[3 + sem], dp=1 - core
        ).start()

    def out_weights_wait():
        for sem in (1, 2, 3):
            arrived(wo_piece(0), wo_sem.at[3 + sem])

    out_weights_send()

    def gather_step(step):
        for n in range(len(flows)):
            for way in (0, 1):
                if step <= longer(way, n):
                    place = step if way else nz - step
                    arrived(part(n, place), ag_sem.at[way, step - 1, n])
                    if step + 1 <= longer(way, n):
                        onward = step + 1 if way else nz - step - 1
                        ring_send(n, way, step + 1, part(n, place), part(n, onward))
                    if flows[n][0] == 1:
                        other_send(place, flows[n][1], part(n, place), part(n, place))

    def weights_step(p):
        here = w2.at[pl.ds(my_share, share), pl.ds((3 + p) * hs, hs)]
        arrived(here, w_sem.at[0, p])
        remote(here, here, send_sem.at[7], w_sem.at[1, p], dp=1 - core).start()

    def weights_last():
        for p in range(3):
            arrived(
                w2.at[pl.ds(sibling_share, share), pl.ds((3 + p) * hs, hs)], w_sem.at[1, p]
            )
        arrived(w2.at[:, pl.ds(0, 3 * hs)], local_sem.at[0])
        arrived(wo2.at[pl.ds(0, hs)], local_sem.at[1])

    def firsts_step(step):
        if step == 1:
            arrived(fv_stage, fx_sem.at[0])
        for away in sorted({step, nz - step}):
            remote(
                fv_own.at[away],
                fv_in.at[nz - away],
                send_sem.at[8],
                fz_sem.at[0],
                tensor_1=lax.rem(z + away, nz),
            ).start()

    arrived(z_part.at[0, :, x], hid_sem.at[0])
    for n, (kind, first, count) in enumerate(flows):
        if kind == 1:
            piece = z_part.at[0, first, pair]
            ring_send(n, 0, 1, piece, z_part.at[nz - 1, first, pair])
            ring_send(n, 1, 1, piece, z_part.at[1, first, pair])
            other_send(0, first, piece, piece)
    for d in (1, 2, 3):
        arrived(x_wide.at[0, :, x], hid_sem.at[d])
    for n, (kind, first, count) in enumerate(flows):
        if kind == 0:
            for d in (1, 2, 3):
                at = pl.ds(first, count)
                piece = x_wide.at[0, at, xs[d]]
                ring_send(n, 0, 1, piece, x_wide.at[nz - 1, at, xs[d]])
                ring_send(n, 1, 1, piece, x_wide.at[1, at, xs[d]])
    arrived(z_part.at[0, :, x], own_sem.at[0])
    arrived(x_wide.at[0, :, x], own_sem.at[1])
    early = max(turns - 3, 0)
    weights_after = {2: (0,), 3: (1,), 4: (2,)}
    for step in range(1, early + 1):
        gather_step(step)
        for p in weights_after.get(step, ()):
            weights_step(p)
    for p in range(3):
        if not any(p in done for step, done in weights_after.items() if step <= early):
            weights_step(p)
    weights_last()

    width = 3 * hs

    def place_of(i):
        return jnp.where(i % 2 == 1, (i + 1) // 2, lax.rem(nz - i // 2, nz))

    def project(i):
        place = place_of(i)
        arrived(z_part.at[place, :, other_stripes], oz_sem.at[place])
        lhs = jnp.concatenate(
            [x_wide[place, s].reshape(block, SUB) for s in range(x_subs)]
            + [z_part[place, s].reshape(block, z_wide) for s in range(z_subs)],
            axis=1,
        )
        term = jnp.dot(lhs, w2[...], preferred_element_type=F32)
        b_send[i] = term[:, width:].astype(BF)
        remote(
            b_send.at[i], b_recv.at[i], send_sem.at[10], b_sem.at[i], tensor_0=pair
        ).start()
        stash[i] = term[:, :width]

    def finish(i):
        arrived(b_recv.at[i], b_sem.at[i])
        total = stash[i] + b_recv[i].astype(F32)
        total = total.astype(BF).reshape(NX, rows, width)
        origin = lax.rem(z + place_of(i), nz)
        q_buf[:, origin] = total[:, :, :hs]
        k_buf[:, origin] = total[:, :, hs : 2 * hs]
        v_buf[:, origin] = total[:, :, 2 * hs :]

    trips = nz + LAG
    late = {}

    def at_trip(i, *steps):
        late.setdefault(min(i, trips - 1), []).extend(steps)

    for step, at in zip(range(early + 1, turns + 1), (2, 7, 12)):
        at_trip(min(at, 2 * step - 1), functools.partial(gather_step, step))
        if step == turns:
            at_trip(
                min(at, 2 * step - 1),
                *(functools.partial(firsts_step, away) for away in range(1, turns + 1)),
            )
    at_trip(12, out_weights_late)
    at_trip(12, functools.partial(out_to_sibling, from_pair, 1))

    def trip(i, carry):
        for at, steps in late.items():

            @pl.when(i == at)
            def _(steps=steps):
                for step in steps:
                    step()

        @pl.when(i < nz)
        def _():
            project(i)

        @pl.when(i >= LAG)
        def _():
            finish(i - LAG)

        return carry

    lax.fori_loop(0, trips, trip, 0)
    for load in loads[2:]:
        load.wait()
    row = mix_index[0]
    weight_now = mix_table[0, row]
    weight_first = mix_table[1, row]

    def mix(origin, first):
        now = v_buf[:, origin].astype(F32)
        v_buf[:, origin] = (weight_now * now + weight_first * first.astype(F32)).astype(BF)

    mix(z, fv_own[0])
    arrived(fv_in.at[pl.ds(1, nz - 1)], fz_sem.at[0])
    for away in range(1, nz):
        mix(lax.rem(z + away, nz), fv_in[away])

    scale = 1.0 / math.sqrt(hs)
    valid = lengths[0]
    stripe = nz * rows
    q_blocks = min(nz, 128 // rows)
    q_rows = q_blocks * rows

    def attend(b):
        n = (b + 1) * stripe
        keys = k_buf[0 : b + 1].reshape(n, hs)
        values = v_buf[0 : b + 1].reshape(n, hs)

        def one(t, carry):
            at = pl.ds(t * q_blocks, q_blocks)
            query = q_buf[b, at].reshape(q_rows, hs)
            scores = (
                lax.dot_general(query, keys, (((1,), (1,)), ((), ())), preferred_element_type=F32)
                * scale
            )
            col = lax.broadcasted_iota(jnp.int32, (q_rows, n), 1)
            line = b * stripe + t * q_rows + lax.broadcasted_iota(jnp.int32, (q_rows, n), 0)
            scores = jnp.where((col <= line) & (col < valid), scores, NEG_FILL)
            raised = jnp.exp(scores - jnp.max(scores, axis=1, keepdims=True))
            weights = (raised * (1.0 / jnp.sum(raised, axis=1, keepdims=True))).astype(BF)
            result = jnp.dot(weights, values, preferred_element_type=F32).astype(BF)
            att[0, at, b] = result.reshape(q_blocks, rows, hs)
            return carry

        lax.fori_loop(0, nz // q_blocks, one, 0)

    near, far = pl.ds(0, nz // 2), pl.ds(nz // 2, nz // 2)

    def att_send(b):
        remote(
            att.at[0, :, b], att.at[3, :, b], send_sem.at[14], att_sem.at[0, b], tensor_0=xs[1]
        ).start()
        remote(
            att.at[0, :, b], att.at[1, :, b], send_sem.at[15], att_sem.at[1, b], tensor_0=xs[3]
        ).start()

    def att_pass(b):
        arrived(att.at[3, :, b], att_sem.at[0, b])
        remote(
            att.at[3, near, b], att.at[2, near, b], send_sem.at[16], att_sem.at[2, b], tensor_0=xs[1]
        ).start()
        arrived(att.at[1, :, b], att_sem.at[1, b])
        remote(
            att.at[1, far, b], att.at[2, far, b], send_sem.at[17], att_sem.at[2, b], tensor_0=xs[3]
        ).start()

    my_columns = pl.ds(pl.multiple_of(x * quarter, 128), quarter)

    def length_of(way, b):
        return turns if (b % 2 == 0) == (way == 0) else turns - 1

    def ready(b):
        arrived(att.at[2, :, b], att_sem.at[2, b])
        lhs = jnp.concatenate([att[r, :, b].reshape(stripe, hs) for r in range(NX)], axis=1)
        for s in range(subs):
            column = slice(s * SUB, (s + 1) * SUB)
            term = jnp.dot(lhs, wo2[:, column], preferred_element_type=F32)
            own_term[b, :, :, column] = term.reshape(nz, rows, SUB)
        fin[b] = own_term[b, z].astype(BF)

    def reduce_step(b, step):
        for way in (0, 1):
            length = length_of(way, b)
            slot = (2 * b + way) * turns + step
            z_next = z_down if way else z_up

            def one(b=b, way=way, length=length, slot=slot, z_next=z_next):
                target = lax.rem(z + (1 - 2 * way) * (length - step + 1) + nz, nz)
                term = own_term[b, target]
                if not (isinstance(step, int) and step == 1):
                    arrived(rs_recv.at[slot - 1], rs_sem.at[slot - 1])
                    term = term + rs_recv[slot - 1].astype(F32)
                rs_send[slot - 1] = term.astype(BF)

                def go_on():
                    remote(
                        rs_send.at[slot - 1],
                        rs_recv.at[slot],
                        send_sem.at[18],
                        rs_sem.at[slot],
                        tensor_1=z_next,
                    ).start()

                def deliver():
                    remote(
                        rs_send.at[slot - 1],
                        out.at[1 + way, :, my_columns],
                        send_sem.at[18],
                        fin_sem.at[0],
                        tensor_0=jnp.int32(b),
                        tensor_1=z_next,
                    ).start()

                if isinstance(step, int):
                    (go_on if step < length else deliver)()
                else:
                    pl.when(step < length)(go_on)
                    pl.when(step == length)(deliver)

            if isinstance(step, int):
                if step <= length:
                    one()
            else:
                pl.when(step <= length)(one)

    for b in range(NX):
        attend(b)
        att_send(b)
    out_to_sibling(from_other, 2)
    out_to_sibling(2, 3)
    for b in range(NX):
        att_pass(b)
    out_weights_wait()
    for b in range(NX):
        ready(b)
        reduce_step(b, 1)
    for d in (1, 2, 3):
        remote(
            fin.at[xs[d]],
            out.at[0, :, my_columns],
            send_sem.at[19],
            fin_sem.at[0],
            tensor_0=xs[d],
        ).start()
    pltpu.make_async_copy(fin.at[x], out.at[0, :, my_columns], fin_sem.at[0]).start()

    def reduce_round(step, carry):
        for b in range(NX):
            reduce_step(b, step)
        return carry

    lax.fori_loop(2, turns + 1, reduce_round, 0)

    n_ring = turns * 2 - 1
    arrived(x_wide.at[pl.ds(0, 3), :, 0], send_sem.at[0])
    arrived(z_part.at[0, :, 0], send_sem.at[1])
    arrived(fv_stage, send_sem.at[2])
    arrived(x_wide.at[pl.ds(0, n_ring)], send_sem.at[3])
    arrived(w2.at[pl.ds(0, share), pl.ds(0, width)], send_sem.at[4])
    arrived(z_part.at[pl.ds(0, n_ring), :, pl.ds(0, 2)], send_sem.at[5])
    arrived(z_part.at[:, :, pl.ds(0, 2)], send_sem.at[6])
    arrived(w2.at[pl.ds(0, share), pl.ds(0, width)], send_sem.at[7])
    arrived(fv_own.at[pl.ds(1, nz - 1)], send_sem.at[8])
    arrived(b_send, send_sem.at[10])
    arrived(wo2.at[pl.ds(0, 3 * hs), pl.ds(0, half)], send_sem.at[11])
    arrived(wo2.at[pl.ds(0, 3 * hs), pl.ds(0, half)], send_sem.at[12])
    arrived(wo_relay, send_sem.at[13])
    arrived(att.at[0], send_sem.at[14])
    arrived(att.at[0], send_sem.at[15])
    arrived(att.at[0, near], send_sem.at[16])
    arrived(att.at[0, far], send_sem.at[17])
    arrived(rs_recv.at[pl.ds(0, 3 * NX)], fin_sem.at[0])
    arrived(rs_send.at[pl.ds(0, NX * n_ring)], send_sem.at[18])
    arrived(fin.at[pl.ds(0, 3)], send_sem.at[19])


def body(hidden_in, first_values, qkv_weight, out_weight, mix_table, mix_index, lengths, *, nz):
    rows, model = hidden_in.shape[1:]
    hs = qkv_weight.shape[2]
    quarter = model // NX
    half = quarter // 2
    halves = model // 2
    subs = quarter // SUB
    x_subs = max(1, halves * 3 // 10 // SUB)
    z_subs = 2
    z_wide = (halves - x_subs * SUB) // z_subs
    turns = nz // 2
    block = NX * rows
    anywhere = pl.BlockSpec(memory_space=pl.ANY)
    dma = pltpu.SemaphoreType.DMA
    scratch = [
        pltpu.VMEM((rows, model), BF),
        pltpu.VMEM(first_values.shape[1:], BF),
        pltpu.SMEM(mix_table.shape[::-1], F32),
        pltpu.SMEM(mix_index.shape, jnp.int32),
        pltpu.SMEM(lengths.shape, jnp.int32),
        dma((5,)),
        pltpu.VMEM((nz, x_subs, NX, rows, SUB), BF),
        pltpu.VMEM((nz, z_subs, NX, rows, z_wide), BF),
        pltpu.VMEM((halves, 2 * 3 * hs), BF),
        pltpu.VMEM((NX * hs, quarter), BF),
        pltpu.VMEM((hs, half), BF),
        pltpu.VMEM((NX - 1, nz, rows, hs), BF),
        pltpu.VMEM((nz, NX, rows, hs), BF),
        pltpu.VMEM((nz, NX, rows, hs), BF),
        pltpu.VMEM((nz, block, 3 * hs), F32),
        pltpu.VMEM((nz, block, 3 * hs), BF),
        pltpu.VMEM((nz, block, 3 * hs), BF),
        pltpu.VMEM((NX, nz, rows, hs), BF),
        pltpu.VMEM((NX, nz, rows, hs), BF),
        pltpu.VMEM((NX, nz, rows, hs), BF),
        pltpu.VMEM((NX, nz, NX, rows, hs), BF),
        pltpu.VMEM((NX * 2 * turns, rows, quarter), BF),
        pltpu.VMEM((NX * 2 * turns, rows, quarter), BF),
        pltpu.VMEM((NX, nz, rows, quarter), F32),
        pltpu.VMEM((NX, rows, quarter), BF),
        dma((2,)),
        dma((20,)),
        dma((2,)),
        dma((NX,)),
        dma((2, turns, (x_subs + 1) // 2 + z_subs)),
        dma((nz,)),
        dma((2, 3)),
        dma((7,)),
        dma((1,)),
        dma((1,)),
        dma((nz,)),
        dma((3, NX)),
        dma((NX * 2 * turns,)),
        dma((1,)),
    ]
    result = pl.pallas_call(
        functools.partial(kernel, nz),
        out_shape=jax.ShapeDtypeStruct((3, rows, model), BF),
        in_specs=[anywhere] * 7,
        out_specs=anywhere,
        scratch_shapes=scratch,
        compiler_params=pltpu.CompilerParams(
            collective_id=0, has_side_effects=True, vmem_limit_bytes=60 * 1024 * 1024
        ),
    )(
        hidden_in[0],
        first_values[0],
        jnp.transpose(qkv_weight, (1, 0, 2)),
        out_weight,
        mix_table.T,
        mix_index,
        lengths,
    )
    first, second, third = (piece.astype(F32) for piece in result)
    return (first + second + third).astype(BF)[None]


def solution(mesh):
    nz = mesh.shape["tensor"] // NX
    torus = Mesh(
        mesh.devices.reshape(mesh.shape["groups"], mesh.shape["dp"], NX, nz),
        ("groups", "dp", "tensor_0", "tensor_1"),
    )
    placed = (
        P(("groups", "dp"), TENSOR, None),
        P(("groups", "dp"), TENSOR, None),
        P(None, None, TENSOR),
        P(TENSOR, None),
        P(),
        P(TENSOR),
        P(("groups", "dp")),
    )
    return jax.shard_map(
        functools.partial(body, nz=nz),
        mesh=torus,
        in_specs=placed,
        out_specs=P(("groups", "dp"), TENSOR, None),
        check_vma=False,
    )
```

```python
import functools
import math

import jax
import jax.numpy as jnp
from jax import lax
from jax.experimental import pallas as pl
from jax.experimental.pallas import tpu as pltpu
from jax.sharding import Mesh
from jax.sharding import PartitionSpec as P

TENSOR = ("tensor_0", "tensor_1")
NEG_FILL = -1e30
BF = jnp.bfloat16
F32 = jnp.float32
NX = 4
SUB = 256
LAG = 3


def kernel(
    nz,
    hid_in,
    firsts_in,
    w_qkv,
    w_out,
    table_in,
    index_in,
    lengths_in,
    out,
    hid,
    firsts,
    mix_table,
    mix_index,
    lengths,
    load_sem,
    x_wide,
    z_part,
    w2,
    wo2,
    wo_relay,
    fv_stage,
    fv_own,
    fv_in,
    stash,
    b_send,
    b_recv,
    q_buf,
    k_buf,
    v_buf,
    att,
    rs_send,
    rs_recv,
    own_term,
    fin,
    local_sem,
    send_sem,
    own_sem,
    hid_sem,
    ag_sem,
    oz_sem,
    w_sem,
    wo_sem,
    fx_sem,
    fz_sem,
    b_sem,
    att_sem,
    rs_sem,
    fin_sem,
):
    rows, model = hid.shape
    hs = w_qkv.shape[2]
    quarter = model // NX
    half = quarter // 2
    halves = model // 2
    subs = quarter // SUB
    turns = nz // 2
    block = NX * rows

    x = lax.axis_index("tensor_0")
    z = lax.axis_index("tensor_1")
    core = lax.axis_index("dp")
    xs = [x] + [lax.rem(x + d, NX) for d in range(1, NX)]
    z_up = lax.rem(z + 1, nz)
    z_down = lax.rem(z + nz - 1, nz)
    x_way = lax.rem(x + 1 + 2 * core, NX)
    odd = lax.rem(x, 2)
    pair = x + 1 - 2 * odd
    other = lax.rem(x + NX - 1 + 2 * odd, NX)

    def remote(src, dst, send, recv, **where):
        return pltpu.make_async_remote_copy(
            src_ref=src,
            dst_ref=dst,
            send_sem=send,
            recv_sem=recv,
            device_id=where,
            device_id_type=pl.DeviceIdType.MESH,
        )

    def arrived(ref, sem):
        pltpu.make_async_copy(ref, ref, sem).wait()

    barrier = pltpu.get_barrier_semaphore()
    partners = [
        {"dp": 1 - core},
        {"tensor_0": xs[1]},
        {"tensor_0": xs[2]},
        {"tensor_0": xs[3]},
        {"tensor_1": z_up},
        {"tensor_1": z_down},
    ]
    for partner in partners:
        pl.semaphore_signal(
            barrier, inc=1, device_id=partner, device_id_type=pl.DeviceIdType.MESH
        )
    loads = [
        pltpu.make_async_copy(source, target, load_sem.at[n])
        for n, (source, target) in enumerate(
            (
                (hid_in, hid),
                (firsts_in, firsts),
                (table_in, mix_table),
                (index_in, mix_index),
                (lengths_in, lengths),
            )
        )
    ]
    for load in loads:
        load.start()
    pl.semaphore_wait(barrier, len(partners))
    loads[0].wait()

    def half_of(at):
        return lax.rem((at + 1) // 2, 2)

    mine, theirs = half_of(x), 1 - half_of(x)
    stripes, other_stripes = pl.ds(x - odd, 2), pl.ds(NX - 2 - x + odd, 2)
    x_subs, z_subs, z_wide = x_wide.shape[1], z_part.shape[1], z_part.shape[4]

    def x_columns(to_half, s):
        return pl.ds(pl.multiple_of(to_half * halves + s * SUB, 128), SUB)

    def z_columns(to_half, s):
        return pl.ds(pl.multiple_of(to_half * halves + x_subs * SUB + s * z_wide, 128), z_wide)

    def hidden_out(d, to, to_half):
        for s in range(x_subs):
            remote(
                hid.at[:, x_columns(to_half, s)],
                x_wide.at[0, s, x],
                send_sem.at[0],
                hid_sem.at[d],
                tensor_0=to,
            ).start()

    for s in range(z_subs):
        remote(
            hid.at[:, z_columns(theirs, s)],
            z_part.at[0, s, x],
            send_sem.at[1],
            hid_sem.at[0],
            tensor_0=pair,
        ).start()
    hidden_out(1, pair, theirs)
    hidden_out(2, other, mine)
    hidden_out(3, xs[2], theirs)
    for s in range(z_subs):
        pltpu.make_async_copy(
            hid.at[:, z_columns(mine, s)], z_part.at[0, s, x], own_sem.at[0]
        ).start()
    for s in range(x_subs):
        pltpu.make_async_copy(
            hid.at[:, x_columns(mine, s)], x_wide.at[0, s, x], own_sem.at[1]
        ).start()

    flows = [(0, s, 1) for s in range(x_subs)]
    flows += [(1, s, 1) for s in range(z_subs)]

    def longer(way, n):
        return turns if (n % 2 == 0) == (way == 0) else turns - 1

    def part(n, place):
        kind, s, count = flows[n]
        if kind == 0:
            return x_wide.at[place, pl.ds(s, count)]
        return z_part.at[place, s, stripes]

    def ring_send(n, way, step, source, target):
        remote(
            source,
            target,
            send_sem.at[3 if flows[n][0] == 0 else 5],
            ag_sem.at[way, step - 1, n],
            tensor_1=z_down if way else z_up,
        ).start()

    def other_send(place, s, source, target):
        remote(source, target, send_sem.at[6], oz_sem.at[place], tensor_0=other).start()

    for n, (kind, first, count) in enumerate(flows):
        for s in range(first, first + count):
            for way in (0, 1):
                target = 1 if way else nz - 1
                if kind == 0:
                    ring_send(n, way, 1, hid.at[:, x_columns(mine, s)], x_wide.at[target, s, x])
                else:
                    ring_send(n, way, 1, hid.at[:, z_columns(mine, s)], z_part.at[target, s, x])
            if kind == 1:
                other_send(0, s, hid.at[:, z_columns(mine, s)], z_part.at[0, s, x])

    def stage_firsts(head, carry):
        away = lax.rem(head - z + nz, nz)
        for d in range(NX):
            column = pl.multiple_of((xs[d] * nz + head) * hs, 128)
            piece = firsts[:, pl.ds(column, hs)]
            if d == 0:
                fv_own[away, x] = piece
            else:
                fv_stage[d - 1, away] = piece
        return carry

    loads[1].wait()
    lax.fori_loop(0, nz, stage_firsts, 0)
    for d in (1, 2, 3):
        remote(
            fv_stage.at[d - 1],
            fv_own.at[:, x],
            send_sem.at[2],
            fx_sem.at[0],
            tensor_0=xs[d],
        ).start()

    share = halves // 2
    my_share = pl.multiple_of(core * share, 128)
    sibling_share = pl.multiple_of((1 - core) * share, 128)
    for p in range(3):
        remote(
            w_qkv.at[p, pl.ds(pl.multiple_of(theirs * halves + core * share, 128), share)],
            w2.at[pl.ds(my_share, share), pl.ds((3 + p) * hs, hs)],
            send_sem.at[4],
            w_sem.at[0, p],
            tensor_0=pair,
        ).start()
    own_weights = []
    for p in range(3):
        own_weights.append(
            pltpu.make_async_copy(
                w_qkv.at[p, pl.ds(pl.multiple_of(mine * halves, 128), halves)],
                w2.at[:, pl.ds(p * hs, hs)],
                local_sem.at[0],
            )
        )
    own_weights.append(
        pltpu.make_async_copy(
            w_out.at[:, pl.ds(pl.multiple_of(x * quarter, 128), quarter)],
            wo2.at[pl.ds(0, hs)],
            local_sem.at[1],
        )
    )
    for copy in own_weights:
        copy.start()

    my_half = pl.multiple_of(core * half, 128)

    def wo_columns(to):
        return pl.ds(pl.multiple_of(to * quarter + core * half, 128), half)

    def wo_piece(r):
        return wo2.at[pl.ds(pl.multiple_of(r * hs, hs), hs), pl.ds(my_half, half)]

    from_pair, from_other = 1 + 2 * odd, 3 - 2 * odd

    def out_weights_send():
        remote(
            w_out.at[:, wo_columns(pair)], wo_piece(from_other), send_sem.at[11], wo_sem.at[1], tensor_0=pair
        ).start()
        remote(
            w_out.at[:, wo_columns(xs[2])], wo_relay, send_sem.at[11], wo_sem.at[0], tensor_0=pair
        ).start()

    def out_weights_late():
        remote(
            w_out.at[:, wo_columns(other)], wo_piece(from_pair), send_sem.at[11], wo_sem.at[2], tensor_0=other
        ).start()
        arrived(wo_relay, wo_sem.at[0])
        remote(wo_relay, wo_piece(2), send_sem.at[13], wo_sem.at[3], tensor_0=other).start()

    def out_to_sibling(r, sem):
        arrived(wo_piece(r), wo_sem.at[sem])
        remote(
            wo_piece(r), wo_piece(r), send_sem.at[12], wo_sem.at[3 + sem], dp=1 - core
        ).start()

    def out_weights_wait():
        for sem in (1, 2, 3):
            arrived(wo_piece(0), wo_sem.at[3 + sem])

    out_weights_send()

    def gather_step(step):
        for n in range(len(flows)):
            for way in (0, 1):
                if step <= longer(way, n):
                    place = step if way else nz - step
                    arrived(part(n, place), ag_sem.at[way, step - 1, n])
                    if step + 1 <= longer(way, n):
                        onward = step + 1 if way else nz - step - 1
                        ring_send(n, way, step + 1, part(n, place), part(n, onward))
                    if flows[n][0] == 1:
                        other_send(place, flows[n][1], part(n, place), part(n, place))

    def weights_step(p):
        here = w2.at[pl.ds(my_share, share), pl.ds((3 + p) * hs, hs)]
        arrived(here, w_sem.at[0, p])
        remote(here, here, send_sem.at[7], w_sem.at[1, p], dp=1 - core).start()

    def weights_last():
        for p in range(3):
            arrived(
                w2.at[pl.ds(sibling_share, share), pl.ds((3 + p) * hs, hs)], w_sem.at[1, p]
            )
        arrived(w2.at[:, pl.ds(0, 3 * hs)], local_sem.at[0])
        arrived(wo2.at[pl.ds(0, hs)], local_sem.at[1])

    def firsts_step(step):
        if step == 1:
            arrived(fv_stage, fx_sem.at[0])
        for away in sorted({step, nz - step}):
            remote(
                fv_own.at[away],
                fv_in.at[nz - away],
                send_sem.at[8],
                fz_sem.at[0],
                tensor_1=lax.rem(z + away, nz),
            ).start()

    arrived(z_part.at[0, :, x], hid_sem.at[0])
    for n, (kind, first, count) in enumerate(flows):
        if kind == 1:
            piece = z_part.at[0, first, pair]
            ring_send(n, 0, 1, piece, z_part.at[nz - 1, first, pair])
            ring_send(n, 1, 1, piece, z_part.at[1, first, pair])
            other_send(0, first, piece, piece)
    for d in (1, 2, 3):
        arrived(x_wide.at[0, :, x], hid_sem.at[d])
    for n, (kind, first, count) in enumerate(flows):
        if kind == 0:
            for d in (1, 2, 3):
                at = pl.ds(first, count)
                piece = x_wide.at[0, at, xs[d]]
                ring_send(n, 0, 1, piece, x_wide.at[nz - 1, at, xs[d]])
                ring_send(n, 1, 1, piece, x_wide.at[1, at, xs[d]])
    arrived(z_part.at[0, :, x], own_sem.at[0])
    arrived(x_wide.at[0, :, x], own_sem.at[1])
    early = max(turns - 3, 0)
    weights_after = {2: (0,), 3: (1,), 4: (2,)}
    for step in range(1, early + 1):
        gather_step(step)
        for p in weights_after.get(step, ()):
            weights_step(p)
    for p in range(3):
        if not any(p in done for step, done in weights_after.items() if step <= early):
            weights_step(p)
    weights_last()

    width = 3 * hs

    def place_of(i):
        return jnp.where(i % 2 == 1, (i + 1) // 2, lax.rem(nz - i // 2, nz))

    def project(i):
        place = place_of(i)
        arrived(z_part.at[place, :, other_stripes], oz_sem.at[place])
        lhs = jnp.concatenate(
            [x_wide[place, s].reshape(block, SUB) for s in range(x_subs)]
            + [z_part[place, s].reshape(block, z_wide) for s in range(z_subs)],
            axis=1,
        )
        term = jnp.dot(lhs, w2[...], preferred_element_type=F32)
        b_send[i] = term[:, width:].astype(BF)
        remote(
            b_send.at[i], b_recv.at[i], send_sem.at[10], b_sem.at[i], tensor_0=pair
        ).start()
        stash[i] = term[:, :width]

    def finish(i):
        arrived(b_recv.at[i], b_sem.at[i])
        total = stash[i] + b_recv[i].astype(F32)
        total = total.astype(BF).reshape(NX, rows, width)
        origin = lax.rem(z + place_of(i), nz)
        q_buf[:, origin] = total[:, :, :hs]
        k_buf[:, origin] = total[:, :, hs : 2 * hs]
        v_buf[:, origin] = total[:, :, 2 * hs :]

    trips = nz + LAG
    late = {}

    def at_trip(i, *steps):
        late.setdefault(min(i, trips - 1), []).extend(steps)

    for step, at in zip(range(early + 1, turns + 1), (2, 7, 12)):
        at_trip(min(at, 2 * step - 1), functools.partial(gather_step, step))
        if step == turns:
            at_trip(
                min(at, 2 * step - 1),
                *(functools.partial(firsts_step, away) for away in range(1, turns + 1)),
            )
    at_trip(12, out_weights_late)
    at_trip(12, functools.partial(out_to_sibling, from_pair, 1))

    def trip(i, carry):
        for at, steps in late.items():

            @pl.when(i == at)
            def _(steps=steps):
                for step in steps:
                    step()

        @pl.when(i < nz)
        def _():
            project(i)

        @pl.when(i >= LAG)
        def _():
            finish(i - LAG)

        return carry

    lax.fori_loop(0, trips, trip, 0)
    for load in loads[2:]:
        load.wait()
    row = mix_index[0]
    weight_now = mix_table[0, row]
    weight_first = mix_table[1, row]

    def mix(origin, first):
        now = v_buf[:, origin].astype(F32)
        v_buf[:, origin] = (weight_now * now + weight_first * first.astype(F32)).astype(BF)

    mix(z, fv_own[0])
    arrived(fv_in.at[pl.ds(1, nz - 1)], fz_sem.at[0])
    for away in range(1, nz):
        mix(lax.rem(z + away, nz), fv_in[away])

    scale = 1.0 / math.sqrt(hs)
    valid = lengths[0]
    stripe = nz * rows
    q_blocks = min(nz, 128 // rows)
    q_rows = q_blocks * rows

    def attend(b):
        n = (b + 1) * stripe
        keys = k_buf[0 : b + 1].reshape(n, hs)
        values = v_buf[0 : b + 1].reshape(n, hs)

        def one(t, carry):
            at = pl.ds(t * q_blocks, q_blocks)
            query = q_buf[b, at].reshape(q_rows, hs)
            scores = (
                lax.dot_general(query, keys, (((1,), (1,)), ((), ())), preferred_element_type=F32)
                * scale
            )
            col = lax.broadcasted_iota(jnp.int32, (q_rows, n), 1)
            line = b * stripe + t * q_rows + lax.broadcasted_iota(jnp.int32, (q_rows, n), 0)
            scores = jnp.where((col <= line) & (col < valid), scores, NEG_FILL)
            raised = jnp.exp(scores - jnp.max(scores, axis=1, keepdims=True))
            weights = (raised * (1.0 / jnp.sum(raised, axis=1, keepdims=True))).astype(BF)
            result = jnp.dot(weights, values, preferred_element_type=F32).astype(BF)
            att[0, at, b] = result.reshape(q_blocks, rows, hs)
            return carry

        lax.fori_loop(0, nz // q_blocks, one, 0)

    near, far = pl.ds(0, nz // 2), pl.ds(nz // 2, nz // 2)

    def att_send(b):
        remote(
            att.at[0, :, b], att.at[3, :, b], send_sem.at[14], att_sem.at[0, b], tensor_0=xs[1]
        ).start()
        remote(
            att.at[0, :, b], att.at[1, :, b], send_sem.at[15], att_sem.at[1, b], tensor_0=xs[3]
        ).start()

    def att_pass(b):
        arrived(att.at[3, :, b], att_sem.at[0, b])
        remote(
            att.at[3, near, b], att.at[2, near, b], send_sem.at[16], att_sem.at[2, b], tensor_0=xs[1]
        ).start()
        arrived(att.at[1, :, b], att_sem.at[1, b])
        remote(
            att.at[1, far, b], att.at[2, far, b], send_sem.at[17], att_sem.at[2, b], tensor_0=xs[3]
        ).start()

    my_columns = pl.ds(pl.multiple_of(x * quarter, 128), quarter)

    def length_of(way, b):
        return turns if (b % 2 == 0) == (way == 0) else turns - 1

    def ready(b):
        arrived(att.at[2, :, b], att_sem.at[2, b])
        lhs = jnp.concatenate([att[r, :, b].reshape(stripe, hs) for r in range(NX)], axis=1)
        for s in range(subs):
            column = slice(s * SUB, (s + 1) * SUB)
            term = jnp.dot(lhs, wo2[:, column], preferred_element_type=F32)
            own_term[b, :, :, column] = term.reshape(nz, rows, SUB)
        fin[b] = own_term[b, z].astype(BF)

    def reduce_step(b, step):
        for way in (0, 1):
            length = length_of(way, b)
            slot = (2 * b + way) * turns + step
            z_next = z_down if way else z_up

            def one(b=b, way=way, length=length, slot=slot, z_next=z_next):
                target = lax.rem(z + (1 - 2 * way) * (length - step + 1) + nz, nz)
                term = own_term[b, target]
                if not (isinstance(step, int) and step == 1):
                    arrived(rs_recv.at[slot - 1], rs_sem.at[slot - 1])
                    term = term + rs_recv[slot - 1].astype(F32)
                rs_send[slot - 1] = term.astype(BF)

                def go_on():
                    remote(
                        rs_send.at[slot - 1],
                        rs_recv.at[slot],
                        send_sem.at[18],
                        rs_sem.at[slot],
                        tensor_1=z_next,
                    ).start()

                def deliver():
                    remote(
                        rs_send.at[slot - 1],
                        out.at[1 + way, :, my_columns],
                        send_sem.at[18],
                        fin_sem.at[0],
                        tensor_0=jnp.int32(b),
                        tensor_1=z_next,
                    ).start()

                if isinstance(step, int):
                    (go_on if step < length else deliver)()
                else:
                    pl.when(step < length)(go_on)
                    pl.when(step == length)(deliver)

            if isinstance(step, int):
                if step <= length:
                    one()
            else:
                pl.when(step <= length)(one)

    for b in range(NX):
        attend(b)
        att_send(b)
    out_to_sibling(from_other, 2)
    out_to_sibling(2, 3)
    for b in range(NX):
        att_pass(b)
    out_weights_wait()
    for b in range(NX):
        ready(b)
        reduce_step(b, 1)
    for d in (1, 2, 3):
        remote(
            fin.at[xs[d]],
            out.at[0, :, my_columns],
            send_sem.at[19],
            fin_sem.at[0],
            tensor_0=xs[d],
        ).start()
    pltpu.make_async_copy(fin.at[x], out.at[0, :, my_columns], fin_sem.at[0]).start()

    def reduce_round(step, carry):
        for b in range(NX):
            reduce_step(b, step)
        return carry

    lax.fori_loop(2, turns + 1, reduce_round, 0)

    n_ring = turns * 2 - 1
    arrived(x_wide.at[pl.ds(0, 3), :, 0], send_sem.at[0])
    arrived(z_part.at[0, :, 0], send_sem.at[1])
    arrived(fv_stage, send_sem.at[2])
    arrived(x_wide.at[pl.ds(0, n_ring)], send_sem.at[3])
    arrived(w2.at[pl.ds(0, share), pl.ds(0, width)], send_sem.at[4])
    arrived(z_part.at[pl.ds(0, n_ring), :, pl.ds(0, 2)], send_sem.at[5])
    arrived(z_part.at[:, :, pl.ds(0, 2)], send_sem.at[6])
    arrived(w2.at[pl.ds(0, share), pl.ds(0, width)], send_sem.at[7])
    arrived(fv_own.at[pl.ds(1, nz - 1)], send_sem.at[8])
    arrived(b_send, send_sem.at[10])
    arrived(wo2.at[pl.ds(0, 3 * hs), pl.ds(0, half)], send_sem.at[11])
    arrived(wo2.at[pl.ds(0, 3 * hs), pl.ds(0, half)], send_sem.at[12])
    arrived(wo_relay, send_sem.at[13])
    arrived(att.at[0], send_sem.at[14])
    arrived(att.at[0], send_sem.at[15])
    arrived(att.at[0, near], send_sem.at[16])
    arrived(att.at[0, far], send_sem.at[17])
    arrived(rs_recv.at[pl.ds(0, 3 * NX)], fin_sem.at[0])
    arrived(rs_send.at[pl.ds(0, NX * n_ring)], send_sem.at[18])
    arrived(fin.at[pl.ds(0, 3)], send_sem.at[19])


def body(hidden_in, first_values, qkv_weight, out_weight, mix_table, mix_index, lengths, *, nz):
    rows, model = hidden_in.shape[1:]
    hs = qkv_weight.shape[2]
    quarter = model // NX
    half = quarter // 2
    halves = model // 2
    subs = quarter // SUB
    x_subs = max(1, halves * 3 // 10 // SUB)
    z_subs = 2
    z_wide = (halves - x_subs * SUB) // z_subs
    turns = nz // 2
    block = NX * rows
    anywhere = pl.BlockSpec(memory_space=pl.ANY)
    dma = pltpu.SemaphoreType.DMA
    scratch = [
        pltpu.VMEM((rows, model), BF),
        pltpu.VMEM(first_values.shape[1:], BF),
        pltpu.SMEM(mix_table.shape[::-1], F32),
        pltpu.SMEM(mix_index.shape, jnp.int32),
        pltpu.SMEM(lengths.shape, jnp.int32),
        dma((5,)),
        pltpu.VMEM((nz, x_subs, NX, rows, SUB), BF),
        pltpu.VMEM((nz, z_subs, NX, rows, z_wide), BF),
        pltpu.VMEM((halves, 2 * 3 * hs), BF),
        pltpu.VMEM((NX * hs, quarter), BF),
        pltpu.VMEM((hs, half), BF),
        pltpu.VMEM((NX - 1, nz, rows, hs), BF),
        pltpu.VMEM((nz, NX, rows, hs), BF),
        pltpu.VMEM((nz, NX, rows, hs), BF),
        pltpu.VMEM((nz, block, 3 * hs), F32),
        pltpu.VMEM((nz, block, 3 * hs), BF),
        pltpu.VMEM((nz, block, 3 * hs), BF),
        pltpu.VMEM((NX, nz, rows, hs), BF),
        pltpu.VMEM((NX, nz, rows, hs), BF),
        pltpu.VMEM((NX, nz, rows, hs), BF),
        pltpu.VMEM((NX, nz, NX, rows, hs), BF),
        pltpu.VMEM((NX * 2 * turns, rows, quarter), BF),
        pltpu.VMEM((NX * 2 * turns, rows, quarter), BF),
        pltpu.VMEM((NX, nz, rows, quarter), F32),
        pltpu.VMEM((NX, rows, quarter), BF),
        dma((2,)),
        dma((20,)),
        dma((2,)),
        dma((NX,)),
        dma((2, turns, x_subs + z_subs)),
        dma((nz,)),
        dma((2, 3)),
        dma((7,)),
        dma((1,)),
        dma((1,)),
        dma((nz,)),
        dma((3, NX)),
        dma((NX * 2 * turns,)),
        dma((1,)),
    ]
    result = pl.pallas_call(
        functools.partial(kernel, nz),
        out_shape=jax.ShapeDtypeStruct((3, rows, model), BF),
        in_specs=[anywhere] * 7,
        out_specs=anywhere,
        scratch_shapes=scratch,
        compiler_params=pltpu.CompilerParams(
            collective_id=0, has_side_effects=True, vmem_limit_bytes=60 * 1024 * 1024
        ),
    )(
        hidden_in[0],
        first_values[0],
        jnp.transpose(qkv_weight, (1, 0, 2)),
        out_weight,
        mix_table.T,
        mix_index,
        lengths,
    )
    first, second, third = (piece.astype(F32) for piece in result)
    return (first + second + third).astype(BF)[None]


def solution(mesh):
    nz = mesh.shape["tensor"] // NX
    torus = Mesh(
        mesh.devices.reshape(mesh.shape["groups"], mesh.shape["dp"], NX, nz),
        ("groups", "dp", "tensor_0", "tensor_1"),
    )
    placed = (
        P(("groups", "dp"), TENSOR, None),
        P(("groups", "dp"), TENSOR, None),
        P(None, None, TENSOR),
        P(TENSOR, None),
        P(),
        P(TENSOR),
        P(("groups", "dp")),
    )
    return jax.shard_map(
        functools.partial(body, nz=nz),
        mesh=torus,
        in_specs=placed,
        out_specs=P(("groups", "dp"), TENSOR, None),
        check_vma=False,
    )
```
